256 devices in a mesh: graph: 32 (over y, z_lo, core), chan: 8 (over x, z_hi).
Axes of the slice: x: 4, y: 4, z: 8 (z_hi: 2, z_lo: 4; z = z_hi * 4 + z_lo), core: 2. Of those that a mesh axis runs over, the one named last changes fastest.
Arguments:
- embed: bfloat16 [25, 512, 4096], P(None, 'chan', 'graph'), may hold values from -200 to 200
- gain: float32 [5, 512], P(None, 'chan'), may hold values from 0.25 to 1.75
- w_zero: bfloat16 [5, 512, 2560], P(None, 'chan'), may hold values from -0.125 to 0.125
- w_one: bfloat16 [2, 4, 512, 2048], P(None, None, 'chan'), may hold values from -0.125 to 0.125
- w_two: bfloat16 [2, 3, 512, 1536], P(None, None, 'chan'), may hold values from -0.15625 to 0.15625
- rot_table: float32 [19, 25, 256], replicated, may hold values from -1 to 1, as said below
- face_atoms: int32 [1024], P('graph'), may hold values from 0 to 127, as said below
- edge_source: int32 [4096], P('graph'), may hold values from 0 to 159
- edge_target: int32 [4096], P('graph'), may hold values from 0 to 127
- rot_index: int32 [4096], P('graph'), may hold values from 0 to 255
- edge_weight: float32 [4096], P('graph'), may hold values from 0.2 to 1
- cotangent: bfloat16 [25, 512, 4096], P(None, 'chan', 'graph'), may hold values from -1.5 to 1.5
Outputs:
- update: bfloat16 [25, 512, 4096], P(None, 'chan', 'graph')
- grad_embed: bfloat16 [25, 512, 4096], P(None, 'chan', 'graph')
- grad_zero: float32 [5, 512, 2560], P(None, 'chan', 'graph')
- grad_one: float32 [2, 4, 512, 2048], P(None, None, 'chan', 'graph')
- grad_two: float32 [2, 3, 512, 1536], P(None, None, 'chan', 'graph')
The draws below stay inside these ranges and needn't reach their ends.
Inputs may be any that keep to these rules, and one draw needn't show every extreme that they name: `rot_table`: for every rotation, frame row (m, l) is nonzero only on the 2l + 1 coefficients of degree l, where it is row l + m of an orthogonal (2l + 1)-square matrix shared by the rows of that degree; the degree-0 entry is 1. `face_atoms`: block b holds 32 distinct atom indices counted from the first atom of block b: the first 16 lie at the face toward block b - 1, the last 16 at the face toward block b + 1. `edge_source`: read as in the step that defines src. `edge_target`: counted from the first atom of the edge's block.
All inputs are finite; a program needn't handle non-finite values.
Results may differ from the reference program's by a relative error of at most 0.0062.
Values may be sent and summed in bfloat16 or wider, within the bound.
A program may use at most 128 MiB of HBM per device.

```python
import math
import jax
import jax.numpy as jnp
from jax import lax

C = 512
ATOM_DEV = 128
HALO = 16
EDGE_DEV = 128
ROTS = 256
ATOMS = 4096
EDGES = 4096
FACES = 1024
N_GRAPH = 32


FRAME = ((0, 0), (1, 0), (2, 0), (3, 0), (4, 0), (1, 1), (2, 1), (3, 1), (4, 1), (1, -1), (2, -1), (3, -1), (4, -1), (2, 2), (3, 2), (4, 2), (2, -2), (3, -2), (4, -2))


def draw_embed(key, part):
    keys = jax.random.split(key, 4)
    ramp = jnp.arange(C, dtype=jnp.float32) / C - 0.5
    channel_scale = jnp.exp(math.log(10.0) * ramp) * jax.random.uniform(keys[1], (C,), jnp.float32, 0.7, 1.4)
    atom_scale = jnp.exp(jax.random.uniform(keys[2], (ATOMS,), jnp.float32, math.log(0.3), math.log(3.0)))
    raw = jnp.clip(jax.random.normal(keys[0], (25, C, ATOMS), jnp.float32), -6.0, 6.0)
    values = raw * channel_scale[None, :, None] * atom_scale[None, None, :]
    return jnp.clip(values, -200.0, 200.0).astype(jnp.bfloat16)


def reflect_block(key, size):
    matrix = jnp.broadcast_to(jnp.eye(size, dtype=jnp.float32), (ROTS, size, size))
    for index in range(size):
        vector = jax.random.normal(jax.random.fold_in(key, index), (ROTS, size), jnp.float32)
        vector = vector / jnp.sqrt(jnp.sum(vector * vector, axis=1, keepdims=True) + 1e-12)
        folded = jnp.einsum('rj,rjk->rk', vector, matrix)
        matrix = matrix - 2.0 * vector[:, :, None] * folded[:, None, :]
    return matrix


def draw_rot_table(key, part):
    blocks = [jnp.ones((ROTS, 1, 1), jnp.float32)]
    for degree in range(1, 5):
        blocks.append(reflect_block(jax.random.fold_in(key, 100 + degree), 2 * degree + 1))
    lines = []
    for pair in FRAME:
        degree = pair[0]
        line = jnp.zeros((ROTS, 25), jnp.float32)
        line = line.at[:, degree * degree:(degree + 1) * (degree + 1)].set(blocks[degree][:, degree + pair[1], :])
        lines.append(line)
    table = jnp.stack(lines, axis=0)
    return jnp.transpose(table, (0, 2, 1))


def draw_face_atoms(key, part):
    count = FACES // (2 * HALO)
    keys = jax.random.split(key, count)
    picks = jax.vmap(lambda single: jax.random.permutation(single, ATOM_DEV)[:2 * HALO])(keys)
    return picks.reshape(FACES).astype(jnp.int32)


def with_ends(entries, own_key, low, largest):
    longest = entries.shape.index(max(entries.shape))
    spots = []
    for shift in (0, 1):
        where = [jax.random.randint(jax.random.fold_in(own_key, axis), (), 0, length) for axis, length in enumerate(entries.shape)]
        where[longest] = (where[longest] + shift) % entries.shape[longest]
        spots.append(tuple(where))
    return entries.at[spots[0]].set(low).at[spots[1]].set(largest)


def steps_of(own_key, extent, shards, low, high):
    def one(axis_at, blocks):
        heights = jax.random.uniform(jax.random.fold_in(jax.random.fold_in(own_key, 6), axis_at), (blocks,), jnp.float32, low / len(shards), high / len(shards))
        return jnp.repeat(jnp.exp(heights), extent[axis_at] // blocks).reshape((-1,) + (1,) * (len(extent) - axis_at - 1))

    factor_of = one(*shards[0])
    for cut in shards[1:]:
        factor_of = factor_of * one(*cut)
    return factor_of


def normal_values(rng, dims, scale, reach, cuts=(), kind=jnp.bfloat16):
    entries = scale * jax.random.normal(rng, dims, jnp.float32)
    if cuts:
        entries = entries * steps_of(rng, dims, cuts, -0.22, 0.18)
    return jnp.clip(entries, -reach, reach).astype(kind)


def setup_inputs(seed: int = 0) -> dict:
    splits = jax.random.split(jax.random.key(seed), 13)
    embed = draw_embed(jax.random.fold_in(splits[12], 71), 0)
    gain = jnp.clip(1.0 + 0.15 * jax.random.normal(splits[1], (5, C), jnp.float32), 0.25, 1.75)
    w_zero = normal_values(splits[2], (5, C, 5 * C), (5 * C) ** -0.5, 0.125, ((1, 8),))
    w_one = normal_values(splits[3], (2, 4, C, 4 * C), (4 * C) ** -0.5, 0.125, ((2, 8),))
    w_two = normal_values(splits[4], (2, 3, C, 3 * C), (3 * C) ** -0.5, 0.15625, ((2, 8),))
    rot_table = draw_rot_table(jax.random.fold_in(splits[12], 71), 0)
    face_atoms = draw_face_atoms(jax.random.fold_in(splits[12], 71), 0)
    edge_source = with_ends(jax.random.randint(splits[7], (EDGES,), 0, ATOM_DEV + 2 * HALO), jax.random.fold_in(splits[7], 1), 0, (ATOM_DEV + 2 * HALO) - 1).astype(jnp.int32)
    edge_target = with_ends(jax.random.randint(splits[8], (EDGES,), 0, ATOM_DEV), jax.random.fold_in(splits[8], 1), 0, ATOM_DEV - 1).astype(jnp.int32)
    rot_index = with_ends(jax.random.randint(splits[9], (EDGES,), 0, ROTS), jax.random.fold_in(splits[9], 1), 0, ROTS - 1).astype(jnp.int32)
    edge_weight = jnp.clip(jnp.exp(math.log(1.0) - 1.609438 * jax.random.uniform(splits[10], (EDGES,), jnp.float32) ** steps_of(splits[10], (EDGES,), ((0, 32),), -0.2, 0.2)), 0.2, 1.0)
    cotangent = normal_values(splits[11], (25, C, ATOMS), 0.25, 1.5, ((1, 8), (2, 32)))
    return {"embed": embed, "gain": gain, "w_zero": w_zero, "w_one": w_one, "w_two": w_two, "rot_table": rot_table, "face_atoms": face_atoms, "edge_source": edge_source, "edge_target": edge_target, "rot_index": rot_index, "edge_weight": edge_weight, "cotangent": cotangent}


EPSILON = 1e-06
HIGHEST = lax.Precision.HIGHEST
FRAME = ((0, 0), (1, 0), (2, 0), (3, 0), (4, 0), (1, 1), (2, 1), (3, 1), (4, 1), (1, -1), (2, -1), (3, -1), (4, -1), (2, 2), (3, 2), (4, 2), (2, -2), (3, -2), (4, -2))

def gain_rows(gain):
    pieces = [jnp.broadcast_to(gain[degree:degree + 1], (2 * degree + 1, gain.shape[1])) for degree in range(5)]
    return jnp.concatenate(pieces, axis=0)

def product(left, right):
    return jnp.dot(left, right, preferred_element_type=jnp.float32)

def across(left, right):
    return lax.dot_general(left, right, (((0,), (0,)), ((), ())), preferred_element_type=jnp.float32)

def outer(left, right):
    return lax.dot_general(left, right, (((1,), (1,)), ((), ())), preferred_element_type=jnp.float32)

def stack_frame(parts, width, edges):
    row_counts = (5, 4, 4, 3, 3)
    return jnp.concatenate([part.reshape(rows, width, edges) for part, rows in zip(parts, row_counts)], axis=0)

def mix_part(w_zero, w_one, w_two, piece, start):
    count = piece.shape[1]
    edges = piece.shape[2]
    outputs = w_zero.shape[1]

    def columns(weight, blocks):
        shaped = weight.reshape(blocks * outputs, blocks, weight.shape[-1] // blocks)
        return lax.dynamic_slice_in_dim(shaped, start, count, 2).reshape(blocks * outputs, blocks * count)

    def frame_rows(first, blocks):
        return piece[first:first + blocks].reshape(blocks * count, edges)
    parts = [product(columns(w_zero, 5), frame_rows(0, 5))]
    for weights, first, blocks in ((w_one, 5, 4), (w_two, 13, 3)):
        real_part = columns(weights[0], blocks)
        imag_part = columns(weights[1], blocks)
        plus = frame_rows(first, blocks)
        minus = frame_rows(first + blocks, blocks)
        parts.append(product(real_part, plus) - product(imag_part, minus))
        parts.append(product(real_part, minus) + product(imag_part, plus))
    return tuple(parts)

def mix_backward(w_zero, w_one, w_two, grads, frame):
    outputs = grads.shape[1]
    width = frame.shape[1]
    edges = grads.shape[2]

    def grad_rows(first, blocks):
        return grads[first:first + blocks].reshape(blocks * outputs, edges)

    def frame_rows(first, blocks):
        return frame[first:first + blocks].reshape(blocks * width, edges)
    zero_weight = w_zero.reshape(5 * outputs, 5 * width)
    grad_first = grad_rows(0, 5)
    back = [across(zero_weight, grad_first)]
    weight_zero = outer(grad_first, frame_rows(0, 5)).reshape(5, outputs, 5 * width)
    pairs = []
    for weights, first, blocks in ((w_one, 5, 4), (w_two, 13, 3)):
        real_part = weights[0].reshape(blocks * outputs, blocks * width)
        imag_part = weights[1].reshape(blocks * outputs, blocks * width)
        grad_plus = grad_rows(first, blocks)
        grad_minus = grad_rows(first + blocks, blocks)
        frame_plus = frame_rows(first, blocks)
        frame_minus = frame_rows(first + blocks, blocks)
        back.append(across(real_part, grad_plus) + across(imag_part, grad_minus))
        back.append(across(real_part, grad_minus) - across(imag_part, grad_plus))
        real_grad = outer(grad_plus, frame_plus) + outer(grad_minus, frame_minus)
        imag_grad = outer(grad_minus, frame_plus) - outer(grad_plus, frame_minus)
        pairs.append(jnp.stack([real_grad.reshape(blocks, outputs, blocks * width), imag_grad.reshape(blocks, outputs, blocks * width)]))
    return (stack_frame(back, width, edges), weight_zero, pairs[0], pairs[1])

def reference(embed, gain, w_zero, w_one, w_two, rot_table, face_atoms, edge_source, edge_target, rot_index, edge_weight, cotangent):
    values = embed.astype(jnp.float32)
    gains = gain_rows(gain)
    inverse = lax.rsqrt(lax.optimization_barrier(jnp.sum(values * values, axis=(0, 1))) / (25 * C) + EPSILON)
    normed = (values * inverse[None, None, :] * gains[:, :, None]).astype(jnp.bfloat16)
    positions = jnp.arange(ATOM_DEV, dtype=jnp.int32)

    def shard_step(carry, shard):
        update, grad_normed, grad_zero, grad_one, grad_two = carry
        left = (shard - 1) % N_GRAPH
        right = (shard + 1) % N_GRAPH
        from_left = lax.dynamic_slice_in_dim(face_atoms, left * (2 * HALO) + HALO, HALO)
        from_right = lax.dynamic_slice_in_dim(face_atoms, right * (2 * HALO), HALO)
        lookup = jnp.concatenate([shard * ATOM_DEV + positions, left * ATOM_DEV + from_left, right * ATOM_DEV + from_right]).astype(jnp.int32)
        first = (shard * EDGE_DEV).astype(jnp.int32)
        sources = lookup[lax.dynamic_slice_in_dim(edge_source, first, EDGE_DEV)]
        targets = (shard * ATOM_DEV + lax.dynamic_slice_in_dim(edge_target, first, EDGE_DEV)).astype(jnp.int32)
        rotations = jnp.take(rot_table, lax.dynamic_slice_in_dim(rot_index, first, EDGE_DEV), axis=2)
        scale = lax.dynamic_slice_in_dim(edge_weight, first, EDGE_DEV)
        gathered = jnp.take(normed, sources, axis=2).astype(jnp.float32)
        frame = jnp.einsum('jke,kce->jce', rotations, gathered, precision=HIGHEST).astype(jnp.bfloat16)
        mixed = stack_frame(mix_part(w_zero, w_one, w_two, frame, 0), C, EDGE_DEV)
        message = jnp.einsum('jke,jce->kce', rotations, mixed * scale[None, None, :], precision=HIGHEST).astype(jnp.bfloat16)
        update = update.at[:, :, targets].add(message.astype(jnp.float32))
        arriving = jnp.take(cotangent, targets, axis=2).astype(jnp.float32)
        grads = (jnp.einsum('jke,kce->jce', rotations, arriving, precision=HIGHEST) * scale[None, None, :]).astype(jnp.bfloat16)
        back, part_zero, part_one, part_two = mix_backward(w_zero, w_one, w_two, grads, frame)
        spread = jnp.einsum('jke,jce->kce', rotations, back, precision=HIGHEST)
        grad_normed = grad_normed.at[:, :, sources].add(spread)
        return ((update, grad_normed, grad_zero + part_zero, grad_one + part_one, grad_two + part_two), None)
    start = (jnp.zeros((25, C, ATOMS), jnp.float32), jnp.zeros((25, C, ATOMS), jnp.float32), jnp.zeros((5, C, 5 * C), jnp.float32), jnp.zeros((2, 4, C, 4 * C), jnp.float32), jnp.zeros((2, 3, C, 3 * C), jnp.float32))
    final, unused = lax.scan(shard_step, start, jnp.arange(N_GRAPH, dtype=jnp.int32))
    update, grad_normed, grad_zero, grad_one, grad_two = final
    tally = lax.optimization_barrier(jnp.sum(values * gains[:, :, None] * grad_normed, axis=(0, 1)))
    grad_embed = (inverse[None, None, :] * gains[:, :, None] * grad_normed - values * (inverse ** 3 * tally / (25 * C))[None, None, :]).astype(jnp.bfloat16)
    return (update.astype(jnp.bfloat16), grad_embed, grad_zero, grad_one, grad_two)
```

```python
import jax
import jax.numpy as jnp
from jax import lax
from jax.experimental import pallas as pl
from jax.experimental.pallas import tpu as pltpu
from jax.sharding import Mesh
from jax.sharding import PartitionSpec as P

C = 512
EPSILON = 1e-06
CHAN = ("x", "zh")
GRAPH = ("y", "z", "core")
DEGREE = (0, 1, 2, 3, 4, 1, 2, 3, 4, 1, 2, 3, 4, 2, 3, 4, 2, 3, 4)
ROWS = tuple(tuple(j for j in range(19) if DEGREE[j] == l) for l in range(5))
F32 = jnp.float32
BF16 = jnp.bfloat16
VMEM_LIMIT = 60 * 1024 * 1024
MESH = pl.DeviceIdType.MESH
PIECES = (slice(0, 10), slice(10, 19))
HALVES = (slice(0, 320), slice(320, 640))


def nt(left, right):
    return lax.dot_general(left, right, (((1,), (1,)), ((), ())), preferred_element_type=F32)


def tn(left, right):
    return lax.dot_general(left, right, (((0,), (0,)), ((), ())), preferred_element_type=F32)


def nn(left, right):
    return jnp.dot(left, right, preferred_element_type=F32)


def hot(index_row, rows, first=0):
    edges = index_row.shape[1]
    row = lax.broadcasted_iota(jnp.int32, (rows, edges), 0) + first
    return jnp.where(row == index_row, 1.0, 0.0).astype(BF16)


def rotate_in(rot, values, j):
    l = DEGREE[j]
    total = None
    for k in range(l * l, (l + 1) * (l + 1)):
        term = rot[j, k : k + 1, :] * values[k]
        total = term if total is None else total + term
    return total


def rotate_out(rot, values, k, l):
    total = None
    for j in ROWS[l]:
        term = rot[j, k : k + 1, :] * values[j]
        total = term if total is None else total + term
    return total


class Net:
    def __init__(self, send, recv):
        self.send, self.recv, self.started = send, recv, []

    def copy(self, source, landing, device):
        at = len(self.started)
        assert at < COPIES
        one = pltpu.make_async_remote_copy(
            src_ref=source,
            dst_ref=landing,
            send_sem=self.send.at[at],
            recv_sem=self.recv.at[at],
            device_id=device,
            device_id_type=MESH,
        )
        one.start()
        self.started.append(one)
        return one

    def finish(self):
        for one in self.started:
            one.wait_send()


COPIES = 83


def layer_kernel(
    embed, cotangent, gain_t, rot_table, face, face_left, face_right,
    source, target, spin, weight, w_zero_hbm, w_one_hbm, w_two_hbm,
    update, grad_embed, sums,
    w_zero, w_one, w_two, faces, halo_t, rot, values, grads, mine, square, squares, every, twin,
    back, relay_left, relay_right, from_left, from_right, to_far, far,
    scaled, scaled_twin, flat_zero, flat_one, flat_two, sel_zero, sel_one, sel_two,
    right_zero, right_one, right_two, part, pass_left, pass_right, up_left, up_right,
    to_line, line, kept, mixed, message, tally, tallies, own, leaving, returned,
    tally_out, tally_in, settled, send, recv, load,
):
    x, h = lax.axis_index("x"), lax.axis_index("zh")
    y, z, core = lax.axis_index("y"), lax.axis_index("z"), lax.axis_index("core")
    xr, xl, xo = lax.rem(x + 1, 4), lax.rem(x + 3, 4), lax.rem(x + 2, 4)
    yr, yl, yo = lax.rem(y + 1, 4), lax.rem(y + 3, 4), lax.rem(y + 2, 4)
    me = y * 8 + z * 2 + core
    ahead, behind = lax.rem(me + 1, 32), lax.rem(me + 31, 32)

    def graph_at(g):
        return {"y": g // 8, "z": lax.rem(g // 2, 4), "core": lax.rem(g, 2)}

    to_xr, to_xl = {"x": xr}, {"x": xl}
    to_yr, to_yl = {"y": yr}, {"y": yl}
    to_far_half = {"zh": 1 - h}
    to_twin = {"core": 1 - core}
    to_ahead, to_behind = graph_at(ahead), graph_at(behind)
    chan_peers = [
        {"x": lax.rem(x + dx, 4), "zh": lax.rem(h + dh, 2)}
        for dx in range(4)
        for dh in range(2)
        if dx or dh
    ]
    line_peers = [None] + [{"z": lax.rem(z + o, 4)} for o in (1, 2, 3)]
    chan = x * 2 + h

    local = embed.shape[1]
    atoms = embed.shape[2]
    edges = source.shape[1]
    count = 25 * local
    net = Net(send, recv)

    loads = [
        pltpu.make_async_copy(a, b, load.at[i])
        for i, (a, b) in enumerate(
            ((w_zero_hbm, w_zero), (w_one_hbm, w_one), (w_two_hbm, w_two))
        )
    ]
    for one in loads:
        one.start()

    barrier = pltpu.get_barrier_semaphore()
    partners = chan_peers + line_peers[1:] + [to_yr, to_yl, to_ahead, to_behind]
    for device in partners:
        pl.semaphore_signal(barrier, inc=1, device_id=device, device_id_type=MESH)

    face_col = lax.broadcasted_iota(jnp.int32, (face.shape[0], atoms), 1)
    face_hot = jnp.where(face_col == face[...], 1.0, 0.0).astype(BF16)
    flat_embed = embed[...].reshape(count, atoms)
    faces[...] = nt(face_hot, flat_embed).astype(BF16)
    pl.semaphore_wait(barrier, len(partners))
    halo = [
        net.copy(faces.at[16:32], halo_t.at[0:16], to_ahead),
        net.copy(faces.at[0:16], halo_t.at[16:32], to_behind),
    ]

    turn = hot(spin[...], rot_table.shape[2])
    for j in range(19):
        line_j = rot_table[j]
        high = line_j.astype(BF16)
        low = (line_j - high.astype(F32)).astype(BF16)
        rot[j] = nn(high, turn) + nn(low, turn)
    total_a = jnp.zeros((1, atoms), F32)
    for k in range(25):
        one = embed[k].astype(F32)
        total_a = total_a + jnp.sum(one * one, axis=0, keepdims=True)
    here = hot(source[...], atoms)
    near = hot(source[...], 32, atoms)

    for one in halo:
        one.wait_recv()
    values[...] = (nn(flat_embed, here) + tn(halo_t[...], near)).reshape(25, local, edges)
    for j in range(19):
        l = DEGREE[j]
        mine[j] = (rotate_in(rot, values, j) * gain_t[:, l : l + 1]).astype(BF16)
    first, second = (
        [mine.at[p] for p in PIECES],
        [every.at[p, chan] for p in PIECES],
    )
    cross = [net.copy(first[p], second[p], to_far_half) for p in (0, 1)]
    near_r = [net.copy(first[p], second[p], to_xr) for p in (0, 1)]
    near_l = [net.copy(first[p], second[p], to_xl) for p in (1, 0)][::-1]
    twins = [net.copy(mine, twin.at[:, chan], to_twin)]
    total_e = jnp.zeros((1, edges), F32)
    for k in range(25):
        one = values[k]
        total_e = total_e + jnp.sum(one * one, axis=0, keepdims=True)
    square[...] = jnp.concatenate([total_e, total_a, jnp.zeros((6, edges), F32)], axis=0)
    asked = [net.copy(square, squares.at[i], d) for i, d in enumerate(chan_peers)]
    for j in range(19):
        every[j, chan] = mine[j]

    arrive = hot(target[...], atoms)
    values[...] = nn(cotangent[...].reshape(count, atoms), arrive).reshape(25, local, edges)
    for j in range(19):
        grads[j] = (rotate_in(rot, values, j) * weight[...]).astype(BF16)

    def forward(p, x_from, h_from, device):
        block = every.at[PIECES[p], x_from * 2 + h_from]
        return net.copy(block, block, device)

    def to_other_core(x_from, h_from):
        at = x_from * 2 + h_from
        twins.append(net.copy(every.at[:, at], twin.at[:, at], to_twin))

    for one in loads:
        one.wait()
    back[0:5] = tn(
        w_zero[...].reshape(5 * local, 5 * C), grads[0:5].reshape(5 * local, edges)
    ).astype(BF16).reshape(5, 8, local, edges)

    near_r[0].wait_recv()
    over_r = [forward(0, xl, h, to_xr)]
    near_l[1].wait_recv()
    over_l = [forward(1, xr, h, to_xl)]
    cross_r, cross_l = [], []
    cross[0].wait_recv()
    cross_r.append(forward(0, x, 1 - h, to_xr))
    cross_l.append(forward(0, x, 1 - h, to_xl))

    for w, start, blocks in ((w_one, 5, 4), (w_two, 13, 3)):
        plus = grads[start : start + blocks].reshape(blocks * local, edges)
        minus = grads[start + blocks : start + 2 * blocks].reshape(blocks * local, edges)
        both = jnp.concatenate([plus, minus], axis=1)
        turned = jnp.concatenate([minus, -plus], axis=1)
        size = blocks * C
        out = tn(w[0].reshape(blocks * local, size), both) + tn(
            w[1].reshape(blocks * local, size), turned
        )
        back[start : start + blocks] = (
            out[:, :edges].astype(BF16).reshape(blocks, 8, local, edges)
        )
        back[start + blocks : start + 2 * blocks] = (
            out[:, edges:].astype(BF16).reshape(blocks, 8, local, edges)
        )

    for one in asked:
        one.wait_recv()
    square_sum = square[...]
    for i in range(7):
        square_sum = square_sum + squares[i]
    inverse_both = lax.rsqrt(square_sum / (25 * C) + EPSILON)
    inverse, inverse_a = inverse_both[0:1, :], inverse_both[1:2, :]
    for j in range(19):
        scaled[j] = (grads[j].astype(F32) * inverse).astype(BF16)
    scaled_copy = net.copy(scaled, scaled_twin, to_twin)

    cross[1].wait_recv()
    cross_r.append(forward(1, x, 1 - h, to_xr))
    cross_l.append(forward(1, x, 1 - h, to_xl))
    to_other_core(x, 1 - h)
    near_r[1].wait_recv()
    to_other_core(xl, h)
    near_l[0].wait_recv()
    to_other_core(xr, h)
    over_r[0].wait_recv()
    over_l[0].wait_recv()
    to_other_core(xo, h)
    cross_r[0].wait_recv()
    over_r.append(forward(0, xl, 1 - h, to_xr))
    cross_l[1].wait_recv()
    over_l.append(forward(1, xr, 1 - h, to_xl))

    half = (1 - h, h)
    steps = []
    for q in (0, 1):
        steps.append(
            [
                net.copy(back.at[PIECES[0], xo * 2 + half[q]], relay_left.at[q], to_xr),
                net.copy(back.at[PIECES[1], xo * 2 + half[q]], relay_right.at[q], to_xl),
                net.copy(
                    back.at[PIECES[1], xr * 2 + half[q]], from_left.at[q, PIECES[1]], to_xr
                ),
                net.copy(
                    back.at[PIECES[0], xl * 2 + half[q]], from_right.at[q, PIECES[0]], to_xl
                ),
            ]
        )

    cross_r[1].wait_recv()
    to_other_core(xl, 1 - h)
    cross_l[0].wait_recv()
    to_other_core(xr, 1 - h)
    over_r[1].wait_recv()
    over_l[1].wait_recv()
    to_other_core(xo, 1 - h)

    def spread_flat(buffer, lane):
        def rows(start, blocks):
            return buffer[start : start + blocks].reshape(blocks * C, edges)

        flat_zero[:, lane * edges : (lane + 1) * edges] = rows(0, 5)
        for flat, start, blocks in ((flat_one, 5, 4), (flat_two, 13, 3)):
            for i in (0, 1):
                at = (2 * lane + i) * edges
                flat[:, at : at + edges] = rows(start + i * blocks, blocks)

    spread_flat(every, 0)

    def right_side(buffer, lane):
        wide = 5 * local
        right_zero[0:wide, lane * edges : (lane + 1) * edges] = buffer[0:5].reshape(wide, edges)
        for right, start, blocks in ((right_one, 5, 4), (right_two, 13, 3)):
            rows = blocks * local
            plus = buffer[start : start + blocks].reshape(rows, edges)
            minus = buffer[start + blocks : start + 2 * blocks].reshape(rows, edges)
            at = 2 * lane * edges
            right[0:rows, at : at + edges] = plus
            right[0:rows, at + edges : at + 2 * edges] = minus
            right[rows : 2 * rows, at : at + edges] = minus
            right[rows : 2 * rows, at + edges : at + 2 * edges] = -plus

    right_zero[...] = jnp.zeros_like(right_zero)
    right_side(scaled, 0)
    scaled_copy.wait_recv()
    right_side(scaled_twin, 1)
    for one in twins:
        one.wait_recv()
    spread_flat(twin, 1)
    for flat, sel, rows in (
        (flat_zero, sel_zero, 80),
        (flat_one, sel_one, 64),
        (flat_two, sel_two, 48),
    ):
        for i in range(16):
            begin = pl.multiple_of((2 * i + core) * rows, 16)
            sel[i * rows : (i + 1) * rows, :] = flat[pl.ds(begin, rows), :]
    at = 0
    for sel, right, rows, tiles in (
        (sel_zero, right_zero, 80, 3),
        (sel_one, right_one, 64, 4),
        (sel_two, right_two, 48, 3),
    ):
        for quarter in range(4):
            out = nt(sel[quarter * 4 * rows : (quarter + 1) * 4 * rows, :], right[...])
            out = out.astype(BF16).reshape(4, rows, 128 * tiles)
            for tile in range(tiles):
                part[quarter, :, at + tile * rows : at + (tile + 1) * rows, :] = out[
                    :, :, 128 * tile : 128 * (tile + 1)
                ]
        at += rows * tiles

    climbs = {}

    def climb(o):
        to = lax.rem(z + o, 4)
        climbs[o] = [
            net.copy(part.at[yo, to, HALVES[0]], pass_left.at[o], to_yr),
            net.copy(part.at[yo, to, HALVES[1]], pass_right.at[o], to_yl),
            net.copy(part.at[yr, to, HALVES[1]], up_left.at[o, HALVES[1]], to_yr),
            net.copy(part.at[yl, to, HALVES[0]], up_right.at[o, HALVES[0]], to_yl),
        ]

    def added(a, b):
        return (a.astype(F32) + b.astype(F32)).astype(BF16)

    def climb_on(o):
        to = lax.rem(z + o, 4)
        climbs[o][0].wait_recv()
        part[yr, to, HALVES[0]] = added(part[yr, to, HALVES[0]], pass_left[o])
        climbs[o].append(
            net.copy(part.at[yr, to, HALVES[0]], up_left.at[o, HALVES[0]], to_yr)
        )
        climbs[o][1].wait_recv()
        part[yl, to, HALVES[1]] = added(part[yl, to, HALVES[1]], pass_right[o])
        climbs[o].append(
            net.copy(part.at[yl, to, HALVES[1]], up_right.at[o, HALVES[1]], to_yl)
        )

    lines = []

    def climbed(o):
        to = lax.rem(z + o, 4)
        for one in climbs[o][2:]:
            one.wait_recv()
        total = part[y, to].astype(F32) + up_left[o].astype(F32) + up_right[o].astype(F32)
        if o:
            to_line[o - 1] = total.astype(BF16)
            lines.append(net.copy(to_line.at[o - 1], line.at[o - 1], line_peers[o]))
        else:
            kept[...] = total

    def step_on(q):
        steps[q][0].wait_recv()
        for j in range(10):
            back[j, xr * 2 + half[q]] = added(back[j, xr * 2 + half[q]], relay_left[q, j])
        steps[q].append(
            net.copy(back.at[PIECES[0], xr * 2 + half[q]], from_left.at[q, PIECES[0]], to_xr)
        )
        steps[q][1].wait_recv()
        for j in range(10, 19):
            back[j, xl * 2 + half[q]] = added(
                back[j, xl * 2 + half[q]], relay_right[q, j - 10]
            )
        steps[q].append(
            net.copy(back.at[PIECES[1], xl * 2 + half[q]], from_right.at[q, PIECES[1]], to_xl)
        )

    def stepped(q):
        for one in steps[q][2:]:
            one.wait_recv()

    def own_sum(q, j):
        return (
            back[j, x * 2 + half[q]].astype(F32)
            + from_left[q, j].astype(F32)
            + from_right[q, j].astype(F32)
        )

    climb(1)
    climb(2)
    step_on(0)

    mixed[0:5] = nn(w_zero[...].reshape(5 * local, 5 * C), flat_zero[:, 0:edges]).reshape(
        5, local, edges
    )
    for w, flat, start, blocks in ((w_one, flat_one, 5, 4), (w_two, flat_two, 13, 3)):
        size = blocks * C
        both = flat[:, 0 : 2 * edges]
        real = nn(w[0].reshape(blocks * local, size), both)
        imag = nn(w[1].reshape(blocks * local, size), both)
        mixed[start : start + blocks] = (real[:, :edges] - imag[:, edges:]).reshape(
            blocks, local, edges
        )
        mixed[start + blocks : start + 2 * blocks] = (
            real[:, edges:] + imag[:, :edges]
        ).reshape(blocks, local, edges)
    total = jnp.zeros((1, edges), F32)
    for j in range(19):
        total = total + jnp.sum(mixed[j] * grads[j].astype(F32), axis=0, keepdims=True)
    tally[...] = jnp.broadcast_to(total, tally.shape)
    counted = [net.copy(tally, tallies.at[i], d) for i, d in enumerate(chan_peers)]

    step_on(1)
    climb_on(1)
    climb(3)
    stepped(0)
    for j in range(19):
        to_far[j] = own_sum(0, j).astype(BF16)
    far_copy = net.copy(to_far, far, to_far_half)
    climb_on(2)
    climb(0)

    scale = weight[...] * inverse
    for j in range(19):
        mixed[j] = mixed[j] * scale
    for l in range(5):
        for k in range(l * l, (l + 1) * (l + 1)):
            message[k] = rotate_out(rot, mixed, k, l).astype(BF16)
    update[...] = (
        nt(message[...].reshape(count, edges), arrive).reshape(25, local, atoms).astype(BF16)
    )

    climbed(1)
    climb_on(3)
    climbed(2)
    climb_on(0)
    stepped(1)
    for j in range(19):
        mixed[j] = own_sum(1, j)
    climbed(3)

    for one in counted:
        one.wait_recv()
    tally_sum = tally[...]
    for i in range(7):
        tally_sum = tally_sum + tallies[i]
    far_copy.wait_recv()
    for j in range(19):
        mixed[j] = mixed[j] + far[j].astype(F32)
    for l in range(5):
        for k in range(l * l, (l + 1) * (l + 1)):
            message[k] = rotate_out(rot, mixed, k, l).astype(BF16)
    flat = message[...].reshape(count, edges)
    leaving[...] = nt(near, flat).astype(BF16)

    def exact(left, right, dims):
        return lax.dot_general(
            left, right, (dims, ((), ())),
            precision=lax.Precision.HIGHEST, preferred_element_type=F32,
        )

    tally_out[...] = exact(
        tally_sum, hot(source[...], 128, atoms).astype(F32), ((1,), (1,))
    )
    halo = [
        net.copy(leaving.at[16:32], returned.at[0:16], to_ahead),
        net.copy(leaving.at[0:16], returned.at[16:32], to_behind),
        net.copy(tally_out, tally_in.at[0], to_ahead),
        net.copy(tally_out, tally_in.at[1], to_behind),
    ]
    own[...] = nt(flat, here).reshape(25, local, atoms)
    tally_a = exact(tally_sum, here.astype(F32), ((1,), (1,)))
    climbed(0)
    for one in halo:
        one.wait_recv()
    settled[...] = tn(returned[...], face_hot).reshape(25, local, atoms)
    wide = lax.broadcasted_iota(jnp.int32, (128, atoms), 1)
    for i, column in ((0, face_left), (1, face_right)):
        tally_a = tally_a + exact(
            tally_in[i], jnp.where(wide == column[...], 1.0, 0.0), ((1,), (0,))
        )
    factor = inverse_a * inverse_a * inverse_a * tally_a[0:1, :] / (25 * C)
    for l in range(5):
        gain = gain_t[:, l : l + 1] * inverse_a
        for k in range(l * l, (l + 1) * (l + 1)):
            grad_embed[k] = (
                (own[k] + settled[k]) * gain - embed[k].astype(F32) * factor
            ).astype(BF16)
    for one in lines:
        one.wait_recv()
    total = kept[...]
    for i in range(3):
        total = total + line[i].astype(F32)
    sums[...] = total
    net.finish()


def shards(
    embed, gain, w_zero, w_one, w_two, rot_table, face_atoms, edge_source, edge_target,
    rot_index, edge_weight, cotangent,
):
    atoms = embed.shape[2]
    local = embed.shape[1]
    edges = edge_source.shape[0]
    row = lambda a: a.reshape(1, edges)
    column = lambda a: a.reshape(-1, 1)
    lost = lambda n: jnp.full((n,), -1, jnp.int32)
    face_left = column(jnp.concatenate([lost(16), face_atoms[:16], lost(96)]))
    face_right = column(jnp.concatenate([face_atoms[16:], lost(112)]))
    vmem = pl.BlockSpec(memory_space=pltpu.VMEM)
    hbm = pl.BlockSpec(memory_space=pl.ANY)
    block = (19, local, edges)
    scratch = [
        (w_zero.shape, BF16),
        (w_one.shape, BF16),
        (w_two.shape, BF16),
        ((32, 25 * local), BF16),
        ((32, 25 * local), BF16),
        ((19, 25, edges), F32),
        ((25, local, edges), F32),
        (block, BF16),
        (block, BF16),
        ((8, edges), F32),
        ((7, 8, edges), F32),
        ((19, 8, local, edges), BF16),
        ((19, 8, local, edges), BF16),
        ((19, 8, local, edges), BF16),
        ((2, 10, local, edges), BF16),
        ((2, 9, local, edges), BF16),
        ((2, 19, local, edges), BF16),
        ((2, 19, local, edges), BF16),
        (block, BF16),
        (block, BF16),
        (block, BF16),
        (block, BF16),
        ((5 * C, 2 * edges), BF16),
        ((4 * C, 4 * edges), BF16),
        ((3 * C, 4 * edges), BF16),
        ((1280, 2 * edges), BF16),
        ((1024, 4 * edges), BF16),
        ((768, 4 * edges), BF16),
        ((384, 2 * edges), BF16),
        ((512, 4 * edges), BF16),
        ((384, 4 * edges), BF16),
        ((4, 4, 640, 128), BF16),
        ((4, 320, 128), BF16),
        ((4, 320, 128), BF16),
        ((4, 640, 128), BF16),
        ((4, 640, 128), BF16),
        ((3, 640, 128), BF16),
        ((3, 640, 128), BF16),
        ((640, 128), F32),
        (block, F32),
        ((25, local, edges), BF16),
        ((8, edges), F32),
        ((7, 8, edges), F32),
        ((25, local, atoms), F32),
        ((32, 25 * local), BF16),
        ((32, 25 * local), BF16),
        ((8, 128), F32),
        ((2, 8, 128), F32),
        ((25, local, atoms), F32),
    ]
    update, grad_embed, sums = pl.pallas_call(
        layer_kernel,
        name="layer",
        out_shape=[
            jax.ShapeDtypeStruct((25, local, atoms), BF16),
            jax.ShapeDtypeStruct((25, local, atoms), BF16),
            jax.ShapeDtypeStruct((640, 128), F32),
        ],
        in_specs=[vmem] * 11 + [hbm] * 3,
        out_specs=[vmem] * 3,
        scratch_shapes=[pltpu.VMEM(s, t) for s, t in scratch]
        + [
            pltpu.SemaphoreType.DMA((COPIES,)),
            pltpu.SemaphoreType.DMA((COPIES,)),
            pltpu.SemaphoreType.DMA((3,)),
        ],
        compiler_params=pltpu.CompilerParams(
            vmem_limit_bytes=VMEM_LIMIT, collective_id=0, has_side_effects=True
        ),
    )(
        embed, cotangent, gain.T, rot_table, column(face_atoms), face_left, face_right,
        row(edge_source), row(edge_target), row(rot_index), row(edge_weight),
        w_zero, w_one, w_two,
    )

    def owned(first, rows, tiles, width):
        piece = sums[first : first + rows * tiles].reshape(tiles, rows, 128)
        return piece.transpose(0, 2, 1).reshape(tiles * 128, rows)[:width]

    grad_zero = owned(0, 80, 3, 5 * local).reshape(5, local, 80)
    grad_one = owned(240, 64, 4, 8 * local).reshape(2, 4, local, 64)
    grad_two = owned(496, 48, 3, 6 * local).reshape(2, 3, local, 48)
    return (update, grad_embed, grad_zero, grad_one, grad_two)


def solution(mesh):
    torus = Mesh(mesh.devices.reshape(4, 4, 2, 4, 2), ("y", "z", "core", "x", "zh"))
    return jax.shard_map(
        shards,
        mesh=torus,
        in_specs=(
            P(None, CHAN, GRAPH),
            P(None, CHAN),
            P(None, CHAN, None),
            P(None, None, CHAN, None),
            P(None, None, CHAN, None),
            P(),
            P(GRAPH),
            P(GRAPH),
            P(GRAPH),
            P(GRAPH),
            P(GRAPH),
            P(None, CHAN, GRAPH),
        ),
        out_specs=(
            P(None, CHAN, GRAPH),
            P(None, CHAN, GRAPH),
            P(None, CHAN, GRAPH),
            P(None, None, CHAN, GRAPH),
            P(None, None, CHAN, GRAPH),
        ),
        check_vma=False,
    )
```

```python
import jax
import jax.numpy as jnp
from jax import lax
from jax.experimental import pallas as pl
from jax.experimental.pallas import tpu as pltpu
from jax.sharding import Mesh
from jax.sharding import PartitionSpec as P

C = 512
EPSILON = 1e-06
CHAN = ("x", "zh")
GRAPH = ("y", "z", "core")
DEGREE = (0, 1, 2, 3, 4, 1, 2, 3, 4, 1, 2, 3, 4, 2, 3, 4, 2, 3, 4)
ROWS = tuple(tuple(j for j in range(19) if DEGREE[j] == l) for l in range(5))
F32 = jnp.float32
BF16 = jnp.bfloat16
VMEM_LIMIT = 60 * 1024 * 1024
MESH = pl.DeviceIdType.MESH
PIECES = (slice(5, 13), slice(0, 5), slice(13, 19))
HALF = (slice(0, 10), slice(10, 19))
UNIT = (64, 80, 48)
TILES = (4, 3, 3)
SPLIT = (128, 128, 80)


def nt(left, right):
    return lax.dot_general(left, right, (((1,), (1,)), ((), ())), preferred_element_type=F32)


def tn(left, right):
    return lax.dot_general(left, right, (((0,), (0,)), ((), ())), preferred_element_type=F32)


def nn(left, right):
    return jnp.dot(left, right, preferred_element_type=F32)


def hot(index_row, rows, first=0):
    edges = index_row.shape[1]
    row = lax.broadcasted_iota(jnp.int32, (rows, edges), 0) + first
    return jnp.where(row == index_row, 1.0, 0.0).astype(BF16)


def rotate_in(rot, values, j):
    l = DEGREE[j]
    total = None
    for k in range(l * l, (l + 1) * (l + 1)):
        term = rot[k, j : j + 1, :] * values[k]
        total = term if total is None else total + term
    return total


def rotate_out(rot, values, k, l):
    total = None
    for j in ROWS[l]:
        term = rot[k, j : j + 1, :] * values[j]
        total = term if total is None else total + term
    return total


class Net:
    def __init__(self, send, recv):
        self.send, self.recv, self.started = send, recv, []

    def copy(self, source, landing, device):
        at = len(self.started)
        assert at < COPIES
        one = pltpu.make_async_remote_copy(
            src_ref=source,
            dst_ref=landing,
            send_sem=self.send.at[at],
            recv_sem=self.recv.at[at],
            device_id=device,
            device_id_type=MESH,
        )
        one.start()
        self.started.append(one)
        return one

    def finish(self):
        for one in self.started:
            one.wait_send()


COPIES = 92


def layer_kernel(
    embed, cotangent, gain, rot_table, face,
    source, target, spin, weight, w_zero_hbm, w_one_hbm, w_two_hbm,
    update, grad_embed, sum_zero, sum_one, sum_two,
    w_zero, w_one, w_two, corner, gain_t, faces, halo_t, rot, values, grads, mine, square, squares, every, twin,
    back, relay_left, relay_right, from_left, from_right, to_far, far,
    scaled, scaled_twin, flat_zero, flat_one, flat_two, sel_zero, sel_one, sel_two,
    right_zero, right_one, right_two,
    part_one, pass_left_one, pass_right_one, up_left_one, up_right_one, to_line_one, line_one,
    kept_one,
    part_zero, pass_left_zero, pass_right_zero, up_left_zero, up_right_zero, to_line_zero,
    line_zero, kept_zero,
    part_two, pass_left_two, pass_right_two, up_left_two, up_right_two, to_line_two, line_two,
    kept_two,
    mixed, message, tally, tallies, own, leaving, returned,
    tally_out, tally_in, settled, send, recv, load,
):
    x, h = lax.axis_index("x"), lax.axis_index("zh")
    y, z, core = lax.axis_index("y"), lax.axis_index("z"), lax.axis_index("core")
    xr, xl, xo = lax.rem(x + 1, 4), lax.rem(x + 3, 4), lax.rem(x + 2, 4)
    yr, yl, yo = lax.rem(y + 1, 4), lax.rem(y + 3, 4), lax.rem(y + 2, 4)
    me = y * 8 + z * 2 + core
    ahead, behind = lax.rem(me + 1, 32), lax.rem(me + 31, 32)

    def graph_at(g):
        return {"y": g // 8, "z": lax.rem(g // 2, 4), "core": lax.rem(g, 2)}

    to_xr, to_xl = {"x": xr}, {"x": xl}
    to_yr, to_yl = {"y": yr}, {"y": yl}
    to_far_half = {"zh": 1 - h}
    to_twin = {"core": 1 - core}
    to_ahead, to_behind = graph_at(ahead), graph_at(behind)
    chan_peers = [
        {"x": lax.rem(x + dx, 4), "zh": lax.rem(h + dh, 2)}
        for dx in range(4)
        for dh in range(2)
        if dx or dh
    ]
    line_peers = [None] + [{"z": lax.rem(z + o, 4)} for o in (1, 2, 3)]
    chan = x * 2 + h

    local = embed.shape[1]
    atoms = embed.shape[2]
    edges = source.shape[1]
    count = 25 * local
    net = Net(send, recv)

    loads = [
        pltpu.make_async_copy(a, b, load.at[i])
        for i, (a, b) in enumerate(
            ((w_zero_hbm, w_zero), (w_one_hbm, w_one), (w_two_hbm, w_two))
        )
    ]
    for one in loads:
        one.start()

    barrier = pltpu.get_barrier_semaphore()
    partners = chan_peers + line_peers[1:] + [to_yr, to_yl, to_ahead, to_behind]
    for device in partners:
        pl.semaphore_signal(barrier, inc=1, device_id=device, device_id_type=MESH)

    corner[...] = jnp.zeros_like(corner)
    corner[0:1, 0:32] = face[...].astype(F32)
    face_col = jnp.broadcast_to(corner[0:1, :], (128, 128)).T[0:32].astype(jnp.int32)
    face_row = lax.broadcasted_iota(jnp.int32, (32, atoms), 1)
    face_hot = jnp.where(face_row == face_col, 1.0, 0.0).astype(BF16)
    flat_embed = embed[...].reshape(count, atoms)
    faces[...] = nt(face_hot, flat_embed).astype(BF16)
    pl.semaphore_wait(barrier, len(partners))
    halo = [
        net.copy(faces.at[16:32], halo_t.at[0:16], to_ahead),
        net.copy(faces.at[0:16], halo_t.at[16:32], to_behind),
    ]

    corner[0:5, 0:local] = gain[...]
    gain_t[...] = corner[...].T
    turn = hot(spin[...], rot_table.shape[2])
    for k in range(25):
        line_k = rot_table[k]
        high = line_k.astype(BF16)
        low = (line_k - high.astype(F32)).astype(BF16)
        rot[k] = nn(high, turn) + nn(low, turn)
    total_a = jnp.zeros((1, atoms), F32)
    for k in range(25):
        one = embed[k].astype(F32)
        total_a = total_a + jnp.sum(one * one, axis=0, keepdims=True)
    here = hot(source[...], atoms)
    near = hot(source[...], 32, atoms)

    for one in halo:
        one.wait_recv()
    values[...] = (nn(flat_embed, here) + tn(halo_t[...], near)).reshape(25, local, edges)
    for j in range(19):
        l = DEGREE[j]
        mine[j] = (rotate_in(rot, values, j) * gain_t[0:local, l : l + 1]).astype(BF16)
    cross, near_r, near_l = [], [], []
    for p in range(3):
        here_at = mine.at[PIECES[p]]
        there_at = every.at[PIECES[p], x, h]
        cross.append(net.copy(here_at, there_at, to_far_half))
        near_r.append(net.copy(here_at, there_at, to_xr))
        near_l.append(net.copy(here_at, there_at, to_xl))
    total_e = jnp.zeros((1, edges), F32)
    for k in range(25):
        one = values[k]
        total_e = total_e + jnp.sum(one * one, axis=0, keepdims=True)
    square[...] = jnp.concatenate([total_e, total_a, jnp.zeros((6, edges), F32)], axis=0)
    asked = [net.copy(square, squares.at[i], d) for i, d in enumerate(chan_peers)]
    for j in range(19):
        every[j, x, h] = mine[j]

    arrive = hot(target[...], atoms)
    values[...] = nn(cotangent[...].reshape(count, atoms), arrive).reshape(25, local, edges)
    for j in range(19):
        grads[j] = (rotate_in(rot, values, j) * weight[...]).astype(BF16)

    for one in loads:
        one.wait()
    back[0:5] = tn(
        w_zero[...].reshape(5 * local, 5 * C), grads[0:5].reshape(5 * local, edges)
    ).astype(BF16).reshape(5, 4, 2, local, edges)
    for w, start, blocks in ((w_one, 5, 4), (w_two, 13, 3)):
        plus = grads[start : start + blocks].reshape(blocks * local, edges)
        minus = grads[start + blocks : start + 2 * blocks].reshape(blocks * local, edges)
        both = jnp.concatenate([plus, minus], axis=1)
        turned = jnp.concatenate([minus, -plus], axis=1)
        size = blocks * C
        out = tn(w[0].reshape(blocks * local, size), both) + tn(
            w[1].reshape(blocks * local, size), turned
        )
        back[start : start + blocks] = (
            out[:, :edges].astype(BF16).reshape(blocks, 4, 2, local, edges)
        )
        back[start + blocks : start + 2 * blocks] = (
            out[:, edges:].astype(BF16).reshape(blocks, 4, 2, local, edges)
        )

    def added(a, b):
        return (a.astype(F32) + b.astype(F32)).astype(BF16)

    half = (1 - h, h)
    steps = [[], []]

    def step(q):
        to = half[q]
        steps[q] = [
            net.copy(back.at[HALF[0], xo, to], relay_left.at[q], to_xr),
            net.copy(back.at[HALF[1], xo, to], relay_right.at[q], to_xl),
            net.copy(back.at[HALF[1], xr, to], from_left.at[q, HALF[1]], to_xr),
            net.copy(back.at[HALF[0], xl, to], from_right.at[q, HALF[0]], to_xl),
        ]

    def step_on(q):
        to = half[q]
        steps[q][0].wait_recv()
        for j in range(10):
            back[j, xr, to] = added(back[j, xr, to], relay_left[q, j])
        steps[q].append(
            net.copy(back.at[HALF[0], xr, to], from_left.at[q, HALF[0]], to_xr)
        )
        steps[q][1].wait_recv()
        for j in range(10, 19):
            back[j, xl, to] = added(back[j, xl, to], relay_right[q, j - 10])
        steps[q].append(
            net.copy(back.at[HALF[1], xl, to], from_right.at[q, HALF[1]], to_xl)
        )

    def own_sum(q, j):
        return (
            back[j, x, half[q]].astype(F32)
            + from_left[q, j].astype(F32)
            + from_right[q, j].astype(F32)
        )

    fars = []

    def send_far(i):
        for at in ((4, 3), (2, 5))[i]:
            steps[0][at].wait_recv()
        for j in range(19)[HALF[i]]:
            to_far[j] = own_sum(0, j).astype(BF16)
        fars.append(net.copy(to_far.at[HALF[i]], far.at[HALF[i]], to_far_half))

    def forward(p, x_from, h_from, device):
        block = every.at[PIECES[p], x_from, h_from]
        return net.copy(block, block, device)

    over_own, over_cross, cross_r, cross_l = {}, {}, {}, {}
    twins = [[], [], []]

    def to_twin_core(p, h_from):
        block = every.at[PIECES[p], :, h_from]
        twins[p].append(net.copy(block, twin.at[PIECES[p], :, h_from], to_twin))

    step(0)
    near_r[0].wait_recv()
    over_own[0] = forward(0, xl, h, to_xr)
    near_l[1].wait_recv()
    over_own[1] = forward(1, xr, h, to_xl)
    near_l[2].wait_recv()
    over_own[2] = forward(2, xr, h, to_xl)
    cross[0].wait_recv()
    cross_r[0] = forward(0, x, 1 - h, to_xr)
    cross_l[0] = forward(0, x, 1 - h, to_xl)
    step_on(0)
    cross[1].wait_recv()
    cross_r[1] = forward(1, x, 1 - h, to_xr)
    cross_l[1] = forward(1, x, 1 - h, to_xl)

    for one in asked:
        one.wait_recv()
    square_sum = square[...]
    for i in range(7):
        square_sum = square_sum + squares[i]
    inverse_both = lax.rsqrt(square_sum / (25 * C) + EPSILON)
    inverse, inverse_a = inverse_both[0:1, :], inverse_both[1:2, :]
    for j in range(19):
        scaled[j] = (grads[j].astype(F32) * inverse).astype(BF16)
    scaled_copy = net.copy(scaled, scaled_twin, to_twin)

    def right_side(buffer, lane):
        wide = 5 * local
        right_zero[0:wide, lane * edges : (lane + 1) * edges] = buffer[0:5].reshape(wide, edges)
        for right, start, blocks in ((right_one, 5, 4), (right_two, 13, 3)):
            rows = blocks * local
            plus = buffer[start : start + blocks].reshape(rows, edges)
            minus = buffer[start + blocks : start + 2 * blocks].reshape(rows, edges)
            at = 2 * lane * edges
            right[0:rows, at : at + edges] = plus
            right[0:rows, at + edges : at + 2 * edges] = minus
            right[rows : 2 * rows, at : at + edges] = minus
            right[rows : 2 * rows, at + edges : at + 2 * edges] = -plus

    right_zero[...] = jnp.zeros_like(right_zero)
    right_side(scaled, 0)

    cross[2].wait_recv()
    cross_r[2] = forward(2, x, 1 - h, to_xr)
    cross_l[2] = forward(2, x, 1 - h, to_xl)
    near_l[0].wait_recv()
    over_own[0].wait_recv()
    to_twin_core(0, h)
    for p in (1, 2):
        near_r[p].wait_recv()
        over_own[p].wait_recv()
        to_twin_core(p, h)
    cross_l[0].wait_recv()
    over_cross[0] = forward(0, xr, 1 - h, to_xl)
    send_far(0)
    cross_r[1].wait_recv()
    over_cross[1] = forward(1, xl, 1 - h, to_xr)
    send_far(1)
    cross_r[2].wait_recv()
    over_cross[2] = forward(2, xl, 1 - h, to_xr)
    step(1)

    flats = (flat_one, flat_zero, flat_two)
    sels = (sel_one, sel_zero, sel_two)
    rights = (right_one, right_zero, right_two)
    parts = (part_one, part_zero, part_two)
    pass_left = (pass_left_one, pass_left_zero, pass_left_two)
    pass_right = (pass_right_one, pass_right_zero, pass_right_two)
    up_left = (up_left_one, up_left_zero, up_left_two)
    up_right = (up_right_one, up_right_zero, up_right_two)
    to_line = (to_line_one, to_line_zero, to_line_two)
    line = (line_one, line_zero, line_two)
    kept = (kept_one, kept_zero, kept_two)

    def spread_flat(buffer, lane, p):
        start, blocks, runs = ((5, 4, 2), (0, 5, 1), (13, 3, 2))[p]
        for i in range(runs):
            at = (runs * lane + i) * edges
            flats[p][:, at : at + edges] = buffer[
                start + i * blocks : start + (i + 1) * blocks
            ].reshape(blocks * C, edges)

    climbs, lines = [None] * 3, []

    def halves(p):
        return slice(0, SPLIT[p]), slice(SPLIT[p], UNIT[p] * TILES[p])

    def climb(p):
        for one in twins[p]:
            one.wait_recv()
        spread_flat(twin, 1, p)
        rows, tiles = UNIT[p], TILES[p]
        for i in range(16):
            begin = pl.multiple_of((2 * i + core) * rows, 16)
            sels[p][i * rows : (i + 1) * rows, :] = flats[p][pl.ds(begin, rows), :]
        for quarter in range(4):
            out = nt(
                sels[p][quarter * 4 * rows : (quarter + 1) * 4 * rows, :], rights[p][...]
            )
            out = out.astype(BF16).reshape(4, rows, 128 * tiles)
            for tile in range(tiles):
                parts[p][quarter, :, tile * rows : (tile + 1) * rows, :] = out[
                    :, :, 128 * tile : 128 * (tile + 1)
                ]
        a, b = halves(p)
        climbs[p] = [
            net.copy(parts[p].at[yo, :, a], pass_left[p], to_yr),
            net.copy(parts[p].at[yo, :, b], pass_right[p], to_yl),
            net.copy(parts[p].at[yr, :, b], up_left[p].at[:, b], to_yr),
            net.copy(parts[p].at[yl, :, a], up_right[p].at[:, a], to_yl),
        ]

    def climb_on(p):
        a, b = halves(p)
        climbs[p][0].wait_recv()
        parts[p][yr, :, a] = added(parts[p][yr, :, a], pass_left[p][...])
        climbs[p].append(net.copy(parts[p].at[yr, :, a], up_left[p].at[:, a], to_yr))
        climbs[p][1].wait_recv()
        parts[p][yl, :, b] = added(parts[p][yl, :, b], pass_right[p][...])
        climbs[p].append(net.copy(parts[p].at[yl, :, b], up_right[p].at[:, b], to_yl))

    def climbed(p):
        for one in climbs[p][2:]:
            one.wait_recv()
        for o in (2, 3, 1, 0):
            to = lax.rem(z + o, 4)
            total = (
                parts[p][y, to].astype(F32)
                + up_left[p][to].astype(F32)
                + up_right[p][to].astype(F32)
            )
            if o:
                to_line[p][o - 1] = total.astype(BF16)
                lines.append(
                    net.copy(to_line[p].at[o - 1], line[p].at[o - 1], line_peers[o])
                )
            else:
                kept[p][...] = total

    cross_r[0].wait_recv()
    over_cross[0].wait_recv()
    to_twin_core(0, 1 - h)
    spread_flat(every, 0, 0)
    scaled_copy.wait_recv()
    right_side(scaled_twin, 1)
    cross_l[1].wait_recv()
    over_cross[1].wait_recv()
    to_twin_core(1, 1 - h)
    climb(0)
    cross_l[2].wait_recv()
    over_cross[2].wait_recv()
    to_twin_core(2, 1 - h)
    spread_flat(every, 0, 1)
    climb(1)
    step_on(1)
    spread_flat(every, 0, 2)
    climb(2)

    mixed[0:5] = nn(w_zero[...].reshape(5 * local, 5 * C), flat_zero[:, 0:edges]).reshape(
        5, local, edges
    )
    for w, flat, start, blocks in ((w_one, flat_one, 5, 4), (w_two, flat_two, 13, 3)):
        size = blocks * C
        both = flat[:, 0 : 2 * edges]
        real = nn(w[0].reshape(blocks * local, size), both)
        imag = nn(w[1].reshape(blocks * local, size), both)
        mixed[start : start + blocks] = (real[:, :edges] - imag[:, edges:]).reshape(
            blocks, local, edges
        )
        mixed[start + blocks : start + 2 * blocks] = (
            real[:, edges:] + imag[:, :edges]
        ).reshape(blocks, local, edges)
    total = jnp.zeros((1, edges), F32)
    for j in range(19):
        total = total + jnp.sum(mixed[j] * grads[j].astype(F32), axis=0, keepdims=True)
    tally[...] = jnp.broadcast_to(total, tally.shape)
    counted = [net.copy(tally, tallies.at[i], d) for i, d in enumerate(chan_peers)]

    climb_on(0)
    scale = weight[...] * inverse
    for j in range(19):
        mixed[j] = mixed[j] * scale
    for l in range(5):
        for k in range(l * l, (l + 1) * (l + 1)):
            message[k] = rotate_out(rot, mixed, k, l).astype(BF16)
    update[...] = (
        nt(message[...].reshape(count, edges), arrive).reshape(25, local, atoms).astype(BF16)
    )
    climb_on(1)
    climbed(0)
    climb_on(2)
    for one in steps[1][2:]:
        one.wait_recv()
    for j in range(19):
        mixed[j] = own_sum(1, j)

    for one in counted:
        one.wait_recv()
    tally_sum = tally[...]
    for i in range(7):
        tally_sum = tally_sum + tallies[i]
    for one in fars:
        one.wait_recv()
    for j in range(19):
        mixed[j] = mixed[j] + far[j].astype(F32)
    for l in range(5):
        for k in range(l * l, (l + 1) * (l + 1)):
            message[k] = rotate_out(rot, mixed, k, l).astype(BF16)
    flat = message[...].reshape(count, edges)
    leaving[...] = nt(near, flat).astype(BF16)

    def exact(left, right, dims):
        return lax.dot_general(
            left, right, (dims, ((), ())),
            precision=lax.Precision.HIGHEST, preferred_element_type=F32,
        )

    side = lax.broadcasted_iota(jnp.int32, (128, edges), 0)
    side = side + jnp.where(side < 16, atoms + 16, atoms - 16)
    side_hot = jnp.where(side == source[...], 1.0, 0.0)
    tally_out[...] = exact(tally_sum, side_hot, ((1,), (1,)))
    halo = [
        net.copy(leaving.at[16:32], returned.at[0:16], to_ahead),
        net.copy(leaving.at[0:16], returned.at[16:32], to_behind),
        net.copy(tally_out, tally_in.at[0], to_ahead),
        net.copy(tally_out, tally_in.at[1], to_behind),
    ]
    climbed(1)
    own[...] = nt(flat, here).reshape(25, local, atoms)
    tally_a = exact(tally_sum, here.astype(F32), ((1,), (1,)))
    climbed(2)
    for one in halo:
        one.wait_recv()
    settled[...] = tn(returned[...], face_hot).reshape(25, local, atoms)
    lane = lax.broadcasted_iota(jnp.int32, (8, 128), 1)
    tally_face = jnp.where(lane < 16, tally_in[0], tally_in[1])
    tally_a = tally_a + exact(tally_face[:, 0:32], face_hot.astype(F32), ((1,), (0,)))
    factor = inverse_a * inverse_a * inverse_a * tally_a[0:1, :] / (25 * C)
    for l in range(5):
        gain_l = gain_t[0:local, l : l + 1] * inverse_a
        for k in range(l * l, (l + 1) * (l + 1)):
            grad_embed[k] = (
                (own[k] + settled[k]) * gain_l - embed[k].astype(F32) * factor
            ).astype(BF16)
    for one in lines:
        one.wait_recv()
    for p, out, width in ((0, sum_one, 512), (1, sum_zero, 320), (2, sum_two, 384)):
        total = kept[p][...]
        for i in range(3):
            total = total + line[p][i].astype(F32)
        for tile in range(TILES[p]):
            begin, end = 128 * tile, min(128 * (tile + 1), width)
            out[:, begin:end] = total[tile * UNIT[p] : (tile + 1) * UNIT[p], 0 : end - begin]
    net.finish()


def shards(
    embed, gain, w_zero, w_one, w_two, rot_table, face_atoms, edge_source, edge_target,
    rot_index, edge_weight, cotangent,
):
    atoms = embed.shape[2]
    local = embed.shape[1]
    edges = edge_source.shape[0]
    row = lambda a: a.reshape(1, edges)
    vmem = pl.BlockSpec(memory_space=pltpu.VMEM)
    hbm = pl.BlockSpec(memory_space=pl.ANY)
    block = (19, local, edges)
    scratch = [
        (w_zero.shape, BF16),
        (w_one.shape, BF16),
        (w_two.shape, BF16),
        ((128, 128), F32),
        ((128, 128), F32),
        ((32, 25 * local), BF16),
        ((32, 25 * local), BF16),
        ((25, 19, edges), F32),
        ((25, local, edges), F32),
        (block, BF16),
        (block, BF16),
        ((8, edges), F32),
        ((7, 8, edges), F32),
        ((19, 4, 2, local, edges), BF16),
        ((19, 4, 2, local, edges), BF16),
        ((19, 4, 2, local, edges), BF16),
        ((2, 10, local, edges), BF16),
        ((2, 9, local, edges), BF16),
        ((2, 19, local, edges), BF16),
        ((2, 19, local, edges), BF16),
        (block, BF16),
        (block, BF16),
        (block, BF16),
        (block, BF16),
        ((5 * C, 2 * edges), BF16),
        ((4 * C, 4 * edges), BF16),
        ((3 * C, 4 * edges), BF16),
        ((1280, 2 * edges), BF16),
        ((1024, 4 * edges), BF16),
        ((768, 4 * edges), BF16),
        ((384, 2 * edges), BF16),
        ((512, 4 * edges), BF16),
        ((384, 4 * edges), BF16),
    ]
    for p in range(3):
        rows = UNIT[p] * TILES[p]
        scratch += [
            ((4, 4, rows, 128), BF16),
            ((4, SPLIT[p], 128), BF16),
            ((4, rows - SPLIT[p], 128), BF16),
            ((4, rows, 128), BF16),
            ((4, rows, 128), BF16),
            ((3, rows, 128), BF16),
            ((3, rows, 128), BF16),
            ((rows, 128), F32),
        ]
    scratch += [
        (block, F32),
        ((25, local, edges), BF16),
        ((8, edges), F32),
        ((7, 8, edges), F32),
        ((25, local, atoms), F32),
        ((32, 25 * local), BF16),
        ((32, 25 * local), BF16),
        ((8, 128), F32),
        ((2, 8, 128), F32),
        ((25, local, atoms), F32),
    ]
    update, grad_embed, sum_zero, sum_one, sum_two = pl.pallas_call(
        layer_kernel,
        name="layer",
        out_shape=[
            jax.ShapeDtypeStruct((25, local, atoms), BF16),
            jax.ShapeDtypeStruct((25, local, atoms), BF16),
            jax.ShapeDtypeStruct((80, 5 * local), F32),
            jax.ShapeDtypeStruct((64, 8 * local), F32),
            jax.ShapeDtypeStruct((48, 6 * local), F32),
        ],
        in_specs=[vmem] * 9 + [hbm] * 3,
        out_specs=[vmem] * 5,
        scratch_shapes=[pltpu.VMEM(s, t) for s, t in scratch]
        + [
            pltpu.SemaphoreType.DMA((COPIES,)),
            pltpu.SemaphoreType.DMA((COPIES,)),
            pltpu.SemaphoreType.DMA((3,)),
        ],
        compiler_params=pltpu.CompilerParams(
            vmem_limit_bytes=VMEM_LIMIT, collective_id=0, has_side_effects=True
        ),
    )(
        embed, cotangent, gain, rot_table.transpose(1, 0, 2), face_atoms.reshape(1, -1),
        row(edge_source), row(edge_target), row(rot_index), row(edge_weight),
        w_zero, w_one, w_two,
    )

    grad_zero = sum_zero.T.reshape(5, local, 80)
    grad_one = sum_one.T.reshape(2, 4, local, 64)
    grad_two = sum_two.T.reshape(2, 3, local, 48)
    return (update, grad_embed, grad_zero, grad_one, grad_two)


def solution(mesh):
    torus = Mesh(mesh.devices.reshape(4, 4, 2, 4, 2), ("y", "z", "core", "x", "zh"))
    return jax.shard_map(
        shards,
        mesh=torus,
        in_specs=(
            P(None, CHAN, GRAPH),
            P(None, CHAN),
            P(None, CHAN, None),
            P(None, None, CHAN, None),
            P(None, None, CHAN, None),
            P(),
            P(GRAPH),
            P(GRAPH),
            P(GRAPH),
            P(GRAPH),
            P(GRAPH),
            P(None, CHAN, GRAPH),
        ),
        out_specs=(
            P(None, CHAN, GRAPH),
            P(None, CHAN, GRAPH),
            P(None, CHAN, GRAPH),
            P(None, None, CHAN, GRAPH),
            P(None, None, CHAN, GRAPH),
        ),
        check_vma=False,
    )
```

```python
import jax
import jax.numpy as jnp
from jax import lax
from jax.experimental import pallas as pl
from jax.experimental.pallas import tpu as pltpu
from jax.sharding import Mesh
from jax.sharding import PartitionSpec as P

C = 512
EPSILON = 1e-06
CHAN = ("x", "zh")
GRAPH = ("y", "z", "core")
DEGREE = (0, 1, 2, 3, 4, 1, 2, 3, 4, 1, 2, 3, 4, 2, 3, 4, 2, 3, 4)
ROWS = tuple(tuple(j for j in range(19) if DEGREE[j] == l) for l in range(5))
F32 = jnp.float32
BF16 = jnp.bfloat16
VMEM_LIMIT = 46 * 1024 * 1024
FINISH_LIMIT = 8 * 1024 * 1024
MESH = pl.DeviceIdType.MESH
PIECES = (slice(5, 13), slice(0, 5), slice(13, 19))
HALF = (slice(0, 10), slice(10, 19))
UNIT = (64, 80, 48)
TILES = (4, 3, 3)
SPLIT = (128, 128, 80)


def nt(left, right):
    return lax.dot_general(left, right, (((1,), (1,)), ((), ())), preferred_element_type=F32)


def tn(left, right):
    return lax.dot_general(left, right, (((0,), (0,)), ((), ())), preferred_element_type=F32)


def nn(left, right):
    return jnp.dot(left, right, preferred_element_type=F32)


def hot(index_row, rows, first=0):
    edges = index_row.shape[1]
    row = lax.broadcasted_iota(jnp.int32, (rows, edges), 0) + first
    return jnp.where(row == index_row, 1.0, 0.0).astype(BF16)


def rotate_in(rot, values, j):
    l = DEGREE[j]
    total = None
    for k in range(l * l, (l + 1) * (l + 1)):
        term = rot[k, j : j + 1, :] * values[k]
        total = term if total is None else total + term
    return total


def rotate_out(rot, values, k, l):
    total = None
    for j in ROWS[l]:
        term = rot[k, j : j + 1, :] * values[j]
        total = term if total is None else total + term
    return total


class Net:
    def __init__(self, send, recv):
        self.send, self.recv, self.started = send, recv, []

    def copy(self, source, landing, device):
        at = len(self.started)
        assert at < COPIES
        one = pltpu.make_async_remote_copy(
            src_ref=source,
            dst_ref=landing,
            send_sem=self.send.at[at],
            recv_sem=self.recv.at[at],
            device_id=device,
            device_id_type=MESH,
        )
        one.start()
        self.started.append(one)
        return one

    def finish(self):
        for one in self.started:
            one.wait_send()


COPIES = 92


def layer_kernel(
    embed_hbm, cotangent_hbm, gain_hbm, rot_table_hbm, face_hbm,
    source_hbm, target_hbm, spin_hbm, weight_hbm, w_zero_hbm, w_one_hbm, w_two_hbm,
    update, grad_embed, sum_zero, sum_one, sum_two,
    embed, cotangent, gain, rot_table, face, source, target, spin, weight,
    w_zero, w_one, w_two, corner, gain_t, faces, halo_t, rot, values, grads, mine, square, squares, every, twin,
    back, relay_left, relay_right, from_left, from_right, to_far, far,
    scaled, scaled_twin, flat_zero, flat_one, flat_two, sel_zero, sel_one, sel_two,
    right_zero, right_one, right_two,
    part_one, pass_left_one, pass_right_one, up_left_one, up_right_one, to_line_one, line_one,
    kept_one,
    part_zero, pass_left_zero, pass_right_zero, up_left_zero, up_right_zero, to_line_zero,
    line_zero, kept_zero,
    part_two, pass_left_two, pass_right_two, up_left_two, up_right_two, to_line_two, line_two,
    kept_two,
    mixed, message, tally, tallies, own, leaving, returned,
    tally_out, tally_in, settled, send, recv, load,
):
    x, h = lax.axis_index("x"), lax.axis_index("zh")
    y, z, core = lax.axis_index("y"), lax.axis_index("z"), lax.axis_index("core")
    xr, xl, xo = lax.rem(x + 1, 4), lax.rem(x + 3, 4), lax.rem(x + 2, 4)
    yr, yl, yo = lax.rem(y + 1, 4), lax.rem(y + 3, 4), lax.rem(y + 2, 4)
    me = y * 8 + z * 2 + core
    ahead, behind = lax.rem(me + 1, 32), lax.rem(me + 31, 32)

    def graph_at(g):
        return {"y": g // 8, "z": lax.rem(g // 2, 4), "core": lax.rem(g, 2)}

    to_xr, to_xl = {"x": xr}, {"x": xl}
    to_yr, to_yl = {"y": yr}, {"y": yl}
    to_far_half = {"zh": 1 - h}
    to_twin = {"core": 1 - core}
    to_ahead, to_behind = graph_at(ahead), graph_at(behind)
    chan_peers = [
        {"x": lax.rem(x + dx, 4), "zh": lax.rem(h + dh, 2)}
        for dx in range(4)
        for dh in range(2)
        if dx or dh
    ]
    line_peers = [None] + [{"z": lax.rem(z + o, 4)} for o in (1, 2, 3)]
    chan = x * 2 + h

    local = embed.shape[1]
    atoms = embed.shape[2]
    edges = source.shape[1]
    count = 25 * local
    net = Net(send, recv)

    loads = [
        pltpu.make_async_copy(a, b, load.at[i])
        for i, (a, b) in enumerate(
            (
                (embed_hbm, embed),
                (face_hbm, face),
                (rot_table_hbm, rot_table),
                (gain_hbm, gain),
                (source_hbm, source),
                (target_hbm, target),
                (spin_hbm, spin),
                (weight_hbm, weight),
                (cotangent_hbm, cotangent),
                (w_zero_hbm, w_zero),
                (w_one_hbm, w_one),
                (w_two_hbm, w_two),
            )
        )
    ]
    for one in loads:
        one.start()

    barrier = pltpu.get_barrier_semaphore()
    partners = chan_peers + line_peers[1:] + [to_yr, to_yl, to_ahead, to_behind]
    for device in partners:
        pl.semaphore_signal(barrier, inc=1, device_id=device, device_id_type=MESH)

    for one in loads[:2]:
        one.wait()
    corner[...] = jnp.zeros_like(corner)
    corner[0:1, 0:32] = face[...].astype(F32)
    face_col = jnp.broadcast_to(corner[0:1, :], (128, 128)).T[0:32].astype(jnp.int32)
    face_row = lax.broadcasted_iota(jnp.int32, (32, atoms), 1)
    face_hot = jnp.where(face_row == face_col, 1.0, 0.0).astype(BF16)
    flat_embed = embed[...].reshape(count, atoms)
    faces[...] = nt(face_hot, flat_embed).astype(BF16)
    pl.semaphore_wait(barrier, len(partners))
    halo = [
        net.copy(faces.at[16:32], halo_t.at[0:16], to_ahead),
        net.copy(faces.at[0:16], halo_t.at[16:32], to_behind),
    ]

    for one in loads[2:8]:
        one.wait()
    corner[0:5, 0:local] = gain[...]
    gain_t[...] = corner[...].T
    turn = hot(spin[...], rot_table.shape[2])
    for k in range(25):
        line_k = rot_table[k]
        high = line_k.astype(BF16)
        low = (line_k - high.astype(F32)).astype(BF16)
        rot[k] = nn(high, turn) + nn(low, turn)
    total_a = jnp.zeros((1, atoms), F32)
    for k in range(25):
        one = embed[k].astype(F32)
        total_a = total_a + jnp.sum(one * one, axis=0, keepdims=True)
    here = hot(source[...], atoms)
    near_hot = hot(source[...], 32, atoms)

    for one in halo:
        one.wait_recv()
    values[...] = (nn(flat_embed, here) + tn(halo_t[...], near_hot)).reshape(25, local, edges)
    for j in range(19):
        l = DEGREE[j]
        mine[j] = (rotate_in(rot, values, j) * gain_t[0:local, l : l + 1]).astype(BF16)
    cross, near_r, near_l = [], [], []

    def near(p):
        here_at = mine.at[PIECES[p]]
        there_at = every.at[PIECES[p], x, h]
        near_r.append(net.copy(here_at, there_at, to_xr))
        near_l.append(net.copy(here_at, there_at, to_xl))

    for p in range(3):
        cross.append(net.copy(mine.at[PIECES[p]], every.at[PIECES[p], x, h], to_far_half))
        if p == 0:
            near(0)
    total_e = jnp.zeros((1, edges), F32)
    for k in range(25):
        one = values[k]
        total_e = total_e + jnp.sum(one * one, axis=0, keepdims=True)
    square[...] = jnp.concatenate([total_e, total_a, jnp.zeros((6, edges), F32)], axis=0)
    asked = [net.copy(square, squares.at[i], d) for i, d in enumerate(chan_peers)]
    for j in range(19):
        every[j, x, h] = mine[j]

    loads[8].wait()
    arrive = hot(target[...], atoms)
    values[...] = nn(cotangent[...].reshape(count, atoms), arrive).reshape(25, local, edges)
    for j in range(19):
        grads[j] = (rotate_in(rot, values, j) * weight[...]).astype(BF16)

    for one in loads[9:]:
        one.wait()
    back[0:5] = tn(
        w_zero[...].reshape(5 * local, 5 * C), grads[0:5].reshape(5 * local, edges)
    ).astype(BF16).reshape(5, 4, 2, local, edges)
    for w, start, blocks in ((w_one, 5, 4), (w_two, 13, 3)):
        plus = grads[start : start + blocks].reshape(blocks * local, edges)
        minus = grads[start + blocks : start + 2 * blocks].reshape(blocks * local, edges)
        both = jnp.concatenate([plus, minus], axis=1)
        turned = jnp.concatenate([minus, -plus], axis=1)
        size = blocks * C
        out = tn(w[0].reshape(blocks * local, size), both) + tn(
            w[1].reshape(blocks * local, size), turned
        )
        back[start : start + blocks] = (
            out[:, :edges].astype(BF16).reshape(blocks, 4, 2, local, edges)
        )
        back[start + blocks : start + 2 * blocks] = (
            out[:, edges:].astype(BF16).reshape(blocks, 4, 2, local, edges)
        )

    def added(a, b):
        return (a.astype(F32) + b.astype(F32)).astype(BF16)

    half = (1 - h, h)
    steps = [[], []]

    def step(q):
        to = half[q]
        steps[q] = [
            net.copy(back.at[HALF[0], xo, to], relay_left.at[q], to_xr),
            net.copy(back.at[HALF[1], xo, to], relay_right.at[q], to_xl),
            net.copy(back.at[HALF[1], xr, to], from_left.at[q, HALF[1]], to_xr),
            net.copy(back.at[HALF[0], xl, to], from_right.at[q, HALF[0]], to_xl),
        ]

    def step_right(q):
        to = half[q]
        steps[q][0].wait_recv()
        for j in range(10):
            back[j, xr, to] = added(back[j, xr, to], relay_left[q, j])
        steps[q].append(
            net.copy(back.at[HALF[0], xr, to], from_left.at[q, HALF[0]], to_xr)
        )

    def step_left(q):
        to = half[q]
        steps[q][1].wait_recv()
        for j in range(10, 19):
            back[j, xl, to] = added(back[j, xl, to], relay_right[q, j - 10])
        steps[q].append(
            net.copy(back.at[HALF[1], xl, to], from_right.at[q, HALF[1]], to_xl)
        )

    def own_sum(q, j):
        return (
            back[j, x, half[q]].astype(F32)
            + from_left[q, j].astype(F32)
            + from_right[q, j].astype(F32)
        )

    fars = []

    def send_far(i):
        for at in ((4, 3), (2, 5))[i]:
            steps[0][at].wait_recv()
        for j in range(19)[HALF[i]]:
            to_far[j] = own_sum(0, j).astype(BF16)
        fars.append(net.copy(to_far.at[HALF[i]], far.at[HALF[i]], to_far_half))

    def forward(p, x_from, h_from, device):
        block = every.at[PIECES[p], x_from, h_from]
        return net.copy(block, block, device)

    over_own, over_cross, cross_r, cross_l = {}, {}, {}, {}
    twins = [[], [], []]

    def to_twin_core(p, h_from):
        block = every.at[PIECES[p], :, h_from]
        twins[p].append(net.copy(block, twin.at[PIECES[p], :, h_from], to_twin))

    flats = (flat_one, flat_zero, flat_two)
    sels = (sel_one, sel_zero, sel_two)
    rights = (right_one, right_zero, right_two)
    parts = (part_one, part_zero, part_two)
    pass_left = (pass_left_one, pass_left_zero, pass_left_two)
    pass_right = (pass_right_one, pass_right_zero, pass_right_two)
    up_left = (up_left_one, up_left_zero, up_left_two)
    up_right = (up_right_one, up_right_zero, up_right_two)
    to_line = (to_line_one, to_line_zero, to_line_two)
    line = (line_one, line_zero, line_two)
    kept = (kept_one, kept_zero, kept_two)

    def spread_flat(buffer, lane, p):
        start, blocks, runs = ((5, 4, 2), (0, 5, 1), (13, 3, 2))[p]
        for i in range(runs):
            at = (runs * lane + i) * edges
            flats[p][:, at : at + edges] = buffer[
                start + i * blocks : start + (i + 1) * blocks
            ].reshape(blocks * C, edges)

    climbs, lines = [None] * 3, []

    def halves(p):
        return slice(0, SPLIT[p]), slice(SPLIT[p], UNIT[p] * TILES[p])

    def climb(p):
        for one in twins[p]:
            one.wait_recv()
        spread_flat(twin, 1, p)
        rows, tiles = UNIT[p], TILES[p]
        for i in range(16):
            begin = pl.multiple_of((2 * i + core) * rows, 16)
            sels[p][i * rows : (i + 1) * rows, :] = flats[p][pl.ds(begin, rows), :]
        for quarter in range(4):
            out = nt(
                sels[p][quarter * 4 * rows : (quarter + 1) * 4 * rows, :], rights[p][...]
            )
            out = out.astype(BF16).reshape(4, rows, 128 * tiles)
            for tile in range(tiles):
                parts[p][quarter, :, tile * rows : (tile + 1) * rows, :] = out[
                    :, :, 128 * tile : 128 * (tile + 1)
                ]
        a, b = halves(p)
        climbs[p] = [
            net.copy(parts[p].at[yo, :, a], pass_left[p], to_yr),
            net.copy(parts[p].at[yo, :, b], pass_right[p], to_yl),
            net.copy(parts[p].at[yr, :, b], up_left[p].at[:, b], to_yr),
            net.copy(parts[p].at[yl, :, a], up_right[p].at[:, a], to_yl),
        ]

    def climb_on(p):
        a, b = halves(p)
        climbs[p][0].wait_recv()
        parts[p][yr, :, a] = added(parts[p][yr, :, a], pass_left[p][...])
        climbs[p].append(net.copy(parts[p].at[yr, :, a], up_left[p].at[:, a], to_yr))
        climbs[p][1].wait_recv()
        parts[p][yl, :, b] = added(parts[p][yl, :, b], pass_right[p][...])
        climbs[p].append(net.copy(parts[p].at[yl, :, b], up_right[p].at[:, b], to_yl))

    def climbed(p):
        for one in climbs[p][2:]:
            one.wait_recv()
        for o in (2, 3, 1, 0):
            to = lax.rem(z + o, 4)
            total = (
                parts[p][y, to].astype(F32)
                + up_left[p][to].astype(F32)
                + up_right[p][to].astype(F32)
            )
            if o:
                to_line[p][o - 1] = total.astype(BF16)
                lines.append(
                    net.copy(to_line[p].at[o - 1], line[p].at[o - 1], line_peers[o])
                )
            else:
                kept[p][...] = total

    def right_side(buffer, lane):
        wide = 5 * local
        right_zero[0:wide, lane * edges : (lane + 1) * edges] = buffer[0:5].reshape(wide, edges)
        for right, start, blocks in ((right_one, 5, 4), (right_two, 13, 3)):
            rows = blocks * local
            plus = buffer[start : start + blocks].reshape(rows, edges)
            minus = buffer[start + blocks : start + 2 * blocks].reshape(rows, edges)
            at = 2 * lane * edges
            right[0:rows, at : at + edges] = plus
            right[0:rows, at + edges : at + 2 * edges] = minus
            right[rows : 2 * rows, at : at + edges] = minus
            right[rows : 2 * rows, at + edges : at + 2 * edges] = -plus

    step(0)
    near_r[0].wait_recv()
    over_own[0] = forward(0, xl, h, to_xr)
    cross[0].wait_recv()
    cross_r[0] = forward(0, x, 1 - h, to_xr)
    cross_l[0] = forward(0, x, 1 - h, to_xl)
    step_right(0)
    cross_l[0].wait_recv()
    over_cross[0] = forward(0, xr, 1 - h, to_xl)
    step_left(0)
    near(1)
    near(2)
    near_l[0].wait_recv()
    over_own[0].wait_recv()
    to_twin_core(0, h)
    for p in (1, 2):
        cross[p].wait_recv()
        cross_r[p] = forward(p, x, 1 - h, to_xr)
        cross_l[p] = forward(p, x, 1 - h, to_xl)
    for one in asked:
        one.wait_recv()
    square_sum = square[...]
    for i in range(7):
        square_sum = square_sum + squares[i]
    inverse_both = lax.rsqrt(square_sum / (25 * C) + EPSILON)
    inverse, inverse_a = inverse_both[0:1, :], inverse_both[1:2, :]
    for j in range(19):
        scaled[j] = (grads[j].astype(F32) * inverse).astype(BF16)
    scaled_copy = net.copy(scaled, scaled_twin, to_twin)

    right_zero[...] = jnp.zeros_like(right_zero)
    right_side(scaled, 0)

    scaled_copy.wait_recv()
    right_side(scaled_twin, 1)
    cross_r[0].wait_recv()
    over_cross[0].wait_recv()
    to_twin_core(0, 1 - h)
    spread_flat(every, 0, 0)
    send_far(0)
    climb(0)
    send_far(1)
    for p in (1, 2):
        near_l[p].wait_recv()
        over_own[p] = forward(p, xr, h, to_xl)
    for p in (1, 2):
        cross_r[p].wait_recv()
        over_cross[p] = forward(p, xl, 1 - h, to_xr)
    step(1)
    climb_on(0)
    near_r[1].wait_recv()
    over_own[1].wait_recv()
    to_twin_core(1, h)
    cross_l[1].wait_recv()
    over_cross[1].wait_recv()
    to_twin_core(1, 1 - h)
    spread_flat(every, 0, 1)
    climb(1)
    near_r[2].wait_recv()
    over_own[2].wait_recv()
    to_twin_core(2, h)
    cross_l[2].wait_recv()
    over_cross[2].wait_recv()
    to_twin_core(2, 1 - h)
    spread_flat(every, 0, 2)
    climbed(0)

    mixed[0:5] = nn(w_zero[...].reshape(5 * local, 5 * C), flat_zero[:, 0:edges]).reshape(
        5, local, edges
    )
    for w, flat, start, blocks in ((w_one, flat_one, 5, 4), (w_two, flat_two, 13, 3)):
        size = blocks * C
        both = flat[:, 0 : 2 * edges]
        real = nn(w[0].reshape(blocks * local, size), both)
        imag = nn(w[1].reshape(blocks * local, size), both)
        mixed[start : start + blocks] = (real[:, :edges] - imag[:, edges:]).reshape(
            blocks, local, edges
        )
        mixed[start + blocks : start + 2 * blocks] = (
            real[:, edges:] + imag[:, :edges]
        ).reshape(blocks, local, edges)
    total = jnp.zeros((1, edges), F32)
    for j in range(19):
        total = total + jnp.sum(mixed[j] * grads[j].astype(F32), axis=0, keepdims=True)
    tally[...] = jnp.broadcast_to(total, tally.shape)
    counted = [net.copy(tally, tallies.at[i], d) for i, d in enumerate(chan_peers)]

    step_right(1)
    step_left(1)
    climb_on(1)
    climb(2)

    scale = weight[...] * inverse
    for j in range(19):
        mixed[j] = mixed[j] * scale
    for l in range(5):
        for k in range(l * l, (l + 1) * (l + 1)):
            message[k] = rotate_out(rot, mixed, k, l).astype(BF16)
    update[...] = (
        nt(message[...].reshape(count, edges), arrive).reshape(25, local, atoms).astype(BF16)
    )
    climbed(1)
    climb_on(2)
    for one in steps[1][2:]:
        one.wait_recv()
    for j in range(19):
        mixed[j] = own_sum(1, j)

    for one in counted:
        one.wait_recv()
    tally_sum = tally[...]
    for i in range(7):
        tally_sum = tally_sum + tallies[i]
    for one in fars:
        one.wait_recv()
    for j in range(19):
        mixed[j] = mixed[j] + far[j].astype(F32)
    for l in range(5):
        for k in range(l * l, (l + 1) * (l + 1)):
            message[k] = rotate_out(rot, mixed, k, l).astype(BF16)
    flat = message[...].reshape(count, edges)
    leaving[...] = nt(near_hot, flat).astype(BF16)

    def exact(left, right, dims):
        return lax.dot_general(
            left, right, (dims, ((), ())),
            precision=lax.Precision.HIGHEST, preferred_element_type=F32,
        )

    side = lax.broadcasted_iota(jnp.int32, (128, edges), 0)
    side = side + jnp.where(side < 16, atoms + 16, atoms - 16)
    side_hot = jnp.where(side == source[...], 1.0, 0.0)
    tally_out[...] = exact(tally_sum, side_hot, ((1,), (1,)))
    halo = [
        net.copy(leaving.at[16:32], returned.at[0:16], to_ahead),
        net.copy(leaving.at[0:16], returned.at[16:32], to_behind),
        net.copy(tally_out, tally_in.at[0], to_ahead),
        net.copy(tally_out, tally_in.at[1], to_behind),
    ]
    own[...] = nt(flat, here).reshape(25, local, atoms)
    tally_a = exact(tally_sum, here.astype(F32), ((1,), (1,)))
    climbed(2)
    for one in halo:
        one.wait_recv()
    settled[...] = tn(returned[...], face_hot).reshape(25, local, atoms)
    lane = lax.broadcasted_iota(jnp.int32, (8, 128), 1)
    tally_face = jnp.where(lane < 16, tally_in[0], tally_in[1])
    tally_a = tally_a + exact(tally_face[:, 0:32], face_hot.astype(F32), ((1,), (0,)))
    factor = inverse_a * inverse_a * inverse_a * tally_a[0:1, :] / (25 * C)
    for l in range(5):
        gain_l = gain_t[0:local, l : l + 1] * inverse_a
        for k in range(l * l, (l + 1) * (l + 1)):
            grad_embed[k] = (
                (own[k] + settled[k]) * gain_l - embed[k].astype(F32) * factor
            ).astype(BF16)
    for one in lines:
        one.wait_recv()
    for p, out, width in ((0, sum_one, 512), (1, sum_zero, 384), (2, sum_two, 384)):
        total = kept[p][...]
        for i in range(3):
            total = total + line[p][i].astype(F32)
        for tile in range(TILES[p]):
            begin, end = 128 * tile, min(128 * (tile + 1), width)
            out[:, begin:end] = total[tile * UNIT[p] : (tile + 1) * UNIT[p], 0 : end - begin]
    net.finish()


def finish_kernel(
    update_in, grad_in, sum_zero, sum_one, sum_two, update, grad, grad_zero, grad_one, grad_two
):
    update[...] = update_in[...]
    grad[...] = grad_in[...]
    local = grad_zero.shape[1]
    for t in range(2):
        turned = sum_zero[:, 128 * t : 128 * (t + 1)].T
        grad_zero[2 * t] = turned[:local]
        grad_zero[2 * t + 1] = turned[local:]
    grad_zero[4] = sum_zero[:, 256:384].T[:local]
    for t in range(4):
        turned = sum_one[:, 128 * t : 128 * (t + 1)].T
        for i in (0, 1):
            grad_one[(2 * t + i) // 4, (2 * t + i) % 4] = turned[i * local : (i + 1) * local]
    for i in range(6):
        grad_two[i // 3, i % 3] = sum_two[:, i * local : (i + 1) * local]


def shards(
    embed, gain, w_zero, w_one, w_two, rot_table, face_atoms, edge_source, edge_target,
    rot_index, edge_weight, cotangent,
):
    atoms = embed.shape[2]
    local = embed.shape[1]
    edges = edge_source.shape[0]
    row = lambda a: a.reshape(1, edges)
    vmem = pl.BlockSpec(memory_space=pltpu.VMEM)
    hbm = pl.BlockSpec(memory_space=pltpu.HBM)
    block = (19, local, edges)
    args = (
        embed, cotangent, gain, rot_table.transpose(1, 0, 2), face_atoms.reshape(1, -1),
        row(edge_source), row(edge_target), row(rot_index), row(edge_weight),
        w_zero, w_one, w_two,
    )
    scratch = [(a.shape, a.dtype) for a in args[:9]]
    scratch += [
        (w_zero.shape, BF16),
        (w_one.shape, BF16),
        (w_two.shape, BF16),
        ((128, 128), F32),
        ((128, 128), F32),
        ((32, 25 * local), BF16),
        ((32, 25 * local), BF16),
        ((25, 19, edges), F32),
        ((25, local, edges), F32),
        (block, BF16),
        (block, BF16),
        ((8, edges), F32),
        ((7, 8, edges), F32),
        ((19, 4, 2, local, edges), BF16),
        ((19, 4, 2, local, edges), BF16),
        ((19, 4, 2, local, edges), BF16),
        ((2, 10, local, edges), BF16),
        ((2, 9, local, edges), BF16),
        ((2, 19, local, edges), BF16),
        ((2, 19, local, edges), BF16),
        (block, BF16),
        (block, BF16),
        (block, BF16),
        (block, BF16),
        ((5 * C, 2 * edges), BF16),
        ((4 * C, 4 * edges), BF16),
        ((3 * C, 4 * edges), BF16),
        ((1280, 2 * edges), BF16),
        ((1024, 4 * edges), BF16),
        ((768, 4 * edges), BF16),
        ((384, 2 * edges), BF16),
        ((512, 4 * edges), BF16),
        ((384, 4 * edges), BF16),
    ]
    for p in range(3):
        rows = UNIT[p] * TILES[p]
        scratch += [
            ((4, 4, rows, 128), BF16),
            ((4, SPLIT[p], 128), BF16),
            ((4, rows - SPLIT[p], 128), BF16),
            ((4, rows, 128), BF16),
            ((4, rows, 128), BF16),
            ((3, rows, 128), BF16),
            ((3, rows, 128), BF16),
            ((rows, 128), F32),
        ]
    scratch += [
        (block, F32),
        ((25, local, edges), BF16),
        ((8, edges), F32),
        ((7, 8, edges), F32),
        ((25, local, atoms), F32),
        ((32, 25 * local), BF16),
        ((32, 25 * local), BF16),
        ((8, 128), F32),
        ((2, 8, 128), F32),
        ((25, local, atoms), F32),
    ]
    update, grad_embed, sum_zero, sum_one, sum_two = pl.pallas_call(
        layer_kernel,
        name="layer",
        out_shape=[
            jax.ShapeDtypeStruct((25, local, atoms), BF16),
            jax.ShapeDtypeStruct((25, local, atoms), BF16),
            jax.ShapeDtypeStruct((80, 384), F32),
            jax.ShapeDtypeStruct((64, 8 * local), F32),
            jax.ShapeDtypeStruct((48, 6 * local), F32),
        ],
        in_specs=[hbm] * 12,
        out_specs=[vmem] * 5,
        scratch_shapes=[pltpu.VMEM(s, t) for s, t in scratch]
        + [
            pltpu.SemaphoreType.DMA((COPIES,)),
            pltpu.SemaphoreType.DMA((COPIES,)),
            pltpu.SemaphoreType.DMA((12,)),
        ],
        compiler_params=pltpu.CompilerParams(
            vmem_limit_bytes=VMEM_LIMIT, collective_id=0, has_side_effects=True
        ),
    )(*(pltpu.with_memory_space_constraint(a, pltpu.HBM) for a in args))
    *outs, grad_two = pl.pallas_call(
        finish_kernel,
        name="finish",
        out_shape=[
            jax.ShapeDtypeStruct((25, local, atoms), BF16),
            jax.ShapeDtypeStruct((25, local, atoms), BF16),
            jax.ShapeDtypeStruct((5, local, 80), F32),
            jax.ShapeDtypeStruct((2, 4, local, 64), F32),
            jax.ShapeDtypeStruct((2, 3, 48, local), F32),
        ],
        in_specs=[vmem] * 5,
        out_specs=[vmem] * 5,
        compiler_params=pltpu.CompilerParams(vmem_limit_bytes=FINISH_LIMIT),
    )(update, grad_embed, sum_zero, sum_one, sum_two)
    return (*outs, grad_two.transpose(0, 1, 3, 2))


def solution(mesh):
    torus = Mesh(mesh.devices.reshape(4, 4, 2, 4, 2), ("y", "z", "core", "x", "zh"))
    return jax.shard_map(
        shards,
        mesh=torus,
        in_specs=(
            P(None, CHAN, GRAPH),
            P(None, CHAN),
            P(None, CHAN, None),
            P(None, None, CHAN, None),
            P(None, None, CHAN, None),
            P(),
            P(GRAPH),
            P(GRAPH),
            P(GRAPH),
            P(GRAPH),
            P(GRAPH),
            P(None, CHAN, GRAPH),
        ),
        out_specs=(
            P(None, CHAN, GRAPH),
            P(None, CHAN, GRAPH),
            P(None, CHAN, GRAPH),
            P(None, None, CHAN, GRAPH),
            P(None, None, CHAN, GRAPH),
        ),
        check_vma=False,
    )
```

```python
import jax
import jax.numpy as jnp
from jax import lax
from jax.experimental import pallas as pl
from jax.experimental.pallas import tpu as pltpu
from jax.sharding import Mesh
from jax.sharding import PartitionSpec as P

C = 512
EPSILON = 1e-06
CHAN = ("x", "zh")
GRAPH = ("y", "z", "core")
DEGREE = (0, 1, 2, 3, 4, 1, 2, 3, 4, 1, 2, 3, 4, 2, 3, 4, 2, 3, 4)
ROWS = tuple(tuple(j for j in range(19) if DEGREE[j] == l) for l in range(5))
F32 = jnp.float32
BF16 = jnp.bfloat16
VMEM_LIMIT = 46 * 1024 * 1024
FINISH_LIMIT = 8 * 1024 * 1024
MESH = pl.DeviceIdType.MESH
PIECES = (slice(5, 13), slice(0, 5), slice(13, 19))
HALF = (slice(0, 10), slice(10, 19))
UNIT = (64, 80, 48)
TILES = (4, 3, 3)
SPLIT = (128, 128, 80)


def nt(left, right):
    return lax.dot_general(left, right, (((1,), (1,)), ((), ())), preferred_element_type=F32)


def tn(left, right):
    return lax.dot_general(left, right, (((0,), (0,)), ((), ())), preferred_element_type=F32)


def nn(left, right):
    return jnp.dot(left, right, preferred_element_type=F32)


def hot(index_row, rows, first=0):
    edges = index_row.shape[1]
    row = lax.broadcasted_iota(jnp.int32, (rows, edges), 0) + first
    return jnp.where(row == index_row, 1.0, 0.0).astype(BF16)


def rotate_in(rot, values, j):
    l = DEGREE[j]
    total = None
    for k in range(l * l, (l + 1) * (l + 1)):
        term = rot[k, j : j + 1, :] * values[k]
        total = term if total is None else total + term
    return total


def rotate_out(rot, values, k, l):
    total = None
    for j in ROWS[l]:
        term = rot[k, j : j + 1, :] * values[j]
        total = term if total is None else total + term
    return total


class Net:
    def __init__(self, send, recv):
        self.send, self.recv, self.started = send, recv, []

    def copy(self, source, landing, device):
        at = len(self.started)
        assert at < COPIES
        one = pltpu.make_async_remote_copy(
            src_ref=source,
            dst_ref=landing,
            send_sem=self.send.at[at],
            recv_sem=self.recv.at[at],
            device_id=device,
            device_id_type=MESH,
        )
        one.start()
        self.started.append(one)
        return one

    def finish(self):
        for one in self.started:
            one.wait_send()


COPIES = 92


def layer_kernel(
    embed_hbm, cotangent_hbm, gain_hbm, rot_table_hbm, face_hbm,
    source_hbm, target_hbm, spin_hbm, weight_hbm, w_zero_hbm, w_one_hbm, w_two_hbm,
    update, grad_embed, sum_zero, sum_one, sum_two,
    embed, cotangent, gain, rot_table, face, source, target, spin, weight,
    w_zero, w_one, w_two, corner, gain_t, faces, halo_t, rot, values, grads, mine, square, squares, every, twin,
    back, relay_left, relay_right, from_left, from_right, to_far, far,
    scaled, scaled_twin, flat_zero, flat_one, flat_two, sel_zero, sel_one, sel_two,
    right_zero, right_one, right_two,
    part_one, pass_left_one, pass_right_one, up_left_one, up_right_one, to_line_one, line_one,
    kept_one,
    part_zero, pass_left_zero, pass_right_zero, up_left_zero, up_right_zero, to_line_zero,
    line_zero, kept_zero,
    part_two, pass_left_two, pass_right_two, up_left_two, up_right_two, to_line_two, line_two,
    kept_two,
    mixed, message, tally, tallies, own, leaving, returned,
    tally_out, tally_in, settled, send, recv, load,
):
    x, h = lax.axis_index("x"), lax.axis_index("zh")
    y, z, core = lax.axis_index("y"), lax.axis_index("z"), lax.axis_index("core")
    xr, xl, xo = lax.rem(x + 1, 4), lax.rem(x + 3, 4), lax.rem(x + 2, 4)
    yr, yl, yo = lax.rem(y + 1, 4), lax.rem(y + 3, 4), lax.rem(y + 2, 4)
    me = y * 8 + z * 2 + core
    ahead, behind = lax.rem(me + 1, 32), lax.rem(me + 31, 32)

    def graph_at(g):
        return {"y": g // 8, "z": lax.rem(g // 2, 4), "core": lax.rem(g, 2)}

    to_xr, to_xl = {"x": xr}, {"x": xl}
    to_yr, to_yl = {"y": yr}, {"y": yl}
    to_far_half = {"zh": 1 - h}
    to_twin = {"core": 1 - core}
    to_ahead, to_behind = graph_at(ahead), graph_at(behind)
    chan_peers = [
        {"x": lax.rem(x + dx, 4), "zh": lax.rem(h + dh, 2)}
        for dx in range(4)
        for dh in range(2)
        if dx or dh
    ]
    line_peers = [None] + [{"z": lax.rem(z + o, 4)} for o in (1, 2, 3)]
    chan = x * 2 + h

    local = embed.shape[1]
    atoms = embed.shape[2]
    edges = source.shape[1]
    count = 25 * local
    net = Net(send, recv)

    loads = [
        pltpu.make_async_copy(a, b, load.at[i])
        for i, (a, b) in enumerate(
            (
                (embed_hbm, embed),
                (face_hbm, face),
                (rot_table_hbm, rot_table),
                (gain_hbm, gain),
                (source_hbm, source),
                (target_hbm, target),
                (spin_hbm, spin),
                (weight_hbm, weight),
                (cotangent_hbm, cotangent),
                (w_zero_hbm, w_zero),
                (w_one_hbm, w_one),
                (w_two_hbm, w_two),
            )
        )
    ]
    for one in loads:
        one.start()

    barrier = pltpu.get_barrier_semaphore()
    partners = chan_peers + line_peers[1:] + [to_yr, to_yl, to_ahead, to_behind]
    for device in partners:
        pl.semaphore_signal(barrier, inc=1, device_id=device, device_id_type=MESH)

    for one in loads[:2]:
        one.wait()
    corner[...] = jnp.zeros_like(corner)
    corner[0:1, 0:32] = face[...].astype(F32)
    face_col = jnp.broadcast_to(corner[0:1, :], (128, 128)).T[0:32].astype(jnp.int32)
    face_row = lax.broadcasted_iota(jnp.int32, (32, atoms), 1)
    face_hot = jnp.where(face_row == face_col, 1.0, 0.0).astype(BF16)
    flat_embed = embed[...].reshape(count, atoms)
    faces[...] = nt(face_hot, flat_embed).astype(BF16)
    pl.semaphore_wait(barrier, len(partners))
    halo = [
        net.copy(faces.at[16:32], halo_t.at[0:16], to_ahead),
        net.copy(faces.at[0:16], halo_t.at[16:32], to_behind),
    ]

    for one in loads[2:8]:
        one.wait()
    corner[0:5, 0:local] = gain[...]
    gain_t[...] = corner[...].T
    turn = hot(spin[...], rot_table.shape[2])
    for k in range(25):
        line_k = rot_table[k]
        high = line_k.astype(BF16)
        low = (line_k - high.astype(F32)).astype(BF16)
        rot[k] = nn(high, turn) + nn(low, turn)
    total_a = jnp.zeros((1, atoms), F32)
    for k in range(25):
        one = embed[k].astype(F32)
        total_a = total_a + jnp.sum(one * one, axis=0, keepdims=True)
    here = hot(source[...], atoms)
    near_hot = hot(source[...], 32, atoms)

    loads[8].wait()
    arrive = hot(target[...], atoms)
    values[...] = nn(cotangent[...].reshape(count, atoms), arrive).reshape(25, local, edges)
    for j in range(19):
        grads[j] = (rotate_in(rot, values, j) * weight[...]).astype(BF16)

    for one in loads[9:]:
        one.wait()
    back[0:5] = tn(
        w_zero[...].reshape(5 * local, 5 * C), grads[0:5].reshape(5 * local, edges)
    ).astype(BF16).reshape(5, 4, 2, local, edges)
    for w, start, blocks in ((w_one, 5, 4), (w_two, 13, 3)):
        plus = grads[start : start + blocks].reshape(blocks * local, edges)
        minus = grads[start + blocks : start + 2 * blocks].reshape(blocks * local, edges)
        both = jnp.concatenate([plus, minus], axis=1)
        turned = jnp.concatenate([minus, -plus], axis=1)
        size = blocks * C
        out = tn(w[0].reshape(blocks * local, size), both) + tn(
            w[1].reshape(blocks * local, size), turned
        )
        back[start : start + blocks] = (
            out[:, :edges].astype(BF16).reshape(blocks, 4, 2, local, edges)
        )
        back[start + blocks : start + 2 * blocks] = (
            out[:, edges:].astype(BF16).reshape(blocks, 4, 2, local, edges)
        )

    def added(a, b):
        return (a.astype(F32) + b.astype(F32)).astype(BF16)

    half = (1 - h, h)
    steps = [[], []]

    def step_over(q):
        to = half[q]
        steps[q] = [
            net.copy(back.at[HALF[0], xo, to], relay_left.at[q], to_xr),
            net.copy(back.at[HALF[1], xo, to], relay_right.at[q], to_xl),
        ]

    def step_next(q):
        to = half[q]
        steps[q] += [
            net.copy(back.at[HALF[1], xr, to], from_left.at[q, HALF[1]], to_xr),
            net.copy(back.at[HALF[0], xl, to], from_right.at[q, HALF[0]], to_xl),
        ]

    step_over(0)
    for one in halo:
        one.wait_recv()
    values[...] = (nn(flat_embed, here) + tn(halo_t[...], near_hot)).reshape(25, local, edges)
    for j in range(19):
        l = DEGREE[j]
        mine[j] = (rotate_in(rot, values, j) * gain_t[0:local, l : l + 1]).astype(BF16)
    cross, near_r, near_l = [], [], []

    def near(p):
        here_at = mine.at[PIECES[p]]
        there_at = every.at[PIECES[p], x, h]
        near_r.append(net.copy(here_at, there_at, to_xr))
        near_l.append(net.copy(here_at, there_at, to_xl))

    for p in range(3):
        cross.append(net.copy(mine.at[PIECES[p]], every.at[PIECES[p], x, h], to_far_half))
        if p == 0:
            near(0)
    step_next(0)
    total_e = jnp.zeros((1, edges), F32)
    for k in range(25):
        one = values[k]
        total_e = total_e + jnp.sum(one * one, axis=0, keepdims=True)
    square[...] = jnp.concatenate([total_e, total_a, jnp.zeros((6, edges), F32)], axis=0)
    asked = [net.copy(square, squares.at[i], d) for i, d in enumerate(chan_peers)]
    for j in range(19):
        every[j, x, h] = mine[j]

    def step_right(q):
        to = half[q]
        steps[q][0].wait_recv()
        for j in range(10):
            back[j, xr, to] = added(back[j, xr, to], relay_left[q, j])
        steps[q].append(
            net.copy(back.at[HALF[0], xr, to], from_left.at[q, HALF[0]], to_xr)
        )

    def step_left(q):
        to = half[q]
        steps[q][1].wait_recv()
        for j in range(10, 19):
            back[j, xl, to] = added(back[j, xl, to], relay_right[q, j - 10])
        steps[q].append(
            net.copy(back.at[HALF[1], xl, to], from_right.at[q, HALF[1]], to_xl)
        )

    def own_sum(q, j):
        return (
            back[j, x, half[q]].astype(F32)
            + from_left[q, j].astype(F32)
            + from_right[q, j].astype(F32)
        )

    fars = []

    def send_far(i):
        for at in ((4, 3), (2, 5))[i]:
            steps[0][at].wait_recv()
        for j in range(19)[HALF[i]]:
            to_far[j] = own_sum(0, j).astype(BF16)
        fars.append(net.copy(to_far.at[HALF[i]], far.at[HALF[i]], to_far_half))

    def forward(p, x_from, h_from, device):
        block = every.at[PIECES[p], x_from, h_from]
        return net.copy(block, block, device)

    over_own, over_cross, cross_r, cross_l = {}, {}, {}, {}
    twins = [[], [], []]

    def to_twin_core(p, h_from):
        block = every.at[PIECES[p], :, h_from]
        twins[p].append(net.copy(block, twin.at[PIECES[p], :, h_from], to_twin))

    flats = (flat_one, flat_zero, flat_two)
    sels = (sel_one, sel_zero, sel_two)
    rights = (right_one, right_zero, right_two)
    parts = (part_one, part_zero, part_two)
    pass_left = (pass_left_one, pass_left_zero, pass_left_two)
    pass_right = (pass_right_one, pass_right_zero, pass_right_two)
    up_left = (up_left_one, up_left_zero, up_left_two)
    up_right = (up_right_one, up_right_zero, up_right_two)
    to_line = (to_line_one, to_line_zero, to_line_two)
    line = (line_one, line_zero, line_two)
    kept = (kept_one, kept_zero, kept_two)

    def spread_flat(buffer, lane, p):
        start, blocks, runs = ((5, 4, 2), (0, 5, 1), (13, 3, 2))[p]
        for i in range(runs):
            at = (runs * lane + i) * edges
            flats[p][:, at : at + edges] = buffer[
                start + i * blocks : start + (i + 1) * blocks
            ].reshape(blocks * C, edges)

    climbs, lines = [None] * 3, []

    def halves(p):
        return slice(0, SPLIT[p]), slice(SPLIT[p], UNIT[p] * TILES[p])

    def climb(p):
        for one in twins[p]:
            one.wait_recv()
        spread_flat(twin, 1, p)
        rows, tiles = UNIT[p], TILES[p]
        for i in range(16):
            begin = pl.multiple_of((2 * i + core) * rows, 16)
            sels[p][i * rows : (i + 1) * rows, :] = flats[p][pl.ds(begin, rows), :]
        for quarter in range(4):
            out = nt(
                sels[p][quarter * 4 * rows : (quarter + 1) * 4 * rows, :], rights[p][...]
            )
            out = out.astype(BF16).reshape(4, rows, 128 * tiles)
            for tile in range(tiles):
                parts[p][quarter, :, tile * rows : (tile + 1) * rows, :] = out[
                    :, :, 128 * tile : 128 * (tile + 1)
                ]
        a, b = halves(p)
        climbs[p] = [
            net.copy(parts[p].at[yo, :, a], pass_left[p], to_yr),
            net.copy(parts[p].at[yo, :, b], pass_right[p], to_yl),
            net.copy(parts[p].at[yr, :, b], up_left[p].at[:, b], to_yr),
            net.copy(parts[p].at[yl, :, a], up_right[p].at[:, a], to_yl),
        ]

    def climb_on(p):
        a, b = halves(p)
        climbs[p][0].wait_recv()
        parts[p][yr, :, a] = added(parts[p][yr, :, a], pass_left[p][...])
        climbs[p].append(net.copy(parts[p].at[yr, :, a], up_left[p].at[:, a], to_yr))
        climbs[p][1].wait_recv()
        parts[p][yl, :, b] = added(parts[p][yl, :, b], pass_right[p][...])
        climbs[p].append(net.copy(parts[p].at[yl, :, b], up_right[p].at[:, b], to_yl))

    def climbed(p):
        for one in climbs[p][2:]:
            one.wait_recv()
        for o in (2, 3, 1, 0):
            to = lax.rem(z + o, 4)
            total = (
                parts[p][y, to].astype(F32)
                + up_left[p][to].astype(F32)
                + up_right[p][to].astype(F32)
            )
            if o:
                to_line[p][o - 1] = total.astype(BF16)
                lines.append(
                    net.copy(to_line[p].at[o - 1], line[p].at[o - 1], line_peers[o])
                )
            else:
                kept[p][...] = total

    def right_side(buffer, lane):
        wide = 5 * local
        right_zero[0:wide, lane * edges : (lane + 1) * edges] = buffer[0:5].reshape(wide, edges)
        for right, start, blocks in ((right_one, 5, 4), (right_two, 13, 3)):
            rows = blocks * local
            plus = buffer[start : start + blocks].reshape(rows, edges)
            minus = buffer[start + blocks : start + 2 * blocks].reshape(rows, edges)
            at = 2 * lane * edges
            right[0:rows, at : at + edges] = plus
            right[0:rows, at + edges : at + 2 * edges] = minus
            right[rows : 2 * rows, at : at + edges] = minus
            right[rows : 2 * rows, at + edges : at + 2 * edges] = -plus

    near_r[0].wait_recv()
    over_own[0] = forward(0, xl, h, to_xr)
    cross[0].wait_recv()
    cross_r[0] = forward(0, x, 1 - h, to_xr)
    cross_l[0] = forward(0, x, 1 - h, to_xl)
    step_right(0)
    near(1)
    cross_l[0].wait_recv()
    over_cross[0] = forward(0, xr, 1 - h, to_xl)
    step_left(0)
    cross[1].wait_recv()
    cross_r[1] = forward(1, x, 1 - h, to_xr)
    cross_l[1] = forward(1, x, 1 - h, to_xl)
    near_l[1].wait_recv()
    over_own[1] = forward(1, xr, h, to_xl)
    near(2)
    near_l[0].wait_recv()
    over_own[0].wait_recv()
    to_twin_core(0, h)
    for one in asked:
        one.wait_recv()
    square_sum = square[...]
    for i in range(7):
        square_sum = square_sum + squares[i]
    inverse_both = lax.rsqrt(square_sum / (25 * C) + EPSILON)
    inverse, inverse_a = inverse_both[0:1, :], inverse_both[1:2, :]
    for j in range(19):
        scaled[j] = (grads[j].astype(F32) * inverse).astype(BF16)
    scaled_copy = net.copy(scaled, scaled_twin, to_twin)

    right_zero[...] = jnp.zeros_like(right_zero)
    right_side(scaled, 0)

    scaled_copy.wait_recv()
    right_side(scaled_twin, 1)
    cross_r[0].wait_recv()
    over_cross[0].wait_recv()
    to_twin_core(0, 1 - h)
    spread_flat(every, 0, 0)
    send_far(0)
    climb(0)
    send_far(1)
    cross_r[1].wait_recv()
    over_cross[1] = forward(1, xl, 1 - h, to_xr)
    cross[2].wait_recv()
    cross_r[2] = forward(2, x, 1 - h, to_xr)
    cross_l[2] = forward(2, x, 1 - h, to_xl)
    near_r[1].wait_recv()
    over_own[1].wait_recv()
    to_twin_core(1, h)
    cross_l[1].wait_recv()
    over_cross[1].wait_recv()
    to_twin_core(1, 1 - h)
    spread_flat(every, 0, 1)
    climb_on(0)
    near_l[2].wait_recv()
    over_own[2] = forward(2, xr, h, to_xl)
    climb(1)
    cross_r[2].wait_recv()
    over_cross[2] = forward(2, xl, 1 - h, to_xr)
    step_over(1)
    step_next(1)
    near_r[2].wait_recv()
    over_own[2].wait_recv()
    to_twin_core(2, h)
    cross_l[2].wait_recv()
    over_cross[2].wait_recv()
    to_twin_core(2, 1 - h)
    spread_flat(every, 0, 2)
    climbed(0)
    climb(2)

    mixed[0:5] = nn(w_zero[...].reshape(5 * local, 5 * C), flat_zero[:, 0:edges]).reshape(
        5, local, edges
    )
    for w, flat, start, blocks in ((w_one, flat_one, 5, 4), (w_two, flat_two, 13, 3)):
        size = blocks * C
        both = flat[:, 0 : 2 * edges]
        real = nn(w[0].reshape(blocks * local, size), both)
        imag = nn(w[1].reshape(blocks * local, size), both)
        mixed[start : start + blocks] = (real[:, :edges] - imag[:, edges:]).reshape(
            blocks, local, edges
        )
        mixed[start + blocks : start + 2 * blocks] = (
            real[:, edges:] + imag[:, :edges]
        ).reshape(blocks, local, edges)
    total = jnp.zeros((1, edges), F32)
    for j in range(19):
        total = total + jnp.sum(mixed[j] * grads[j].astype(F32), axis=0, keepdims=True)
    tally[...] = jnp.broadcast_to(total, tally.shape)
    counted = [net.copy(tally, tallies.at[i], d) for i, d in enumerate(chan_peers)]

    step_right(1)
    step_left(1)
    climb_on(1)

    scale = weight[...] * inverse
    for j in range(19):
        mixed[j] = mixed[j] * scale
    for l in range(5):
        for k in range(l * l, (l + 1) * (l + 1)):
            message[k] = rotate_out(rot, mixed, k, l).astype(BF16)
    update[...] = (
        nt(message[...].reshape(count, edges), arrive).reshape(25, local, atoms).astype(BF16)
    )
    climbed(1)
    climb_on(2)
    for one in steps[1][2:]:
        one.wait_recv()
    for j in range(19):
        mixed[j] = own_sum(1, j)

    for one in counted:
        one.wait_recv()
    tally_sum = tally[...]
    for i in range(7):
        tally_sum = tally_sum + tallies[i]
    for one in fars:
        one.wait_recv()
    for j in range(19):
        mixed[j] = mixed[j] + far[j].astype(F32)
    for l in range(5):
        for k in range(l * l, (l + 1) * (l + 1)):
            message[k] = rotate_out(rot, mixed, k, l).astype(BF16)
    flat = message[...].reshape(count, edges)
    leaving[...] = nt(near_hot, flat).astype(BF16)

    def exact(left, right, dims):
        return lax.dot_general(
            left, right, (dims, ((), ())),
            precision=lax.Precision.HIGHEST, preferred_element_type=F32,
        )

    side = lax.broadcasted_iota(jnp.int32, (128, edges), 0)
    side = side + jnp.where(side < 16, atoms + 16, atoms - 16)
    side_hot = jnp.where(side == source[...], 1.0, 0.0)
    tally_out[...] = exact(tally_sum, side_hot, ((1,), (1,)))
    halo = [
        net.copy(leaving.at[16:32], returned.at[0:16], to_ahead),
        net.copy(leaving.at[0:16], returned.at[16:32], to_behind),
        net.copy(tally_out, tally_in.at[0], to_ahead),
        net.copy(tally_out, tally_in.at[1], to_behind),
    ]
    own[...] = nt(flat, here).reshape(25, local, atoms)
    tally_a = exact(tally_sum, here.astype(F32), ((1,), (1,)))
    climbed(2)
    for one in halo:
        one.wait_recv()
    settled[...] = tn(returned[...], face_hot).reshape(25, local, atoms)
    lane = lax.broadcasted_iota(jnp.int32, (8, 128), 1)
    tally_face = jnp.where(lane < 16, tally_in[0], tally_in[1])
    tally_a = tally_a + exact(tally_face[:, 0:32], face_hot.astype(F32), ((1,), (0,)))
    factor = inverse_a * inverse_a * inverse_a * tally_a[0:1, :] / (25 * C)
    for l in range(5):
        gain_l = gain_t[0:local, l : l + 1] * inverse_a
        for k in range(l * l, (l + 1) * (l + 1)):
            grad_embed[k] = (
                (own[k] + settled[k]) * gain_l - embed[k].astype(F32) * factor
            ).astype(BF16)
    for one in lines:
        one.wait_recv()
    for p, out, width in ((0, sum_one, 512), (1, sum_zero, 384), (2, sum_two, 384)):
        total = kept[p][...]
        for i in range(3):
            total = total + line[p][i].astype(F32)
        for tile in range(TILES[p]):
            begin, end = 128 * tile, min(128 * (tile + 1), width)
            out[:, begin:end] = total[tile * UNIT[p] : (tile + 1) * UNIT[p], 0 : end - begin]
    net.finish()


def finish_kernel(
    update_in, grad_in, sum_zero, sum_one, sum_two, update, grad, grad_zero, grad_one, grad_two
):
    update[...] = update_in[...]
    grad[...] = grad_in[...]
    local = grad_zero.shape[1]
    for t in range(2):
        turned = sum_zero[:, 128 * t : 128 * (t + 1)].T
        grad_zero[2 * t] = turned[:local]
        grad_zero[2 * t + 1] = turned[local:]
    grad_zero[4] = sum_zero[:, 256:384].T[:local]
    for t in range(4):
        turned = sum_one[:, 128 * t : 128 * (t + 1)].T
        for i in (0, 1):
            grad_one[(2 * t + i) // 4, (2 * t + i) % 4] = turned[i * local : (i + 1) * local]
    for i in range(6):
        grad_two[i // 3, i % 3] = sum_two[:, i * local : (i + 1) * local]


def shards(
    embed, gain, w_zero, w_one, w_two, rot_table, face_atoms, edge_source, edge_target,
    rot_index, edge_weight, cotangent,
):
    atoms = embed.shape[2]
    local = embed.shape[1]
    edges = edge_source.shape[0]
    row = lambda a: a.reshape(1, edges)
    vmem = pl.BlockSpec(memory_space=pltpu.VMEM)
    hbm = pl.BlockSpec(memory_space=pltpu.HBM)
    block = (19, local, edges)
    args = (
        embed, cotangent, gain, rot_table.transpose(1, 0, 2), face_atoms.reshape(1, -1),
        row(edge_source), row(edge_target), row(rot_index), row(edge_weight),
        w_zero, w_one, w_two,
    )
    scratch = [(a.shape, a.dtype) for a in args[:9]]
    scratch += [
        (w_zero.shape, BF16),
        (w_one.shape, BF16),
        (w_two.shape, BF16),
        ((128, 128), F32),
        ((128, 128), F32),
        ((32, 25 * local), BF16),
        ((32, 25 * local), BF16),
        ((25, 19, edges), F32),
        ((25, local, edges), F32),
        (block, BF16),
        (block, BF16),
        ((8, edges), F32),
        ((7, 8, edges), F32),
        ((19, 4, 2, local, edges), BF16),
        ((19, 4, 2, local, edges), BF16),
        ((19, 4, 2, local, edges), BF16),
        ((2, 10, local, edges), BF16),
        ((2, 9, local, edges), BF16),
        ((2, 19, local, edges), BF16),
        ((2, 19, local, edges), BF16),
        (block, BF16),
        (block, BF16),
        (block, BF16),
        (block, BF16),
        ((5 * C, 2 * edges), BF16),
        ((4 * C, 4 * edges), BF16),
        ((3 * C, 4 * edges), BF16),
        ((1280, 2 * edges), BF16),
        ((1024, 4 * edges), BF16),
        ((768, 4 * edges), BF16),
        ((384, 2 * edges), BF16),
        ((512, 4 * edges), BF16),
        ((384, 4 * edges), BF16),
    ]
    for p in range(3):
        rows = UNIT[p] * TILES[p]
        scratch += [
            ((4, 4, rows, 128), BF16),
            ((4, SPLIT[p], 128), BF16),
            ((4, rows - SPLIT[p], 128), BF16),
            ((4, rows, 128), BF16),
            ((4, rows, 128), BF16),
            ((3, rows, 128), BF16),
            ((3, rows, 128), BF16),
            ((rows, 128), F32),
        ]
    scratch += [
        (block, F32),
        ((25, local, edges), BF16),
        ((8, edges), F32),
        ((7, 8, edges), F32),
        ((25, local, atoms), F32),
        ((32, 25 * local), BF16),
        ((32, 25 * local), BF16),
        ((8, 128), F32),
        ((2, 8, 128), F32),
        ((25, local, atoms), F32),
    ]
    update, grad_embed, sum_zero, sum_one, sum_two = pl.pallas_call(
        layer_kernel,
        name="layer",
        out_shape=[
            jax.ShapeDtypeStruct((25, local, atoms), BF16),
            jax.ShapeDtypeStruct((25, local, atoms), BF16),
            jax.ShapeDtypeStruct((80, 384), F32),
            jax.ShapeDtypeStruct((64, 8 * local), F32),
            jax.ShapeDtypeStruct((48, 6 * local), F32),
        ],
        in_specs=[hbm] * 12,
        out_specs=[vmem] * 5,
        scratch_shapes=[pltpu.VMEM(s, t) for s, t in scratch]
        + [
            pltpu.SemaphoreType.DMA((COPIES,)),
            pltpu.SemaphoreType.DMA((COPIES,)),
            pltpu.SemaphoreType.DMA((12,)),
        ],
        compiler_params=pltpu.CompilerParams(
            vmem_limit_bytes=VMEM_LIMIT, collective_id=0, has_side_effects=True
        ),
    )(*(pltpu.with_memory_space_constraint(a, pltpu.HBM) for a in args))
    *outs, grad_two = pl.pallas_call(
        finish_kernel,
        name="finish",
        out_shape=[
            jax.ShapeDtypeStruct((25, local, atoms), BF16),
            jax.ShapeDtypeStruct((25, local, atoms), BF16),
            jax.ShapeDtypeStruct((5, local, 80), F32),
            jax.ShapeDtypeStruct((2, 4, local, 64), F32),
            jax.ShapeDtypeStruct((2, 3, 48, local), F32),
        ],
        in_specs=[vmem] * 5,
        out_specs=[vmem] * 5,
        compiler_params=pltpu.CompilerParams(vmem_limit_bytes=FINISH_LIMIT),
    )(update, grad_embed, sum_zero, sum_one, sum_two)
    return (*outs, grad_two.transpose(0, 1, 3, 2))


def solution(mesh):
    torus = Mesh(mesh.devices.reshape(4, 4, 2, 4, 2), ("y", "z", "core", "x", "zh"))
    return jax.shard_map(
        shards,
        mesh=torus,
        in_specs=(
            P(None, CHAN, GRAPH),
            P(None, CHAN),
            P(None, CHAN, None),
            P(None, None, CHAN, None),
            P(None, None, CHAN, None),
            P(),
            P(GRAPH),
            P(GRAPH),
            P(GRAPH),
            P(GRAPH),
            P(GRAPH),
            P(None, CHAN, GRAPH),
        ),
        out_specs=(
            P(None, CHAN, GRAPH),
            P(None, CHAN, GRAPH),
            P(None, CHAN, GRAPH),
            P(None, None, CHAN, GRAPH),
            P(None, None, CHAN, GRAPH),
        ),
        check_vma=False,
    )
```

```python
import jax
import jax.numpy as jnp
from jax import lax
from jax.experimental import pallas as pl
from jax.experimental.pallas import tpu as pltpu
from jax.sharding import Mesh
from jax.sharding import PartitionSpec as P

C = 512
EPSILON = 1e-06
CHAN = ("x", "zh")
GRAPH = ("y", "z", "core")
DEGREE = (0, 1, 2, 3, 4, 1, 2, 3, 4, 1, 2, 3, 4, 2, 3, 4, 2, 3, 4)
ROWS = tuple(tuple(j for j in range(19) if DEGREE[j] == l) for l in range(5))
F32 = jnp.float32
BF16 = jnp.bfloat16
VMEM_LIMIT = 46 * 1024 * 1024
FINISH_LIMIT = 8 * 1024 * 1024
MESH = pl.DeviceIdType.MESH
PIECES = (slice(5, 13), slice(0, 5), slice(13, 19))
HALF = (slice(0, 10), slice(10, 19))
UNIT = (64, 80, 48)
TILES = (4, 3, 3)
SPLIT = (128, 128, 80)


def nt(left, right):
    return lax.dot_general(left, right, (((1,), (1,)), ((), ())), preferred_element_type=F32)


def tn(left, right):
    return lax.dot_general(left, right, (((0,), (0,)), ((), ())), preferred_element_type=F32)


def nn(left, right):
    return jnp.dot(left, right, preferred_element_type=F32)


def hot(index_row, rows, first=0):
    edges = index_row.shape[1]
    row = lax.broadcasted_iota(jnp.int32, (rows, edges), 0) + first
    return jnp.where(row == index_row, 1.0, 0.0).astype(BF16)


def rotate_in(rot, values, j):
    l = DEGREE[j]
    total = None
    for k in range(l * l, (l + 1) * (l + 1)):
        term = rot[k, j : j + 1, :] * values[k]
        total = term if total is None else total + term
    return total


def rotate_out(rot, values, k, l):
    total = None
    for j in ROWS[l]:
        term = rot[k, j : j + 1, :] * values[j]
        total = term if total is None else total + term
    return total


class Net:
    def __init__(self, send, recv):
        self.send, self.recv, self.started = send, recv, []

    def copy(self, source, landing, device):
        at = len(self.started)
        assert at < COPIES
        one = pltpu.make_async_remote_copy(
            src_ref=source,
            dst_ref=landing,
            send_sem=self.send.at[at],
            recv_sem=self.recv.at[at],
            device_id=device,
            device_id_type=MESH,
        )
        one.start()
        self.started.append(one)
        return one

    def finish(self):
        for one in self.started:
            one.wait_send()


COPIES = 92


def layer_kernel(
    embed_hbm, cotangent_hbm, gain_hbm, rot_table_hbm, face_hbm,
    source_hbm, target_hbm, spin_hbm, weight_hbm, w_zero_hbm, w_one_hbm, w_two_hbm,
    update, grad_embed, sum_zero, sum_one, sum_two,
    embed, cotangent, gain, rot_table, face, source, target, spin, weight,
    w_zero, w_one, w_two, corner, gain_t, faces, halo_t, rot, values, grads, mine, square, squares, every, twin,
    back, relay_left, relay_right, from_left, from_right, to_far, far,
    scaled, scaled_twin, flat_zero, flat_one, flat_two, sel_zero, sel_one, sel_two,
    right_zero, right_one, right_two,
    part_one, pass_left_one, pass_right_one, up_left_one, up_right_one, to_line_one, line_one,
    kept_one,
    part_zero, pass_left_zero, pass_right_zero, up_left_zero, up_right_zero, to_line_zero,
    line_zero, kept_zero,
    part_two, pass_left_two, pass_right_two, up_left_two, up_right_two, to_line_two, line_two,
    kept_two,
    mixed, message, tally, tallies, own, leaving, returned,
    tally_out, tally_in, settled, send, recv, load,
):
    x, h = lax.axis_index("x"), lax.axis_index("zh")
    y, z, core = lax.axis_index("y"), lax.axis_index("z"), lax.axis_index("core")
    xr, xl, xo = lax.rem(x + 1, 4), lax.rem(x + 3, 4), lax.rem(x + 2, 4)
    yr, yl, yo = lax.rem(y + 1, 4), lax.rem(y + 3, 4), lax.rem(y + 2, 4)
    me = y * 8 + z * 2 + core
    ahead, behind = lax.rem(me + 1, 32), lax.rem(me + 31, 32)

    def graph_at(g):
        return {"y": g // 8, "z": lax.rem(g // 2, 4), "core": lax.rem(g, 2)}

    to_xr, to_xl = {"x": xr}, {"x": xl}
    to_yr, to_yl = {"y": yr}, {"y": yl}
    to_far_half = {"zh": 1 - h}
    to_twin = {"core": 1 - core}
    to_ahead, to_behind = graph_at(ahead), graph_at(behind)
    chan_peers = [
        {"x": lax.rem(x + dx, 4), "zh": lax.rem(h + dh, 2)}
        for dx in range(4)
        for dh in range(2)
        if dx or dh
    ]
    line_peers = [None] + [{"z": lax.rem(z + o, 4)} for o in (1, 2, 3)]
    chan = x * 2 + h

    local = embed.shape[1]
    atoms = embed.shape[2]
    edges = source.shape[1]
    count = 25 * local
    net = Net(send, recv)

    loads = [
        pltpu.make_async_copy(a, b, load.at[i])
        for i, (a, b) in enumerate(
            (
                (embed_hbm, embed),
                (face_hbm, face),
                (rot_table_hbm, rot_table),
                (gain_hbm, gain),
                (source_hbm, source),
                (target_hbm, target),
                (spin_hbm, spin),
                (weight_hbm, weight),
                (cotangent_hbm, cotangent),
                (w_zero_hbm, w_zero),
                (w_one_hbm, w_one),
                (w_two_hbm, w_two),
            )
        )
    ]
    for one in loads:
        one.start()

    barrier = pltpu.get_barrier_semaphore()
    partners = chan_peers + line_peers[1:] + [to_yr, to_yl, to_ahead, to_behind]
    for device in partners:
        pl.semaphore_signal(barrier, inc=1, device_id=device, device_id_type=MESH)

    for one in loads[:2]:
        one.wait()
    corner[...] = jnp.zeros_like(corner)
    corner[0:1, 0:32] = face[...].astype(F32)
    face_col = jnp.broadcast_to(corner[0:1, :], (128, 128)).T[0:32].astype(jnp.int32)
    face_row = lax.broadcasted_iota(jnp.int32, (32, atoms), 1)
    face_hot = jnp.where(face_row == face_col, 1.0, 0.0).astype(BF16)
    flat_embed = embed[...].reshape(count, atoms)
    faces[...] = nt(face_hot, flat_embed).astype(BF16)
    pl.semaphore_wait(barrier, len(partners))
    halo = [
        net.copy(faces.at[16:32], halo_t.at[0:16], to_ahead),
        net.copy(faces.at[0:16], halo_t.at[16:32], to_behind),
    ]

    for one in loads[2:8]:
        one.wait()
    corner[0:5, 0:local] = gain[...]
    gain_t[...] = corner[...].T
    turn = hot(spin[...], rot_table.shape[2])
    for k in range(25):
        line_k = rot_table[k]
        high = line_k.astype(BF16)
        low = (line_k - high.astype(F32)).astype(BF16)
        rot[k] = nn(high, turn) + nn(low, turn)
    total_a = jnp.zeros((1, atoms), F32)
    for k in range(25):
        one = embed[k].astype(F32)
        total_a = total_a + jnp.sum(one * one, axis=0, keepdims=True)
    here = hot(source[...], atoms)
    near_hot = hot(source[...], 32, atoms)

    values[...] = nn(flat_embed, here).reshape(25, local, edges)
    for one in halo:
        one.wait_recv()
    values[...] += tn(halo_t[...], near_hot).reshape(25, local, edges)
    cross, near_r, near_l = [], [], []

    def near(p):
        here_at = mine.at[PIECES[p]]
        there_at = every.at[PIECES[p], x, h]
        near_r.append(net.copy(here_at, there_at, to_xr))
        near_l.append(net.copy(here_at, there_at, to_xl))

    def over(p):
        cross.append(net.copy(mine.at[PIECES[p]], every.at[PIECES[p], x, h], to_far_half))

    def own_frames(p):
        for j in range(19)[PIECES[p]]:
            l = DEGREE[j]
            one = (rotate_in(rot, values, j) * gain_t[0:local, l : l + 1]).astype(BF16)
            mine[j] = one
            every[j, x, h] = one

    own_frames(0)
    over(0)
    near(0)
    own_frames(1)
    own_frames(2)
    total_e = jnp.zeros((1, edges), F32)
    for k in range(25):
        one = values[k]
        total_e = total_e + jnp.sum(one * one, axis=0, keepdims=True)
    square[...] = jnp.concatenate([total_e, total_a, jnp.zeros((6, edges), F32)], axis=0)
    asked = [net.copy(square, squares.at[i], d) for i, d in enumerate(chan_peers)]
    over(1)
    over(2)

    loads[8].wait()
    arrive = hot(target[...], atoms)
    values[...] = nn(cotangent[...].reshape(count, atoms), arrive).reshape(25, local, edges)
    for j in range(19):
        grads[j] = (rotate_in(rot, values, j) * weight[...]).astype(BF16)

    for one in loads[9:]:
        one.wait()
    back[0:5] = tn(
        w_zero[...].reshape(5 * local, 5 * C), grads[0:5].reshape(5 * local, edges)
    ).astype(BF16).reshape(5, 4, 2, local, edges)
    for w, start, blocks in ((w_one, 5, 4), (w_two, 13, 3)):
        plus = grads[start : start + blocks].reshape(blocks * local, edges)
        minus = grads[start + blocks : start + 2 * blocks].reshape(blocks * local, edges)
        both = jnp.concatenate([plus, minus], axis=1)
        turned = jnp.concatenate([minus, -plus], axis=1)
        size = blocks * C
        out = tn(w[0].reshape(blocks * local, size), both) + tn(
            w[1].reshape(blocks * local, size), turned
        )
        back[start : start + blocks] = (
            out[:, :edges].astype(BF16).reshape(blocks, 4, 2, local, edges)
        )
        back[start + blocks : start + 2 * blocks] = (
            out[:, edges:].astype(BF16).reshape(blocks, 4, 2, local, edges)
        )

    def added(a, b):
        return (a.astype(F32) + b.astype(F32)).astype(BF16)

    half = (1 - h, h)
    steps = [[], []]

    def step_over(q):
        to = half[q]
        steps[q] = [
            net.copy(back.at[HALF[0], xo, to], relay_left.at[q], to_xr),
            net.copy(back.at[HALF[1], xo, to], relay_right.at[q], to_xl),
        ]

    def step_next(q):
        to = half[q]
        steps[q] += [
            net.copy(back.at[HALF[1], xr, to], from_left.at[q, HALF[1]], to_xr),
            net.copy(back.at[HALF[0], xl, to], from_right.at[q, HALF[0]], to_xl),
        ]

    step_over(0)
    step_next(0)

    def step_right(q):
        to = half[q]
        steps[q][0].wait_recv()
        for j in range(10):
            back[j, xr, to] = added(back[j, xr, to], relay_left[q, j])
        steps[q].append(
            net.copy(back.at[HALF[0], xr, to], from_left.at[q, HALF[0]], to_xr)
        )

    def step_left(q):
        to = half[q]
        steps[q][1].wait_recv()
        for j in range(10, 19):
            back[j, xl, to] = added(back[j, xl, to], relay_right[q, j - 10])
        steps[q].append(
            net.copy(back.at[HALF[1], xl, to], from_right.at[q, HALF[1]], to_xl)
        )

    def own_sum(q, j):
        return (
            back[j, x, half[q]].astype(F32)
            + from_left[q, j].astype(F32)
            + from_right[q, j].astype(F32)
        )

    fars = []

    def send_far(i):
        for at in ((4, 3), (2, 5))[i]:
            steps[0][at].wait_recv()
        for j in range(19)[HALF[i]]:
            to_far[j] = own_sum(0, j).astype(BF16)
        fars.append(net.copy(to_far.at[HALF[i]], far.at[HALF[i]], to_far_half))

    def forward(p, x_from, h_from, device):
        block = every.at[PIECES[p], x_from, h_from]
        return net.copy(block, block, device)

    over_own, over_cross, cross_r, cross_l = {}, {}, {}, {}
    twins = [[], [], []]

    def to_twin_core(p, h_from):
        block = every.at[PIECES[p], :, h_from]
        twins[p].append(net.copy(block, twin.at[PIECES[p], :, h_from], to_twin))

    flats = (flat_one, flat_zero, flat_two)
    sels = (sel_one, sel_zero, sel_two)
    rights = (right_one, right_zero, right_two)
    parts = (part_one, part_zero, part_two)
    pass_left = (pass_left_one, pass_left_zero, pass_left_two)
    pass_right = (pass_right_one, pass_right_zero, pass_right_two)
    up_left = (up_left_one, up_left_zero, up_left_two)
    up_right = (up_right_one, up_right_zero, up_right_two)
    to_line = (to_line_one, to_line_zero, to_line_two)
    line = (line_one, line_zero, line_two)
    kept = (kept_one, kept_zero, kept_two)

    def spread_flat(buffer, lane, p):
        start, blocks, runs = ((5, 4, 2), (0, 5, 1), (13, 3, 2))[p]
        for i in range(runs):
            at = (runs * lane + i) * edges
            flats[p][:, at : at + edges] = buffer[
                start + i * blocks : start + (i + 1) * blocks
            ].reshape(blocks * C, edges)

    climbs, lines = [None] * 3, []

    def halves(p):
        return slice(0, SPLIT[p]), slice(SPLIT[p], UNIT[p] * TILES[p])

    def climb(p):
        for one in twins[p]:
            one.wait_recv()
        spread_flat(twin, 1, p)
        rows, tiles = UNIT[p], TILES[p]
        for i in range(16):
            begin = pl.multiple_of((2 * i + core) * rows, 16)
            sels[p][i * rows : (i + 1) * rows, :] = flats[p][pl.ds(begin, rows), :]
        for quarter in range(4):
            out = nt(
                sels[p][quarter * 4 * rows : (quarter + 1) * 4 * rows, :], rights[p][...]
            )
            out = out.astype(BF16).reshape(4, rows, 128 * tiles)
            for tile in range(tiles):
                parts[p][quarter, :, tile * rows : (tile + 1) * rows, :] = out[
                    :, :, 128 * tile : 128 * (tile + 1)
                ]
        a, b = halves(p)
        climbs[p] = [
            net.copy(parts[p].at[yo, :, a], pass_left[p], to_yr),
            net.copy(parts[p].at[yo, :, b], pass_right[p], to_yl),
            net.copy(parts[p].at[yr, :, b], up_left[p].at[:, b], to_yr),
            net.copy(parts[p].at[yl, :, a], up_right[p].at[:, a], to_yl),
        ]

    def climb_on(p):
        a, b = halves(p)
        climbs[p][0].wait_recv()
        parts[p][yr, :, a] = added(parts[p][yr, :, a], pass_left[p][...])
        climbs[p].append(net.copy(parts[p].at[yr, :, a], up_left[p].at[:, a], to_yr))
        climbs[p][1].wait_recv()
        parts[p][yl, :, b] = added(parts[p][yl, :, b], pass_right[p][...])
        climbs[p].append(net.copy(parts[p].at[yl, :, b], up_right[p].at[:, b], to_yl))

    def climbed(p):
        for one in climbs[p][2:]:
            one.wait_recv()
        for o in (2, 3, 1, 0):
            to = lax.rem(z + o, 4)
            total = (
                parts[p][y, to].astype(F32)
                + up_left[p][to].astype(F32)
                + up_right[p][to].astype(F32)
            )
            if o:
                to_line[p][o - 1] = total.astype(BF16)
                lines.append(
                    net.copy(to_line[p].at[o - 1], line[p].at[o - 1], line_peers[o])
                )
            else:
                kept[p][...] = total

    def right_side(buffer, lane):
        wide = 5 * local
        right_zero[0:wide, lane * edges : (lane + 1) * edges] = buffer[0:5].reshape(wide, edges)
        for right, start, blocks in ((right_one, 5, 4), (right_two, 13, 3)):
            rows = blocks * local
            plus = buffer[start : start + blocks].reshape(rows, edges)
            minus = buffer[start + blocks : start + 2 * blocks].reshape(rows, edges)
            at = 2 * lane * edges
            right[0:rows, at : at + edges] = plus
            right[0:rows, at + edges : at + 2 * edges] = minus
            right[rows : 2 * rows, at : at + edges] = minus
            right[rows : 2 * rows, at + edges : at + 2 * edges] = -plus

    near_r[0].wait_recv()
    over_own[0] = forward(0, xl, h, to_xr)
    cross[0].wait_recv()
    cross_r[0] = forward(0, x, 1 - h, to_xr)
    cross_l[0] = forward(0, x, 1 - h, to_xl)
    step_right(0)
    near(1)
    cross_l[0].wait_recv()
    over_cross[0] = forward(0, xr, 1 - h, to_xl)
    step_left(0)
    cross[1].wait_recv()
    cross_r[1] = forward(1, x, 1 - h, to_xr)
    cross_l[1] = forward(1, x, 1 - h, to_xl)
    near_l[1].wait_recv()
    over_own[1] = forward(1, xr, h, to_xl)
    near(2)
    near_l[0].wait_recv()
    over_own[0].wait_recv()
    to_twin_core(0, h)
    for one in asked:
        one.wait_recv()
    square_sum = square[...]
    for i in range(7):
        square_sum = square_sum + squares[i]
    inverse_both = lax.rsqrt(square_sum / (25 * C) + EPSILON)
    inverse, inverse_a = inverse_both[0:1, :], inverse_both[1:2, :]
    for j in range(19):
        scaled[j] = (grads[j].astype(F32) * inverse).astype(BF16)
    scaled_copy = net.copy(scaled, scaled_twin, to_twin)

    right_zero[...] = jnp.zeros_like(right_zero)
    right_side(scaled, 0)

    cross_r[0].wait_recv()
    over_cross[0].wait_recv()
    to_twin_core(0, 1 - h)
    spread_flat(every, 0, 0)
    send_far(0)
    scaled_copy.wait_recv()
    right_side(scaled_twin, 1)
    climb(0)
    send_far(1)
    cross_r[1].wait_recv()
    over_cross[1] = forward(1, xl, 1 - h, to_xr)
    cross[2].wait_recv()
    cross_r[2] = forward(2, x, 1 - h, to_xr)
    cross_l[2] = forward(2, x, 1 - h, to_xl)
    near_r[1].wait_recv()
    over_own[1].wait_recv()
    to_twin_core(1, h)
    cross_l[1].wait_recv()
    over_cross[1].wait_recv()
    to_twin_core(1, 1 - h)
    spread_flat(every, 0, 1)
    climb_on(0)
    near_l[2].wait_recv()
    over_own[2] = forward(2, xr, h, to_xl)
    climb(1)
    cross_r[2].wait_recv()
    over_cross[2] = forward(2, xl, 1 - h, to_xr)
    step_over(1)
    step_next(1)
    near_r[2].wait_recv()
    over_own[2].wait_recv()
    to_twin_core(2, h)
    cross_l[2].wait_recv()
    over_cross[2].wait_recv()
    to_twin_core(2, 1 - h)
    spread_flat(every, 0, 2)
    climb_on(1)
    step_right(1)
    step_left(1)
    climbed(0)

    mixed[0:5] = nn(w_zero[...].reshape(5 * local, 5 * C), flat_zero[:, 0:edges]).reshape(
        5, local, edges
    )
    for w, flat, start, blocks in ((w_one, flat_one, 5, 4), (w_two, flat_two, 13, 3)):
        size = blocks * C
        both = flat[:, 0 : 2 * edges]
        real = nn(w[0].reshape(blocks * local, size), both)
        imag = nn(w[1].reshape(blocks * local, size), both)
        mixed[start : start + blocks] = (real[:, :edges] - imag[:, edges:]).reshape(
            blocks, local, edges
        )
        mixed[start + blocks : start + 2 * blocks] = (
            real[:, edges:] + imag[:, :edges]
        ).reshape(blocks, local, edges)
    total = jnp.zeros((1, edges), F32)
    for j in range(19):
        total = total + jnp.sum(mixed[j] * grads[j].astype(F32), axis=0, keepdims=True)
    tally[...] = jnp.broadcast_to(total, tally.shape)
    counted = [net.copy(tally, tallies.at[i], d) for i, d in enumerate(chan_peers)]

    climb(2)

    scale = weight[...] * inverse
    for j in range(19):
        mixed[j] = mixed[j] * scale
    for l in range(5):
        for k in range(l * l, (l + 1) * (l + 1)):
            message[k] = rotate_out(rot, mixed, k, l).astype(BF16)
    update[...] = (
        nt(message[...].reshape(count, edges), arrive).reshape(25, local, atoms).astype(BF16)
    )
    climbed(1)
    climb_on(2)
    for one in steps[1][2:]:
        one.wait_recv()
    for j in range(19):
        mixed[j] = own_sum(1, j)

    for one in counted:
        one.wait_recv()
    tally_sum = tally[...]
    for i in range(7):
        tally_sum = tally_sum + tallies[i]
    for one in fars:
        one.wait_recv()
    for j in range(19):
        mixed[j] = mixed[j] + far[j].astype(F32)
    for l in range(5):
        for k in range(l * l, (l + 1) * (l + 1)):
            message[k] = rotate_out(rot, mixed, k, l).astype(BF16)
    flat = message[...].reshape(count, edges)
    leaving[...] = nt(near_hot, flat).astype(BF16)

    def exact(left, right, dims):
        return lax.dot_general(
            left, right, (dims, ((), ())),
            precision=lax.Precision.HIGHEST, preferred_element_type=F32,
        )

    side = lax.broadcasted_iota(jnp.int32, (128, edges), 0)
    side = side + jnp.where(side < 16, atoms + 16, atoms - 16)
    side_hot = jnp.where(side == source[...], 1.0, 0.0)
    tally_out[...] = exact(tally_sum, side_hot, ((1,), (1,)))
    halo = [
        net.copy(leaving.at[16:32], returned.at[0:16], to_ahead),
        net.copy(leaving.at[0:16], returned.at[16:32], to_behind),
        net.copy(tally_out, tally_in.at[0], to_ahead),
        net.copy(tally_out, tally_in.at[1], to_behind),
    ]
    own[...] = nt(flat, here).reshape(25, local, atoms)
    tally_a = exact(tally_sum, here.astype(F32), ((1,), (1,)))
    climbed(2)
    for one in halo:
        one.wait_recv()
    settled[...] = tn(returned[...], face_hot).reshape(25, local, atoms)
    lane = lax.broadcasted_iota(jnp.int32, (8, 128), 1)
    tally_face = jnp.where(lane < 16, tally_in[0], tally_in[1])
    tally_a = tally_a + exact(tally_face[:, 0:32], face_hot.astype(F32), ((1,), (0,)))
    factor = inverse_a * inverse_a * inverse_a * tally_a[0:1, :] / (25 * C)
    for l in range(5):
        gain_l = gain_t[0:local, l : l + 1] * inverse_a
        for k in range(l * l, (l + 1) * (l + 1)):
            grad_embed[k] = (
                (own[k] + settled[k]) * gain_l - embed[k].astype(F32) * factor
            ).astype(BF16)
    for one in lines:
        one.wait_recv()
    for p, out, width in ((0, sum_one, 512), (1, sum_zero, 384), (2, sum_two, 384)):
        total = kept[p][...]
        for i in range(3):
            total = total + line[p][i].astype(F32)
        for tile in range(TILES[p]):
            begin, end = 128 * tile, min(128 * (tile + 1), width)
            out[:, begin:end] = total[tile * UNIT[p] : (tile + 1) * UNIT[p], 0 : end - begin]
    net.finish()


def finish_kernel(
    update_in, grad_in, sum_zero, sum_one, sum_two, update, grad, grad_zero, grad_one, grad_two
):
    update[...] = update_in[...]
    grad[...] = grad_in[...]
    local = grad_zero.shape[1]
    for t in range(2):
        turned = sum_zero[:, 128 * t : 128 * (t + 1)].T
        grad_zero[2 * t] = turned[:local]
        grad_zero[2 * t + 1] = turned[local:]
    grad_zero[4] = sum_zero[:, 256:384].T[:local]
    for t in range(4):
        turned = sum_one[:, 128 * t : 128 * (t + 1)].T
        for i in (0, 1):
            grad_one[(2 * t + i) // 4, (2 * t + i) % 4] = turned[i * local : (i + 1) * local]
    for i in range(6):
        grad_two[i // 3, i % 3] = sum_two[:, i * local : (i + 1) * local]


def shards(
    embed, gain, w_zero, w_one, w_two, rot_table, face_atoms, edge_source, edge_target,
    rot_index, edge_weight, cotangent,
):
    atoms = embed.shape[2]
    local = embed.shape[1]
    edges = edge_source.shape[0]
    row = lambda a: a.reshape(1, edges)
    vmem = pl.BlockSpec(memory_space=pltpu.VMEM)
    hbm = pl.BlockSpec(memory_space=pltpu.HBM)
    block = (19, local, edges)
    args = (
        embed, cotangent, gain, rot_table.transpose(1, 0, 2), face_atoms.reshape(1, -1),
        row(edge_source), row(edge_target), row(rot_index), row(edge_weight),
        w_zero, w_one, w_two,
    )
    scratch = [(a.shape, a.dtype) for a in args[:9]]
    scratch += [
        (w_zero.shape, BF16),
        (w_one.shape, BF16),
        (w_two.shape, BF16),
        ((128, 128), F32),
        ((128, 128), F32),
        ((32, 25 * local), BF16),
        ((32, 25 * local), BF16),
        ((25, 19, edges), F32),
        ((25, local, edges), F32),
        (block, BF16),
        (block, BF16),
        ((8, edges), F32),
        ((7, 8, edges), F32),
        ((19, 4, 2, local, edges), BF16),
        ((19, 4, 2, local, edges), BF16),
        ((19, 4, 2, local, edges), BF16),
        ((2, 10, local, edges), BF16),
        ((2, 9, local, edges), BF16),
        ((2, 19, local, edges), BF16),
        ((2, 19, local, edges), BF16),
        (block, BF16),
        (block, BF16),
        (block, BF16),
        (block, BF16),
        ((5 * C, 2 * edges), BF16),
        ((4 * C, 4 * edges), BF16),
        ((3 * C, 4 * edges), BF16),
        ((1280, 2 * edges), BF16),
        ((1024, 4 * edges), BF16),
        ((768, 4 * edges), BF16),
        ((384, 2 * edges), BF16),
        ((512, 4 * edges), BF16),
        ((384, 4 * edges), BF16),
    ]
    for p in range(3):
        rows = UNIT[p] * TILES[p]
        scratch += [
            ((4, 4, rows, 128), BF16),
            ((4, SPLIT[p], 128), BF16),
            ((4, rows - SPLIT[p], 128), BF16),
            ((4, rows, 128), BF16),
            ((4, rows, 128), BF16),
            ((3, rows, 128), BF16),
            ((3, rows, 128), BF16),
            ((rows, 128), F32),
        ]
    scratch += [
        (block, F32),
        ((25, local, edges), BF16),
        ((8, edges), F32),
        ((7, 8, edges), F32),
        ((25, local, atoms), F32),
        ((32, 25 * local), BF16),
        ((32, 25 * local), BF16),
        ((8, 128), F32),
        ((2, 8, 128), F32),
        ((25, local, atoms), F32),
    ]
    update, grad_embed, sum_zero, sum_one, sum_two = pl.pallas_call(
        layer_kernel,
        name="layer",
        out_shape=[
            jax.ShapeDtypeStruct((25, local, atoms), BF16),
            jax.ShapeDtypeStruct((25, local, atoms), BF16),
            jax.ShapeDtypeStruct((80, 384), F32),
            jax.ShapeDtypeStruct((64, 8 * local), F32),
            jax.ShapeDtypeStruct((48, 6 * local), F32),
        ],
        in_specs=[hbm] * 12,
        out_specs=[vmem] * 5,
        scratch_shapes=[pltpu.VMEM(s, t) for s, t in scratch]
        + [
            pltpu.SemaphoreType.DMA((COPIES,)),
            pltpu.SemaphoreType.DMA((COPIES,)),
            pltpu.SemaphoreType.DMA((12,)),
        ],
        compiler_params=pltpu.CompilerParams(
            vmem_limit_bytes=VMEM_LIMIT, collective_id=0, has_side_effects=True
        ),
    )(*(pltpu.with_memory_space_constraint(a, pltpu.HBM) for a in args))
    *outs, grad_two = pl.pallas_call(
        finish_kernel,
        name="finish",
        out_shape=[
            jax.ShapeDtypeStruct((25, local, atoms), BF16),
            jax.ShapeDtypeStruct((25, local, atoms), BF16),
            jax.ShapeDtypeStruct((5, local, 80), F32),
            jax.ShapeDtypeStruct((2, 4, local, 64), F32),
            jax.ShapeDtypeStruct((2, 3, 48, local), F32),
        ],
        in_specs=[vmem] * 5,
        out_specs=[vmem] * 5,
        compiler_params=pltpu.CompilerParams(vmem_limit_bytes=FINISH_LIMIT),
    )(update, grad_embed, sum_zero, sum_one, sum_two)
    return (*outs, grad_two.transpose(0, 1, 3, 2))


def solution(mesh):
    torus = Mesh(mesh.devices.reshape(4, 4, 2, 4, 2), ("y", "z", "core", "x", "zh"))
    return jax.shard_map(
        shards,
        mesh=torus,
        in_specs=(
            P(None, CHAN, GRAPH),
            P(None, CHAN),
            P(None, CHAN, None),
            P(None, None, CHAN, None),
            P(None, None, CHAN, None),
            P(),
            P(GRAPH),
            P(GRAPH),
            P(GRAPH),
            P(GRAPH),
            P(GRAPH),
            P(None, CHAN, GRAPH),
        ),
        out_specs=(
            P(None, CHAN, GRAPH),
            P(None, CHAN, GRAPH),
            P(None, CHAN, GRAPH),
            P(None, None, CHAN, GRAPH),
            P(None, None, CHAN, GRAPH),
        ),
        check_vma=False,
    )
```

```python
import jax
import jax.numpy as jnp
from jax import lax
from jax.experimental import pallas as pl
from jax.experimental.pallas import tpu as pltpu
from jax.sharding import Mesh
from jax.sharding import PartitionSpec as P

C = 512
EPSILON = 1e-06
CHAN = ("x", "zh")
GRAPH = ("y", "z", "core")
DEGREE = (0, 1, 2, 3, 4, 1, 2, 3, 4, 1, 2, 3, 4, 2, 3, 4, 2, 3, 4)
ROWS = tuple(tuple(j for j in range(19) if DEGREE[j] == l) for l in range(5))
F32 = jnp.float32
BF16 = jnp.bfloat16
VMEM_LIMIT = 46 * 1024 * 1024
FINISH_LIMIT = 8 * 1024 * 1024
MESH = pl.DeviceIdType.MESH
PIECES = (slice(5, 13), slice(0, 5), slice(13, 19))
HALF = (slice(0, 10), slice(10, 19))
UNIT = (64, 80, 48)
TILES = (4, 3, 3)
SPLIT = (128, 128, 80)


def nt(left, right):
    return lax.dot_general(left, right, (((1,), (1,)), ((), ())), preferred_element_type=F32)


def tn(left, right):
    return lax.dot_general(left, right, (((0,), (0,)), ((), ())), preferred_element_type=F32)


def nn(left, right):
    return jnp.dot(left, right, preferred_element_type=F32)


def hot(index_row, rows, first=0):
    edges = index_row.shape[1]
    row = lax.broadcasted_iota(jnp.int32, (rows, edges), 0) + first
    return jnp.where(row == index_row, 1.0, 0.0).astype(BF16)


def rotate_in(rot, values, j):
    l = DEGREE[j]
    total = None
    for k in range(l * l, (l + 1) * (l + 1)):
        term = rot[k, j : j + 1, :] * values[k]
        total = term if total is None else total + term
    return total


def rotate_out(rot, values, k, l):
    total = None
    for j in ROWS[l]:
        term = rot[k, j : j + 1, :] * values[j]
        total = term if total is None else total + term
    return total


class Net:
    def __init__(self, send, recv):
        self.send, self.recv, self.started = send, recv, []

    def copy(self, source, landing, device):
        at = len(self.started)
        assert at < COPIES
        one = pltpu.make_async_remote_copy(
            src_ref=source,
            dst_ref=landing,
            send_sem=self.send.at[at],
            recv_sem=self.recv.at[at],
            device_id=device,
            device_id_type=MESH,
        )
        one.start()
        self.started.append(one)
        return one

    def finish(self):
        for one in self.started:
            one.wait_send()


COPIES = 92


def layer_kernel(
    embed_hbm, cotangent_hbm, gain_hbm, rot_table_hbm, face_hbm,
    source_hbm, target_hbm, spin_hbm, weight_hbm, w_zero_hbm, w_one_hbm, w_two_hbm,
    update, grad_embed, sum_zero, sum_one, sum_two,
    embed, cotangent, gain, rot_table, face, source, target, spin, weight,
    w_zero, w_one, w_two, corner, gain_t, faces, halo_t, rot, values, grads, mine, square, squares, every, twin,
    back, relay_left, relay_right, from_left, from_right, to_far, far,
    scaled, scaled_twin, flat_zero, flat_one, flat_two, sel_zero, sel_one, sel_two,
    right_zero, right_one, right_two,
    part_one, pass_left_one, pass_right_one, up_left_one, up_right_one, to_line_one, line_one,
    kept_one,
    part_zero, pass_left_zero, pass_right_zero, up_left_zero, up_right_zero, to_line_zero,
    line_zero, kept_zero,
    part_two, pass_left_two, pass_right_two, up_left_two, up_right_two, to_line_two, line_two,
    kept_two,
    mixed, message, tally, tallies, own, leaving, returned,
    tally_out, tally_in, settled, send, recv, load,
):
    x, h = lax.axis_index("x"), lax.axis_index("zh")
    y, z, core = lax.axis_index("y"), lax.axis_index("z"), lax.axis_index("core")
    xr, xl, xo = lax.rem(x + 1, 4), lax.rem(x + 3, 4), lax.rem(x + 2, 4)
    yr, yl, yo = lax.rem(y + 1, 4), lax.rem(y + 3, 4), lax.rem(y + 2, 4)
    me = y * 8 + z * 2 + core
    ahead, behind = lax.rem(me + 1, 32), lax.rem(me + 31, 32)

    def graph_at(g):
        return {"y": g // 8, "z": lax.rem(g // 2, 4), "core": lax.rem(g, 2)}

    to_xr, to_xl = {"x": xr}, {"x": xl}
    to_yr, to_yl = {"y": yr}, {"y": yl}
    to_far_half = {"zh": 1 - h}
    to_twin = {"core": 1 - core}
    to_ahead, to_behind = graph_at(ahead), graph_at(behind)
    chan_peers = [
        {"x": lax.rem(x + dx, 4), "zh": lax.rem(h + dh, 2)}
        for dx in range(4)
        for dh in range(2)
        if dx or dh
    ]
    line_peers = [None] + [{"z": lax.rem(z + o, 4)} for o in (1, 2, 3)]
    chan = x * 2 + h

    local = embed.shape[1]
    atoms = embed.shape[2]
    edges = source.shape[1]
    count = 25 * local
    net = Net(send, recv)

    loads = [
        pltpu.make_async_copy(a, b, load.at[i])
        for i, (a, b) in enumerate(
            (
                (embed_hbm, embed),
                (face_hbm, face),
                (rot_table_hbm, rot_table),
                (gain_hbm, gain),
                (source_hbm, source),
                (target_hbm, target),
                (spin_hbm, spin),
                (weight_hbm, weight),
                (cotangent_hbm, cotangent),
                (w_zero_hbm, w_zero),
                (w_one_hbm, w_one),
                (w_two_hbm, w_two),
            )
        )
    ]
    for one in loads:
        one.start()

    barrier = pltpu.get_barrier_semaphore()
    partners = chan_peers + line_peers[1:] + [to_yr, to_yl, to_ahead, to_behind]
    for device in partners:
        pl.semaphore_signal(barrier, inc=1, device_id=device, device_id_type=MESH)

    for one in loads[:2]:
        one.wait()
    corner[...] = jnp.zeros_like(corner)
    corner[0:1, 0:32] = face[...].astype(F32)
    face_col = jnp.broadcast_to(corner[0:1, :], (128, 128)).T[0:32].astype(jnp.int32)
    face_row = lax.broadcasted_iota(jnp.int32, (32, atoms), 1)
    face_hot = jnp.where(face_row == face_col, 1.0, 0.0).astype(BF16)
    flat_embed = embed[...].reshape(count, atoms)
    faces[...] = nt(face_hot, flat_embed).astype(BF16)
    pl.semaphore_wait(barrier, len(partners))
    halo = [
        net.copy(faces.at[16:32], halo_t.at[0:16], to_ahead),
        net.copy(faces.at[0:16], halo_t.at[16:32], to_behind),
    ]

    for one in loads[2:8]:
        one.wait()
    corner[0:5, 0:local] = gain[...]
    gain_t[...] = corner[...].T
    turn = hot(spin[...], rot_table.shape[2])
    for k in range(25):
        line_k = rot_table[k]
        high = line_k.astype(BF16)
        low = (line_k - high.astype(F32)).astype(BF16)
        rot[k] = nn(high, turn) + nn(low, turn)
    total_a = jnp.zeros((1, atoms), F32)
    for k in range(25):
        one = embed[k].astype(F32)
        total_a = total_a + jnp.sum(one * one, axis=0, keepdims=True)
    here = hot(source[...], atoms)
    near_hot = hot(source[...], 32, atoms)

    values[...] = nn(flat_embed, here).reshape(25, local, edges)
    for one in halo:
        one.wait_recv()
    values[...] += tn(halo_t[...], near_hot).reshape(25, local, edges)
    cross, near_r, near_l = [], [], []

    def near(p):
        here_at = mine.at[PIECES[p]]
        there_at = every.at[PIECES[p], x, h]
        near_r.append(net.copy(here_at, there_at, to_xr))
        near_l.append(net.copy(here_at, there_at, to_xl))

    def over(p):
        cross.append(net.copy(mine.at[PIECES[p]], every.at[PIECES[p], x, h], to_far_half))

    def own_frames(p):
        for j in range(19)[PIECES[p]]:
            l = DEGREE[j]
            one = (rotate_in(rot, values, j) * gain_t[0:local, l : l + 1]).astype(BF16)
            mine[j] = one
            every[j, x, h] = one

    own_frames(0)
    over(0)
    near(0)
    own_frames(1)
    own_frames(2)
    total_e = jnp.zeros((1, edges), F32)
    for k in range(25):
        one = values[k]
        total_e = total_e + jnp.sum(one * one, axis=0, keepdims=True)
    square[...] = jnp.concatenate([total_e, total_a, jnp.zeros((6, edges), F32)], axis=0)
    asked = [net.copy(square, squares.at[i], d) for i, d in enumerate(chan_peers)]
    over(1)
    over(2)

    loads[8].wait()
    arrive = hot(target[...], atoms)
    values[...] = nn(cotangent[...].reshape(count, atoms), arrive).reshape(25, local, edges)
    for j in range(19):
        grads[j] = (rotate_in(rot, values, j) * weight[...]).astype(BF16)

    for one in loads[9:]:
        one.wait()
    back[0:5] = tn(
        w_zero[...].reshape(5 * local, 5 * C), grads[0:5].reshape(5 * local, edges)
    ).astype(BF16).reshape(5, 4, 2, local, edges)
    for w, start, blocks in ((w_one, 5, 4), (w_two, 13, 3)):
        plus = grads[start : start + blocks].reshape(blocks * local, edges)
        minus = grads[start + blocks : start + 2 * blocks].reshape(blocks * local, edges)
        both = jnp.concatenate([plus, minus], axis=1)
        turned = jnp.concatenate([minus, -plus], axis=1)
        size = blocks * C
        out = tn(w[0].reshape(blocks * local, size), both) + tn(
            w[1].reshape(blocks * local, size), turned
        )
        back[start : start + blocks] = (
            out[:, :edges].astype(BF16).reshape(blocks, 4, 2, local, edges)
        )
        back[start + blocks : start + 2 * blocks] = (
            out[:, edges:].astype(BF16).reshape(blocks, 4, 2, local, edges)
        )

    def added(a, b):
        return (a.astype(F32) + b.astype(F32)).astype(BF16)

    half = (1 - h, h)
    steps = [[], []]

    def step_over(q):
        to = half[q]
        steps[q] = [
            net.copy(back.at[HALF[0], xo, to], relay_left.at[q], to_xr),
            net.copy(back.at[HALF[1], xo, to], relay_right.at[q], to_xl),
        ]

    def step_next(q):
        to = half[q]
        steps[q] += [
            net.copy(back.at[HALF[1], xr, to], from_left.at[q, HALF[1]], to_xr),
            net.copy(back.at[HALF[0], xl, to], from_right.at[q, HALF[0]], to_xl),
        ]

    step_over(0)
    step_next(0)

    def step_right(q):
        to = half[q]
        steps[q][0].wait_recv()
        for j in range(10):
            back[j, xr, to] = added(back[j, xr, to], relay_left[q, j])
        steps[q].append(
            net.copy(back.at[HALF[0], xr, to], from_left.at[q, HALF[0]], to_xr)
        )

    def step_left(q):
        to = half[q]
        steps[q][1].wait_recv()
        for j in range(10, 19):
            back[j, xl, to] = added(back[j, xl, to], relay_right[q, j - 10])
        steps[q].append(
            net.copy(back.at[HALF[1], xl, to], from_right.at[q, HALF[1]], to_xl)
        )

    def own_sum(q, j):
        return (
            back[j, x, half[q]].astype(F32)
            + from_left[q, j].astype(F32)
            + from_right[q, j].astype(F32)
        )

    fars = []

    def send_far(i):
        for at in ((4, 3), (2, 5))[i]:
            steps[0][at].wait_recv()
        for j in range(19)[HALF[i]]:
            to_far[j] = own_sum(0, j).astype(BF16)
        fars.append(net.copy(to_far.at[HALF[i]], far.at[HALF[i]], to_far_half))

    def forward(p, x_from, h_from, device):
        block = every.at[PIECES[p], x_from, h_from]
        return net.copy(block, block, device)

    over_own, over_cross, cross_r, cross_l = {}, {}, {}, {}
    twins = [[], [], []]

    def to_twin_core(p, h_from):
        block = every.at[PIECES[p], :, h_from]
        twins[p].append(net.copy(block, twin.at[PIECES[p], :, h_from], to_twin))

    flats = (flat_one, flat_zero, flat_two)
    sels = (sel_one, sel_zero, sel_two)
    rights = (right_one, right_zero, right_two)
    parts = (part_one, part_zero, part_two)
    pass_left = (pass_left_one, pass_left_zero, pass_left_two)
    pass_right = (pass_right_one, pass_right_zero, pass_right_two)
    up_left = (up_left_one, up_left_zero, up_left_two)
    up_right = (up_right_one, up_right_zero, up_right_two)
    to_line = (to_line_one, to_line_zero, to_line_two)
    line = (line_one, line_zero, line_two)
    kept = (kept_one, kept_zero, kept_two)

    def spread_flat(buffer, lane, p):
        start, blocks, runs = ((5, 4, 2), (0, 5, 1), (13, 3, 2))[p]
        for i in range(runs):
            at = (runs * lane + i) * edges
            flats[p][:, at : at + edges] = buffer[
                start + i * blocks : start + (i + 1) * blocks
            ].reshape(blocks * C, edges)

    climbs, lines = [None] * 3, []

    def halves(p):
        return slice(0, SPLIT[p]), slice(SPLIT[p], UNIT[p] * TILES[p])

    def climb(p):
        for one in twins[p]:
            one.wait_recv()
        spread_flat(twin, 1, p)
        rows, tiles = UNIT[p], TILES[p]
        for i in range(16):
            begin = pl.multiple_of((2 * i + core) * rows, 16)
            sels[p][i * rows : (i + 1) * rows, :] = flats[p][pl.ds(begin, rows), :]
        for quarter in range(4):
            out = nt(
                sels[p][quarter * 4 * rows : (quarter + 1) * 4 * rows, :], rights[p][...]
            )
            out = out.astype(BF16).reshape(4, rows, 128 * tiles)
            for tile in range(tiles):
                parts[p][quarter, :, tile * rows : (tile + 1) * rows, :] = out[
                    :, :, 128 * tile : 128 * (tile + 1)
                ]
        a, b = halves(p)
        climbs[p] = [
            net.copy(parts[p].at[yo, :, a], pass_left[p], to_yr),
            net.copy(parts[p].at[yo, :, b], pass_right[p], to_yl),
            net.copy(parts[p].at[yr, :, b], up_left[p].at[:, b], to_yr),
            net.copy(parts[p].at[yl, :, a], up_right[p].at[:, a], to_yl),
        ]

    def climb_on(p):
        a, b = halves(p)
        climbs[p][0].wait_recv()
        parts[p][yr, :, a] = added(parts[p][yr, :, a], pass_left[p][...])
        climbs[p].append(net.copy(parts[p].at[yr, :, a], up_left[p].at[:, a], to_yr))
        climbs[p][1].wait_recv()
        parts[p][yl, :, b] = added(parts[p][yl, :, b], pass_right[p][...])
        climbs[p].append(net.copy(parts[p].at[yl, :, b], up_right[p].at[:, b], to_yl))

    def climbed(p):
        for one in climbs[p][2:]:
            one.wait_recv()
        for o in (2, 3, 1, 0):
            to = lax.rem(z + o, 4)
            total = (
                parts[p][y, to].astype(F32)
                + up_left[p][to].astype(F32)
                + up_right[p][to].astype(F32)
            )
            if o:
                to_line[p][o - 1] = total.astype(BF16)
                lines.append(
                    net.copy(to_line[p].at[o - 1], line[p].at[o - 1], line_peers[o])
                )
            else:
                kept[p][...] = total

    def right_side(buffer, lane):
        wide = 5 * local
        right_zero[0:wide, lane * edges : (lane + 1) * edges] = buffer[0:5].reshape(wide, edges)
        for right, start, blocks in ((right_one, 5, 4), (right_two, 13, 3)):
            rows = blocks * local
            plus = buffer[start : start + blocks].reshape(rows, edges)
            minus = buffer[start + blocks : start + 2 * blocks].reshape(rows, edges)
            at = 2 * lane * edges
            right[0:rows, at : at + edges] = plus
            right[0:rows, at + edges : at + 2 * edges] = minus
            right[rows : 2 * rows, at : at + edges] = minus
            right[rows : 2 * rows, at + edges : at + 2 * edges] = -plus

    near_r[0].wait_recv()
    over_own[0] = forward(0, xl, h, to_xr)
    cross[0].wait_recv()
    cross_r[0] = forward(0, x, 1 - h, to_xr)
    cross_l[0] = forward(0, x, 1 - h, to_xl)
    step_right(0)
    near(1)
    cross_l[0].wait_recv()
    over_cross[0] = forward(0, xr, 1 - h, to_xl)
    step_left(0)
    cross[1].wait_recv()
    cross_r[1] = forward(1, x, 1 - h, to_xr)
    cross_l[1] = forward(1, x, 1 - h, to_xl)
    near_l[1].wait_recv()
    over_own[1] = forward(1, xr, h, to_xl)
    near(2)
    near_l[0].wait_recv()
    over_own[0].wait_recv()
    to_twin_core(0, h)
    for one in asked:
        one.wait_recv()
    square_sum = square[...]
    for i in range(7):
        square_sum = square_sum + squares[i]
    inverse_both = lax.rsqrt(square_sum / (25 * C) + EPSILON)
    inverse, inverse_a = inverse_both[0:1, :], inverse_both[1:2, :]
    for j in range(19):
        scaled[j] = (grads[j].astype(F32) * inverse).astype(BF16)
    scaled_copy = net.copy(scaled, scaled_twin, to_twin)

    right_zero[...] = jnp.zeros_like(right_zero)
    right_side(scaled, 0)

    cross_r[0].wait_recv()
    over_cross[0].wait_recv()
    to_twin_core(0, 1 - h)
    spread_flat(every, 0, 0)
    send_far(0)
    scaled_copy.wait_recv()
    right_side(scaled_twin, 1)
    climb(0)
    send_far(1)
    cross_r[1].wait_recv()
    over_cross[1] = forward(1, xl, 1 - h, to_xr)
    cross[2].wait_recv()
    cross_r[2] = forward(2, x, 1 - h, to_xr)
    cross_l[2] = forward(2, x, 1 - h, to_xl)
    near_r[1].wait_recv()
    over_own[1].wait_recv()
    to_twin_core(1, h)
    cross_l[1].wait_recv()
    over_cross[1].wait_recv()
    to_twin_core(1, 1 - h)
    spread_flat(every, 0, 1)
    climb_on(0)
    near_l[2].wait_recv()
    over_own[2] = forward(2, xr, h, to_xl)
    climb(1)
    cross_r[2].wait_recv()
    over_cross[2] = forward(2, xl, 1 - h, to_xr)
    step_over(1)
    step_next(1)
    near_r[2].wait_recv()
    over_own[2].wait_recv()
    to_twin_core(2, h)
    cross_l[2].wait_recv()
    over_cross[2].wait_recv()
    to_twin_core(2, 1 - h)
    spread_flat(every, 0, 2)

    mixed[0:5] = nn(w_zero[...].reshape(5 * local, 5 * C), flat_zero[:, 0:edges]).reshape(
        5, local, edges
    )
    for w, flat, start, blocks in ((w_one, flat_one, 5, 4), (w_two, flat_two, 13, 3)):
        size = blocks * C
        both = flat[:, 0 : 2 * edges]
        real = nn(w[0].reshape(blocks * local, size), both)
        imag = nn(w[1].reshape(blocks * local, size), both)
        mixed[start : start + blocks] = (real[:, :edges] - imag[:, edges:]).reshape(
            blocks, local, edges
        )
        mixed[start + blocks : start + 2 * blocks] = (
            real[:, edges:] + imag[:, :edges]
        ).reshape(blocks, local, edges)
    total = jnp.zeros((1, edges), F32)
    for j in range(19):
        total = total + jnp.sum(mixed[j] * grads[j].astype(F32), axis=0, keepdims=True)
    tally[...] = jnp.broadcast_to(total, tally.shape)
    counted = [net.copy(tally, tallies.at[i], d) for i, d in enumerate(chan_peers)]

    climb_on(1)
    climb(2)
    climbed(0)
    step_right(1)
    step_left(1)

    scale = weight[...] * inverse
    for j in range(19):
        mixed[j] = mixed[j] * scale
    for l in range(5):
        for k in range(l * l, (l + 1) * (l + 1)):
            message[k] = rotate_out(rot, mixed, k, l).astype(BF16)
    update[...] = (
        nt(message[...].reshape(count, edges), arrive).reshape(25, local, atoms).astype(BF16)
    )
    climbed(1)
    climb_on(2)
    for one in steps[1][2:]:
        one.wait_recv()
    for j in range(19):
        mixed[j] = own_sum(1, j)

    for one in counted:
        one.wait_recv()
    tally_sum = tally[...]
    for i in range(7):
        tally_sum = tally_sum + tallies[i]
    for one in fars:
        one.wait_recv()
    for j in range(19):
        mixed[j] = mixed[j] + far[j].astype(F32)
    for l in range(5):
        for k in range(l * l, (l + 1) * (l + 1)):
            message[k] = rotate_out(rot, mixed, k, l).astype(BF16)
    flat = message[...].reshape(count, edges)
    leaving[...] = nt(near_hot, flat).astype(BF16)

    def exact(left, right, dims):
        return lax.dot_general(
            left, right, (dims, ((), ())),
            precision=lax.Precision.HIGHEST, preferred_element_type=F32,
        )

    side = lax.broadcasted_iota(jnp.int32, (128, edges), 0)
    side = side + jnp.where(side < 16, atoms + 16, atoms - 16)
    side_hot = jnp.where(side == source[...], 1.0, 0.0)
    tally_out[...] = exact(tally_sum, side_hot, ((1,), (1,)))
    halo = [
        net.copy(leaving.at[16:32], returned.at[0:16], to_ahead),
        net.copy(leaving.at[0:16], returned.at[16:32], to_behind),
        net.copy(tally_out, tally_in.at[0], to_ahead),
        net.copy(tally_out, tally_in.at[1], to_behind),
    ]
    own[...] = nt(flat, here).reshape(25, local, atoms)
    tally_a = exact(tally_sum, here.astype(F32), ((1,), (1,)))
    climbed(2)
    for one in halo:
        one.wait_recv()
    settled[...] = tn(returned[...], face_hot).reshape(25, local, atoms)
    lane = lax.broadcasted_iota(jnp.int32, (8, 128), 1)
    tally_face = jnp.where(lane < 16, tally_in[0], tally_in[1])
    tally_a = tally_a + exact(tally_face[:, 0:32], face_hot.astype(F32), ((1,), (0,)))
    factor = inverse_a * inverse_a * inverse_a * tally_a[0:1, :] / (25 * C)
    for l in range(5):
        gain_l = gain_t[0:local, l : l + 1] * inverse_a
        for k in range(l * l, (l + 1) * (l + 1)):
            grad_embed[k] = (
                (own[k] + settled[k]) * gain_l - embed[k].astype(F32) * factor
            ).astype(BF16)
    for one in lines:
        one.wait_recv()
    for p, out, width in ((0, sum_one, 512), (1, sum_zero, 384), (2, sum_two, 384)):
        total = kept[p][...]
        for i in range(3):
            total = total + line[p][i].astype(F32)
        for tile in range(TILES[p]):
            begin, end = 128 * tile, min(128 * (tile + 1), width)
            out[:, begin:end] = total[tile * UNIT[p] : (tile + 1) * UNIT[p], 0 : end - begin]
    net.finish()


def finish_kernel(
    update_in, grad_in, sum_zero, sum_one, sum_two, update, grad, grad_zero, grad_one, grad_two
):
    update[...] = update_in[...]
    grad[...] = grad_in[...]
    local = grad_zero.shape[1]
    for t in range(2):
        turned = sum_zero[:, 128 * t : 128 * (t + 1)].T
        grad_zero[2 * t] = turned[:local]
        grad_zero[2 * t + 1] = turned[local:]
    grad_zero[4] = sum_zero[:, 256:384].T[:local]
    for t in range(4):
        turned = sum_one[:, 128 * t : 128 * (t + 1)].T
        for i in (0, 1):
            grad_one[(2 * t + i) // 4, (2 * t + i) % 4] = turned[i * local : (i + 1) * local]
    for i in range(6):
        grad_two[i // 3, i % 3] = sum_two[:, i * local : (i + 1) * local]


def shards(
    embed, gain, w_zero, w_one, w_two, rot_table, face_atoms, edge_source, edge_target,
    rot_index, edge_weight, cotangent,
):
    atoms = embed.shape[2]
    local = embed.shape[1]
    edges = edge_source.shape[0]
    row = lambda a: a.reshape(1, edges)
    vmem = pl.BlockSpec(memory_space=pltpu.VMEM)
    hbm = pl.BlockSpec(memory_space=pltpu.HBM)
    block = (19, local, edges)
    args = (
        embed, cotangent, gain, rot_table.transpose(1, 0, 2), face_atoms.reshape(1, -1),
        row(edge_source), row(edge_target), row(rot_index), row(edge_weight),
        w_zero, w_one, w_two,
    )
    scratch = [(a.shape, a.dtype) for a in args[:9]]
    scratch += [
        (w_zero.shape, BF16),
        (w_one.shape, BF16),
        (w_two.shape, BF16),
        ((128, 128), F32),
        ((128, 128), F32),
        ((32, 25 * local), BF16),
        ((32, 25 * local), BF16),
        ((25, 19, edges), F32),
        ((25, local, edges), F32),
        (block, BF16),
        (block, BF16),
        ((8, edges), F32),
        ((7, 8, edges), F32),
        ((19, 4, 2, local, edges), BF16),
        ((19, 4, 2, local, edges), BF16),
        ((19, 4, 2, local, edges), BF16),
        ((2, 10, local, edges), BF16),
        ((2, 9, local, edges), BF16),
        ((2, 19, local, edges), BF16),
        ((2, 19, local, edges), BF16),
        (block, BF16),
        (block, BF16),
        (block, BF16),
        (block, BF16),
        ((5 * C, 2 * edges), BF16),
        ((4 * C, 4 * edges), BF16),
        ((3 * C, 4 * edges), BF16),
        ((1280, 2 * edges), BF16),
        ((1024, 4 * edges), BF16),
        ((768, 4 * edges), BF16),
        ((384, 2 * edges), BF16),
        ((512, 4 * edges), BF16),
        ((384, 4 * edges), BF16),
    ]
    for p in range(3):
        rows = UNIT[p] * TILES[p]
        scratch += [
            ((4, 4, rows, 128), BF16),
            ((4, SPLIT[p], 128), BF16),
            ((4, rows - SPLIT[p], 128), BF16),
            ((4, rows, 128), BF16),
            ((4, rows, 128), BF16),
            ((3, rows, 128), BF16),
            ((3, rows, 128), BF16),
            ((rows, 128), F32),
        ]
    scratch += [
        (block, F32),
        ((25, local, edges), BF16),
        ((8, edges), F32),
        ((7, 8, edges), F32),
        ((25, local, atoms), F32),
        ((32, 25 * local), BF16),
        ((32, 25 * local), BF16),
        ((8, 128), F32),
        ((2, 8, 128), F32),
        ((25, local, atoms), F32),
    ]
    update, grad_embed, sum_zero, sum_one, sum_two = pl.pallas_call(
        layer_kernel,
        name="layer",
        out_shape=[
            jax.ShapeDtypeStruct((25, local, atoms), BF16),
            jax.ShapeDtypeStruct((25, local, atoms), BF16),
            jax.ShapeDtypeStruct((80, 384), F32),
            jax.ShapeDtypeStruct((64, 8 * local), F32),
            jax.ShapeDtypeStruct((48, 6 * local), F32),
        ],
        in_specs=[hbm] * 12,
        out_specs=[vmem] * 5,
        scratch_shapes=[pltpu.VMEM(s, t) for s, t in scratch]
        + [
            pltpu.SemaphoreType.DMA((COPIES,)),
            pltpu.SemaphoreType.DMA((COPIES,)),
            pltpu.SemaphoreType.DMA((12,)),
        ],
        compiler_params=pltpu.CompilerParams(
            vmem_limit_bytes=VMEM_LIMIT, collective_id=0, has_side_effects=True
        ),
    )(*(pltpu.with_memory_space_constraint(a, pltpu.HBM) for a in args))
    *outs, grad_two = pl.pallas_call(
        finish_kernel,
        name="finish",
        out_shape=[
            jax.ShapeDtypeStruct((25, local, atoms), BF16),
            jax.ShapeDtypeStruct((25, local, atoms), BF16),
            jax.ShapeDtypeStruct((5, local, 80), F32),
            jax.ShapeDtypeStruct((2, 4, local, 64), F32),
            jax.ShapeDtypeStruct((2, 3, 48, local), F32),
        ],
        in_specs=[vmem] * 5,
        out_specs=[vmem] * 5,
        compiler_params=pltpu.CompilerParams(vmem_limit_bytes=FINISH_LIMIT),
    )(update, grad_embed, sum_zero, sum_one, sum_two)
    return (*outs, grad_two.transpose(0, 1, 3, 2))


def solution(mesh):
    torus = Mesh(mesh.devices.reshape(4, 4, 2, 4, 2), ("y", "z", "core", "x", "zh"))
    return jax.shard_map(
        shards,
        mesh=torus,
        in_specs=(
            P(None, CHAN, GRAPH),
            P(None, CHAN),
            P(None, CHAN, None),
            P(None, None, CHAN, None),
            P(None, None, CHAN, None),
            P(),
            P(GRAPH),
            P(GRAPH),
            P(GRAPH),
            P(GRAPH),
            P(GRAPH),
            P(None, CHAN, GRAPH),
        ),
        out_specs=(
            P(None, CHAN, GRAPH),
            P(None, CHAN, GRAPH),
            P(None, CHAN, GRAPH),
            P(None, None, CHAN, GRAPH),
            P(None, None, CHAN, GRAPH),
        ),
        check_vma=False,
    )
```

```python
import jax
import jax.numpy as jnp
from jax import lax
from jax.experimental import pallas as pl
from jax.experimental.pallas import tpu as pltpu
from jax.sharding import Mesh
from jax.sharding import PartitionSpec as P

C = 512
EPSILON = 1e-06
CHAN = ("x", "zh")
GRAPH = ("y", "z", "core")
DEGREE = (0, 1, 2, 3, 4, 1, 2, 3, 4, 1, 2, 3, 4, 2, 3, 4, 2, 3, 4)
ROWS = tuple(tuple(j for j in range(19) if DEGREE[j] == l) for l in range(5))
F32 = jnp.float32
BF16 = jnp.bfloat16
VMEM_LIMIT = 46 * 1024 * 1024
FINISH_LIMIT = 8 * 1024 * 1024
MESH = pl.DeviceIdType.MESH
PIECES = (slice(5, 13), slice(0, 5), slice(13, 19))
HALF = (slice(0, 10), slice(10, 19))
UNIT = (64, 80, 48)
TILES = (4, 3, 3)
SPLIT = (128, 128, 80)


def nt(left, right):
    return lax.dot_general(left, right, (((1,), (1,)), ((), ())), preferred_element_type=F32)


def tn(left, right):
    return lax.dot_general(left, right, (((0,), (0,)), ((), ())), preferred_element_type=F32)


def nn(left, right):
    return jnp.dot(left, right, preferred_element_type=F32)


def hot(index_row, rows, first=0):
    edges = index_row.shape[1]
    row = lax.broadcasted_iota(jnp.int32, (rows, edges), 0) + first
    return jnp.where(row == index_row, 1.0, 0.0).astype(BF16)


def rotate_in(rot, values, j):
    l = DEGREE[j]
    total = None
    for k in range(l * l, (l + 1) * (l + 1)):
        term = rot[k, j : j + 1, :] * values[k]
        total = term if total is None else total + term
    return total


def rotate_out(rot, values, k, l):
    total = None
    for j in ROWS[l]:
        term = rot[k, j : j + 1, :] * values[j]
        total = term if total is None else total + term
    return total


class Net:
    def __init__(self, send, recv):
        self.send, self.recv, self.started = send, recv, []

    def copy(self, source, landing, device):
        at = len(self.started)
        assert at < COPIES
        one = pltpu.make_async_remote_copy(
            src_ref=source,
            dst_ref=landing,
            send_sem=self.send.at[at],
            recv_sem=self.recv.at[at],
            device_id=device,
            device_id_type=MESH,
        )
        one.start()
        self.started.append(one)
        return one

    def finish(self):
        for one in self.started:
            one.wait_send()


COPIES = 92


def layer_kernel(
    embed_hbm, cotangent_hbm, gain_hbm, rot_table_hbm, face_hbm,
    source_hbm, target_hbm, spin_hbm, weight_hbm, w_zero_hbm, w_one_hbm, w_two_hbm,
    update, grad_embed, sum_zero, sum_one, sum_two,
    embed, cotangent, gain, rot_table, face, source, target, spin, weight,
    w_zero, w_one, w_two, corner, gain_t, faces, halo_t, rot, values, grads, mine, square, squares, every, twin,
    back, relay_left, relay_right, from_left, from_right, to_far, far,
    scaled, scaled_twin, flat_zero, flat_one, flat_two, sel_zero, sel_one, sel_two,
    right_zero, right_one, right_two,
    part_one, pass_left_one, pass_right_one, up_left_one, up_right_one, to_line_one, line_one,
    kept_one,
    part_zero, pass_left_zero, pass_right_zero, up_left_zero, up_right_zero, to_line_zero,
    line_zero, kept_zero,
    part_two, pass_left_two, pass_right_two, up_left_two, up_right_two, to_line_two, line_two,
    kept_two,
    mixed, message, tally, tallies, own, leaving, returned,
    tally_out, tally_in, settled, send, recv, load,
):
    x, h = lax.axis_index("x"), lax.axis_index("zh")
    y, z, core = lax.axis_index("y"), lax.axis_index("z"), lax.axis_index("core")
    xr, xl, xo = lax.rem(x + 1, 4), lax.rem(x + 3, 4), lax.rem(x + 2, 4)
    yr, yl, yo = lax.rem(y + 1, 4), lax.rem(y + 3, 4), lax.rem(y + 2, 4)
    me = y * 8 + z * 2 + core
    ahead, behind = lax.rem(me + 1, 32), lax.rem(me + 31, 32)

    def graph_at(g):
        return {"y": g // 8, "z": lax.rem(g // 2, 4), "core": lax.rem(g, 2)}

    to_xr, to_xl = {"x": xr}, {"x": xl}
    to_yr, to_yl = {"y": yr}, {"y": yl}
    to_far_half = {"zh": 1 - h}
    to_twin = {"core": 1 - core}
    to_ahead, to_behind = graph_at(ahead), graph_at(behind)
    chan_peers = [
        {"x": lax.rem(x + dx, 4), "zh": lax.rem(h + dh, 2)}
        for dx in range(4)
        for dh in range(2)
        if dx or dh
    ]
    line_peers = [None] + [{"z": lax.rem(z + o, 4)} for o in (1, 2, 3)]
    chan = x * 2 + h

    local = embed.shape[1]
    atoms = embed.shape[2]
    edges = source.shape[1]
    count = 25 * local
    net = Net(send, recv)

    loads = [
        pltpu.make_async_copy(a, b, load.at[i])
        for i, (a, b) in enumerate(
            (
                (embed_hbm, embed),
                (face_hbm, face),
                (rot_table_hbm, rot_table),
                (gain_hbm, gain),
                (source_hbm, source),
                (target_hbm, target),
                (spin_hbm, spin),
                (weight_hbm, weight),
                (cotangent_hbm, cotangent),
                (w_zero_hbm, w_zero),
                (w_one_hbm, w_one),
                (w_two_hbm, w_two),
            )
        )
    ]
    for one in loads:
        one.start()

    barrier = pltpu.get_barrier_semaphore()
    partners = chan_peers + line_peers[1:] + [to_yr, to_yl, to_ahead, to_behind]
    for device in partners:
        pl.semaphore_signal(barrier, inc=1, device_id=device, device_id_type=MESH)

    for one in loads[:2]:
        one.wait()
    corner[...] = jnp.zeros_like(corner)
    corner[0:1, 0:32] = face[...].astype(F32)
    face_col = jnp.broadcast_to(corner[0:1, :], (128, 128)).T[0:32].astype(jnp.int32)
    face_row = lax.broadcasted_iota(jnp.int32, (32, atoms), 1)
    face_hot = jnp.where(face_row == face_col, 1.0, 0.0).astype(BF16)
    flat_embed = embed[...].reshape(count, atoms)
    faces[...] = nt(face_hot, flat_embed).astype(BF16)
    pl.semaphore_wait(barrier, len(partners))
    halo = [
        net.copy(faces.at[16:32], halo_t.at[0:16], to_ahead),
        net.copy(faces.at[0:16], halo_t.at[16:32], to_behind),
    ]

    for one in loads[2:8]:
        one.wait()
    corner[0:5, 0:local] = gain[...]
    gain_t[...] = corner[...].T
    turn = hot(spin[...], rot_table.shape[2])
    for k in range(25):
        line_k = rot_table[k]
        high = line_k.astype(BF16)
        low = (line_k - high.astype(F32)).astype(BF16)
        rot[k] = nn(high, turn) + nn(low, turn)
    total_a = jnp.zeros((1, atoms), F32)
    for k in range(25):
        one = embed[k].astype(F32)
        total_a = total_a + jnp.sum(one * one, axis=0, keepdims=True)
    here = hot(source[...], atoms)
    near_hot = hot(source[...], 32, atoms)

    values[...] = nn(flat_embed, here).reshape(25, local, edges)
    for one in halo:
        one.wait_recv()
    values[...] += tn(halo_t[...], near_hot).reshape(25, local, edges)
    cross, near_r, near_l = [], [], []

    def near(p):
        here_at = mine.at[PIECES[p]]
        there_at = every.at[PIECES[p], x, h]
        near_r.append(net.copy(here_at, there_at, to_xr))
        near_l.append(net.copy(here_at, there_at, to_xl))

    def over(p):
        cross.append(net.copy(mine.at[PIECES[p]], every.at[PIECES[p], x, h], to_far_half))

    def own_frames(p):
        for j in range(19)[PIECES[p]]:
            l = DEGREE[j]
            one = (rotate_in(rot, values, j) * gain_t[0:local, l : l + 1]).astype(BF16)
            mine[j] = one
            every[j, x, h] = one

    own_frames(0)
    over(0)
    near(0)
    own_frames(1)
    own_frames(2)
    total_e = jnp.zeros((1, edges), F32)
    for k in range(25):
        one = values[k]
        total_e = total_e + jnp.sum(one * one, axis=0, keepdims=True)
    square[...] = jnp.concatenate([total_e, total_a, jnp.zeros((6, edges), F32)], axis=0)
    asked = [net.copy(square, squares.at[i], d) for i, d in enumerate(chan_peers)]
    over(1)
    over(2)

    loads[8].wait()
    arrive = hot(target[...], atoms)
    values[...] = nn(cotangent[...].reshape(count, atoms), arrive).reshape(25, local, edges)
    for j in range(19):
        grads[j] = (rotate_in(rot, values, j) * weight[...]).astype(BF16)

    for one in loads[9:]:
        one.wait()
    back[0:5] = tn(
        w_zero[...].reshape(5 * local, 5 * C), grads[0:5].reshape(5 * local, edges)
    ).astype(BF16).reshape(5, 4, 2, local, edges)
    for w, start, blocks in ((w_one, 5, 4), (w_two, 13, 3)):
        plus = grads[start : start + blocks].reshape(blocks * local, edges)
        minus = grads[start + blocks : start + 2 * blocks].reshape(blocks * local, edges)
        both = jnp.concatenate([plus, minus], axis=1)
        turned = jnp.concatenate([minus, -plus], axis=1)
        size = blocks * C
        out = tn(w[0].reshape(blocks * local, size), both) + tn(
            w[1].reshape(blocks * local, size), turned
        )
        back[start : start + blocks] = (
            out[:, :edges].astype(BF16).reshape(blocks, 4, 2, local, edges)
        )
        back[start + blocks : start + 2 * blocks] = (
            out[:, edges:].astype(BF16).reshape(blocks, 4, 2, local, edges)
        )

    def added(a, b):
        return (a.astype(F32) + b.astype(F32)).astype(BF16)

    half = (1 - h, h)
    steps = [[], []]

    def step_over(q):
        to = half[q]
        steps[q] = [
            net.copy(back.at[HALF[0], xo, to], relay_left.at[q], to_xr),
            net.copy(back.at[HALF[1], xo, to], relay_right.at[q], to_xl),
        ]

    def step_next(q):
        to = half[q]
        steps[q] += [
            net.copy(back.at[HALF[1], xr, to], from_left.at[q, HALF[1]], to_xr),
            net.copy(back.at[HALF[0], xl, to], from_right.at[q, HALF[0]], to_xl),
        ]

    step_over(0)
    step_next(0)

    def step_right(q):
        to = half[q]
        steps[q][0].wait_recv()
        for j in range(10):
            back[j, xr, to] = added(back[j, xr, to], relay_left[q, j])
        steps[q].append(
            net.copy(back.at[HALF[0], xr, to], from_left.at[q, HALF[0]], to_xr)
        )

    def step_left(q):
        to = half[q]
        steps[q][1].wait_recv()
        for j in range(10, 19):
            back[j, xl, to] = added(back[j, xl, to], relay_right[q, j - 10])
        steps[q].append(
            net.copy(back.at[HALF[1], xl, to], from_right.at[q, HALF[1]], to_xl)
        )

    def own_sum(q, j):
        return (
            back[j, x, half[q]].astype(F32)
            + from_left[q, j].astype(F32)
            + from_right[q, j].astype(F32)
        )

    fars = []

    def send_far(i):
        for at in ((4, 3), (2, 5))[i]:
            steps[0][at].wait_recv()
        for j in range(19)[HALF[i]]:
            to_far[j] = own_sum(0, j).astype(BF16)
        fars.append(net.copy(to_far.at[HALF[i]], far.at[HALF[i]], to_far_half))

    def forward(p, x_from, h_from, device):
        block = every.at[PIECES[p], x_from, h_from]
        return net.copy(block, block, device)

    over_own, over_cross, cross_r, cross_l = {}, {}, {}, {}
    twins = [[], [], []]

    def to_twin_core(p, h_from):
        block = every.at[PIECES[p], :, h_from]
        twins[p].append(net.copy(block, twin.at[PIECES[p], :, h_from], to_twin))

    flats = (flat_one, flat_zero, flat_two)
    sels = (sel_one, sel_zero, sel_two)
    rights = (right_one, right_zero, right_two)
    parts = (part_one, part_zero, part_two)
    pass_left = (pass_left_one, pass_left_zero, pass_left_two)
    pass_right = (pass_right_one, pass_right_zero, pass_right_two)
    up_left = (up_left_one, up_left_zero, up_left_two)
    up_right = (up_right_one, up_right_zero, up_right_two)
    to_line = (to_line_one, to_line_zero, to_line_two)
    line = (line_one, line_zero, line_two)
    kept = (kept_one, kept_zero, kept_two)

    def spread_flat(buffer, lane, p):
        start, blocks, runs = ((5, 4, 2), (0, 5, 1), (13, 3, 2))[p]
        for i in range(runs):
            at = (runs * lane + i) * edges
            flats[p][:, at : at + edges] = buffer[
                start + i * blocks : start + (i + 1) * blocks
            ].reshape(blocks * C, edges)

    climbs, lines = [None] * 3, []

    def halves(p):
        return slice(0, SPLIT[p]), slice(SPLIT[p], UNIT[p] * TILES[p])

    def climb(p):
        for one in twins[p]:
            one.wait_recv()
        spread_flat(twin, 1, p)
        rows, tiles = UNIT[p], TILES[p]
        for i in range(16):
            begin = pl.multiple_of((2 * i + core) * rows, 16)
            sels[p][i * rows : (i + 1) * rows, :] = flats[p][pl.ds(begin, rows), :]
        for quarter in range(4):
            out = nt(
                sels[p][quarter * 4 * rows : (quarter + 1) * 4 * rows, :], rights[p][...]
            )
            out = out.astype(BF16).reshape(4, rows, 128 * tiles)
            for tile in range(tiles):
                parts[p][quarter, :, tile * rows : (tile + 1) * rows, :] = out[
                    :, :, 128 * tile : 128 * (tile + 1)
                ]
        a, b = halves(p)
        climbs[p] = [
            net.copy(parts[p].at[yo, :, a], pass_left[p], to_yr),
            net.copy(parts[p].at[yo, :, b], pass_right[p], to_yl),
            net.copy(parts[p].at[yr, :, b], up_left[p].at[:, b], to_yr),
            net.copy(parts[p].at[yl, :, a], up_right[p].at[:, a], to_yl),
        ]

    def climb_on(p):
        a, b = halves(p)
        climbs[p][0].wait_recv()
        parts[p][yr, :, a] = added(parts[p][yr, :, a], pass_left[p][...])
        climbs[p].append(net.copy(parts[p].at[yr, :, a], up_left[p].at[:, a], to_yr))
        climbs[p][1].wait_recv()
        parts[p][yl, :, b] = added(parts[p][yl, :, b], pass_right[p][...])
        climbs[p].append(net.copy(parts[p].at[yl, :, b], up_right[p].at[:, b], to_yl))

    def climbed(p):
        for one in climbs[p][2:]:
            one.wait_recv()
        for o in (2, 3, 1, 0):
            to = lax.rem(z + o, 4)
            total = (
                parts[p][y, to].astype(F32)
                + up_left[p][to].astype(F32)
                + up_right[p][to].astype(F32)
            )
            if o:
                to_line[p][o - 1] = total.astype(BF16)
                lines.append(
                    net.copy(to_line[p].at[o - 1], line[p].at[o - 1], line_peers[o])
                )
            else:
                kept[p][...] = total

    def right_side(buffer, lane):
        wide = 5 * local
        right_zero[0:wide, lane * edges : (lane + 1) * edges] = buffer[0:5].reshape(wide, edges)
        for right, start, blocks in ((right_one, 5, 4), (right_two, 13, 3)):
            rows = blocks * local
            plus = buffer[start : start + blocks].reshape(rows, edges)
            minus = buffer[start + blocks : start + 2 * blocks].reshape(rows, edges)
            at = 2 * lane * edges
            right[0:rows, at : at + edges] = plus
            right[0:rows, at + edges : at + 2 * edges] = minus
            right[rows : 2 * rows, at : at + edges] = minus
            right[rows : 2 * rows, at + edges : at + 2 * edges] = -plus

    near_r[0].wait_recv()
    over_own[0] = forward(0, xl, h, to_xr)
    cross[0].wait_recv()
    cross_r[0] = forward(0, x, 1 - h, to_xr)
    cross_l[0] = forward(0, x, 1 - h, to_xl)
    step_right(0)
    near(1)
    cross_l[0].wait_recv()
    over_cross[0] = forward(0, xr, 1 - h, to_xl)
    step_left(0)
    cross[1].wait_recv()
    cross_r[1] = forward(1, x, 1 - h, to_xr)
    cross_l[1] = forward(1, x, 1 - h, to_xl)
    near_l[1].wait_recv()
    over_own[1] = forward(1, xr, h, to_xl)
    near(2)
    near_l[0].wait_recv()
    over_own[0].wait_recv()
    to_twin_core(0, h)
    for one in asked:
        one.wait_recv()
    square_sum = square[...]
    for i in range(7):
        square_sum = square_sum + squares[i]
    inverse_both = lax.rsqrt(square_sum / (25 * C) + EPSILON)
    inverse, inverse_a = inverse_both[0:1, :], inverse_both[1:2, :]
    for j in range(19):
        scaled[j] = (grads[j].astype(F32) * inverse).astype(BF16)
    scaled_copy = net.copy(scaled, scaled_twin, to_twin)

    right_zero[...] = jnp.zeros_like(right_zero)
    right_side(scaled, 0)

    cross_r[0].wait_recv()
    over_cross[0].wait_recv()
    to_twin_core(0, 1 - h)
    spread_flat(every, 0, 0)
    send_far(0)
    scaled_copy.wait_recv()
    right_side(scaled_twin, 1)
    climb(0)
    send_far(1)
    cross_r[1].wait_recv()
    over_cross[1] = forward(1, xl, 1 - h, to_xr)
    cross[2].wait_recv()
    cross_r[2] = forward(2, x, 1 - h, to_xr)
    cross_l[2] = forward(2, x, 1 - h, to_xl)
    near_r[1].wait_recv()
    over_own[1].wait_recv()
    to_twin_core(1, h)
    cross_l[1].wait_recv()
    over_cross[1].wait_recv()
    to_twin_core(1, 1 - h)
    spread_flat(every, 0, 1)
    climb_on(0)
    near_l[2].wait_recv()
    over_own[2] = forward(2, xr, h, to_xl)
    climb(1)
    cross_r[2].wait_recv()
    over_cross[2] = forward(2, xl, 1 - h, to_xr)
    step_over(1)
    step_next(1)
    near_r[2].wait_recv()
    over_own[2].wait_recv()
    to_twin_core(2, h)
    climbed(0)
    cross_l[2].wait_recv()
    over_cross[2].wait_recv()
    to_twin_core(2, 1 - h)
    spread_flat(every, 0, 2)

    mixed[0:5] = nn(w_zero[...].reshape(5 * local, 5 * C), flat_zero[:, 0:edges]).reshape(
        5, local, edges
    )
    for w, flat, start, blocks in ((w_one, flat_one, 5, 4), (w_two, flat_two, 13, 3)):
        size = blocks * C
        both = flat[:, 0 : 2 * edges]
        real = nn(w[0].reshape(blocks * local, size), both)
        imag = nn(w[1].reshape(blocks * local, size), both)
        mixed[start : start + blocks] = (real[:, :edges] - imag[:, edges:]).reshape(
            blocks, local, edges
        )
        mixed[start + blocks : start + 2 * blocks] = (
            real[:, edges:] + imag[:, :edges]
        ).reshape(blocks, local, edges)
    total = jnp.zeros((1, edges), F32)
    for j in range(19):
        total = total + jnp.sum(mixed[j] * grads[j].astype(F32), axis=0, keepdims=True)
    tally[...] = jnp.broadcast_to(total, tally.shape)
    counted = [net.copy(tally, tallies.at[i], d) for i, d in enumerate(chan_peers)]

    climb_on(1)
    climb(2)
    step_right(1)
    step_left(1)

    scale = weight[...] * inverse
    for j in range(19):
        mixed[j] = mixed[j] * scale
    for l in range(5):
        for k in range(l * l, (l + 1) * (l + 1)):
            message[k] = rotate_out(rot, mixed, k, l).astype(BF16)
    update[...] = (
        nt(message[...].reshape(count, edges), arrive).reshape(25, local, atoms).astype(BF16)
    )
    climbed(1)
    climb_on(2)
    for one in steps[1][2:]:
        one.wait_recv()
    for j in range(19):
        mixed[j] = own_sum(1, j)

    for one in counted:
        one.wait_recv()
    tally_sum = tally[...]
    for i in range(7):
        tally_sum = tally_sum + tallies[i]
    for one in fars:
        one.wait_recv()
    for j in range(19):
        mixed[j] = mixed[j] + far[j].astype(F32)
    for l in range(5):
        for k in range(l * l, (l + 1) * (l + 1)):
            message[k] = rotate_out(rot, mixed, k, l).astype(BF16)
    flat = message[...].reshape(count, edges)
    leaving[...] = nt(near_hot, flat).astype(BF16)

    def exact(left, right, dims):
        return lax.dot_general(
            left, right, (dims, ((), ())),
            precision=lax.Precision.HIGHEST, preferred_element_type=F32,
        )

    side = lax.broadcasted_iota(jnp.int32, (128, edges), 0)
    side = side + jnp.where(side < 16, atoms + 16, atoms - 16)
    side_hot = jnp.where(side == source[...], 1.0, 0.0)
    tally_out[...] = exact(tally_sum, side_hot, ((1,), (1,)))
    halo = [
        net.copy(leaving.at[16:32], returned.at[0:16], to_ahead),
        net.copy(leaving.at[0:16], returned.at[16:32], to_behind),
        net.copy(tally_out, tally_in.at[0], to_ahead),
        net.copy(tally_out, tally_in.at[1], to_behind),
    ]
    own[...] = nt(flat, here).reshape(25, local, atoms)
    tally_a = exact(tally_sum, here.astype(F32), ((1,), (1,)))
    climbed(2)
    for one in halo:
        one.wait_recv()
    settled[...] = tn(returned[...], face_hot).reshape(25, local, atoms)
    lane = lax.broadcasted_iota(jnp.int32, (8, 128), 1)
    tally_face = jnp.where(lane < 16, tally_in[0], tally_in[1])
    tally_a = tally_a + exact(tally_face[:, 0:32], face_hot.astype(F32), ((1,), (0,)))
    factor = inverse_a * inverse_a * inverse_a * tally_a[0:1, :] / (25 * C)
    for l in range(5):
        gain_l = gain_t[0:local, l : l + 1] * inverse_a
        for k in range(l * l, (l + 1) * (l + 1)):
            grad_embed[k] = (
                (own[k] + settled[k]) * gain_l - embed[k].astype(F32) * factor
            ).astype(BF16)
    for p, out, width in ((0, sum_one, 512), (1, sum_zero, 384), (2, sum_two, 384)):
        for one in lines[3 * p : 3 * p + 3]:
            one.wait_recv()
        total = kept[p][...]
        for i in range(3):
            total = total + line[p][i].astype(F32)
        for tile in range(TILES[p]):
            begin, end = 128 * tile, min(128 * (tile + 1), width)
            out[:, begin:end] = total[tile * UNIT[p] : (tile + 1) * UNIT[p], 0 : end - begin]
    net.finish()


def finish_kernel(
    update_in, grad_in, sum_zero, sum_one, sum_two, update, grad, grad_zero, grad_one, grad_two
):
    update[...] = update_in[...]
    grad[...] = grad_in[...]
    local = grad_zero.shape[1]
    for t in range(2):
        turned = sum_zero[:, 128 * t : 128 * (t + 1)].T
        grad_zero[2 * t] = turned[:local]
        grad_zero[2 * t + 1] = turned[local:]
    grad_zero[4] = sum_zero[:, 256:384].T[:local]
    for t in range(4):
        turned = sum_one[:, 128 * t : 128 * (t + 1)].T
        for i in (0, 1):
            grad_one[(2 * t + i) // 4, (2 * t + i) % 4] = turned[i * local : (i + 1) * local]
    for i in range(6):
        grad_two[i // 3, i % 3] = sum_two[:, i * local : (i + 1) * local]


def shards(
    embed, gain, w_zero, w_one, w_two, rot_table, face_atoms, edge_source, edge_target,
    rot_index, edge_weight, cotangent,
):
    atoms = embed.shape[2]
    local = embed.shape[1]
    edges = edge_source.shape[0]
    row = lambda a: a.reshape(1, edges)
    vmem = pl.BlockSpec(memory_space=pltpu.VMEM)
    hbm = pl.BlockSpec(memory_space=pltpu.HBM)
    block = (19, local, edges)
    args = (
        embed, cotangent, gain, rot_table.transpose(1, 0, 2), face_atoms.reshape(1, -1),
        row(edge_source), row(edge_target), row(rot_index), row(edge_weight),
        w_zero, w_one, w_two,
    )
    scratch = [(a.shape, a.dtype) for a in args[:9]]
    scratch += [
        (w_zero.shape, BF16),
        (w_one.shape, BF16),
        (w_two.shape, BF16),
        ((128, 128), F32),
        ((128, 128), F32),
        ((32, 25 * local), BF16),
        ((32, 25 * local), BF16),
        ((25, 19, edges), F32),
        ((25, local, edges), F32),
        (block, BF16),
        (block, BF16),
        ((8, edges), F32),
        ((7, 8, edges), F32),
        ((19, 4, 2, local, edges), BF16),
        ((19, 4, 2, local, edges), BF16),
        ((19, 4, 2, local, edges), BF16),
        ((2, 10, local, edges), BF16),
        ((2, 9, local, edges), BF16),
        ((2, 19, local, edges), BF16),
        ((2, 19, local, edges), BF16),
        (block, BF16),
        (block, BF16),
        (block, BF16),
        (block, BF16),
        ((5 * C, 2 * edges), BF16),
        ((4 * C, 4 * edges), BF16),
        ((3 * C, 4 * edges), BF16),
        ((1280, 2 * edges), BF16),
        ((1024, 4 * edges), BF16),
        ((768, 4 * edges), BF16),
        ((384, 2 * edges), BF16),
        ((512, 4 * edges), BF16),
        ((384, 4 * edges), BF16),
    ]
    for p in range(3):
        rows = UNIT[p] * TILES[p]
        scratch += [
            ((4, 4, rows, 128), BF16),
            ((4, SPLIT[p], 128), BF16),
            ((4, rows - SPLIT[p], 128), BF16),
            ((4, rows, 128), BF16),
            ((4, rows, 128), BF16),
            ((3, rows, 128), BF16),
            ((3, rows, 128), BF16),
            ((rows, 128), F32),
        ]
    scratch += [
        (block, F32),
        ((25, local, edges), BF16),
        ((8, edges), F32),
        ((7, 8, edges), F32),
        ((25, local, atoms), F32),
        ((32, 25 * local), BF16),
        ((32, 25 * local), BF16),
        ((8, 128), F32),
        ((2, 8, 128), F32),
        ((25, local, atoms), F32),
    ]
    update, grad_embed, sum_zero, sum_one, sum_two = pl.pallas_call(
        layer_kernel,
        name="layer",
        out_shape=[
            jax.ShapeDtypeStruct((25, local, atoms), BF16),
            jax.ShapeDtypeStruct((25, local, atoms), BF16),
            jax.ShapeDtypeStruct((80, 384), F32),
            jax.ShapeDtypeStruct((64, 8 * local), F32),
            jax.ShapeDtypeStruct((48, 6 * local), F32),
        ],
        in_specs=[hbm] * 12,
        out_specs=[vmem] * 5,
        scratch_shapes=[pltpu.VMEM(s, t) for s, t in scratch]
        + [
            pltpu.SemaphoreType.DMA((COPIES,)),
            pltpu.SemaphoreType.DMA((COPIES,)),
            pltpu.SemaphoreType.DMA((12,)),
        ],
        compiler_params=pltpu.CompilerParams(
            vmem_limit_bytes=VMEM_LIMIT, collective_id=0, has_side_effects=True
        ),
    )(*(pltpu.with_memory_space_constraint(a, pltpu.HBM) for a in args))
    *outs, grad_two = pl.pallas_call(
        finish_kernel,
        name="finish",
        out_shape=[
            jax.ShapeDtypeStruct((25, local, atoms), BF16),
            jax.ShapeDtypeStruct((25, local, atoms), BF16),
            jax.ShapeDtypeStruct((5, local, 80), F32),
            jax.ShapeDtypeStruct((2, 4, local, 64), F32),
            jax.ShapeDtypeStruct((2, 3, 48, local), F32),
        ],
        in_specs=[vmem] * 5,
        out_specs=[vmem] * 5,
        compiler_params=pltpu.CompilerParams(vmem_limit_bytes=FINISH_LIMIT),
    )(update, grad_embed, sum_zero, sum_one, sum_two)
    return (*outs, grad_two.transpose(0, 1, 3, 2))


def solution(mesh):
    torus = Mesh(mesh.devices.reshape(4, 4, 2, 4, 2), ("y", "z", "core", "x", "zh"))
    return jax.shard_map(
        shards,
        mesh=torus,
        in_specs=(
            P(None, CHAN, GRAPH),
            P(None, CHAN),
            P(None, CHAN, None),
            P(None, None, CHAN, None),
            P(None, None, CHAN, None),
            P(),
            P(GRAPH),
            P(GRAPH),
            P(GRAPH),
            P(GRAPH),
            P(GRAPH),
            P(None, CHAN, GRAPH),
        ),
        out_specs=(
            P(None, CHAN, GRAPH),
            P(None, CHAN, GRAPH),
            P(None, CHAN, GRAPH),
            P(None, None, CHAN, GRAPH),
            P(None, None, CHAN, GRAPH),
        ),
        check_vma=False,
    )
```
